32 devices in a mesh: grp: 4 (over z), wave: 8 (over y, x, core).
Axes of the slice: x: 2, y: 2, z: 4, core: 2. Of those that a mesh axis runs over, the one named last changes fastest.
Arguments:
- state: bfloat16 [275, 61760], P(None, ('grp', 'wave')), may hold values from -6 to 6
- held_orders: int32 [160], P(('grp', 'wave')), may hold values from -1 to 95, as said below
- pair_lows: int32 [96], P(('grp', 'wave')), may hold values from 0 to 95, each once
- inverses: bfloat16 [96, 2, 137, 137], P(('grp', 'wave')), may hold values from -2 to 3
- height_operator: bfloat16 [137, 137], replicated, may hold values from -0.5 to 0.5
- pressure_column: bfloat16 [137], replicated, may hold values from -5 to 5
- thermal_response_matrix: bfloat16 [137, 137], replicated, may hold values from -0.5 to 0.5
- mass_row: bfloat16 [137], replicated, may hold values from -0.5 to 0.5
Outputs:
- advanced: bfloat16 [275, 61760], P(None, ('grp', 'wave'))
The draws below stay inside these ranges and needn't reach their ends.
Inputs may be any that keep to these rules, and one draw needn't show every extreme that they name: `held_orders`: each of 0 to 95 appears exactly once, all other entries are -1; some device has all 5 of its slots filled.
All inputs are finite; a program needn't handle non-finite values.
Results may differ from the reference program's by a relative error of at most 0.0052.
Values may be sent and summed in bfloat16 or wider, within the bound.
A program may use at most 128 MiB of HBM per device.

```python
import jax
import jax.numpy as jnp
from jax import lax

LEVELS = 137
KMAX = 5
HALF = 96
TRUNC = 191
ORDER_SLOTS = 160
WIDTH_SLOT = 386
COLS = 61760


def draw_held_orders(key, part):
    key_a, key_b, key_c = jax.random.split(jax.random.fold_in(key, 11), 3)
    slot_total = ORDER_SLOTS
    device_total = slot_total // KMAX
    scores = jax.random.permutation(key_a, slot_total).astype(jnp.int32)
    full_device = jax.random.randint(key_b, (), 0, device_total)
    owners = jnp.arange(slot_total, dtype=jnp.int32) // KMAX
    scores = scores - jnp.where(owners == full_device, slot_total, 0).astype(jnp.int32)
    ranking = jnp.argsort(jnp.argsort(scores))
    filled = ranking < HALF
    serial = jnp.cumsum(filled.astype(jnp.int32)) - 1
    orders = jax.random.permutation(key_c, HALF).astype(jnp.int32)
    picked = orders[jnp.clip(serial, 0, HALF - 1)]
    return jnp.where(filled, picked, -1).astype(jnp.int32)


def draw_inverses(key, part):
    key_a, key_b = jax.random.split(jax.random.fold_in(key, 23))
    diagonal = jax.random.uniform(key_a, (HALF, 2, LEVELS), jnp.float32, 0.6, 1.4)
    spread = jnp.clip(jax.random.normal(key_b, (HALF, 2, LEVELS, LEVELS), jnp.float32), -6.0, 6.0) * (0.6 / LEVELS ** 0.5)
    identity = jnp.eye(LEVELS, dtype=jnp.float32)
    return (spread + diagonal[..., None] * identity).astype(jnp.bfloat16)


def levels(rng, dims, pieces, low, top_value):
    level = 1.0
    for dim, parts in pieces:
        draws = jax.random.uniform(jax.random.fold_in(jax.random.fold_in(rng, 6), dim), (parts,), jnp.float32, low / len(pieces), top_value / len(pieces))
        level = level * jnp.repeat(jnp.exp(draws), dims[dim] // parts).reshape((-1,) + (1,) * (len(dims) - 1 - dim))
    return level


def noise(own_key, dims, deviation, most, pieces=(), held_as=jnp.bfloat16):
    loudness = levels(own_key, dims, pieces, -0.22, 0.18) if pieces else 1.0
    drawn = jax.random.normal(own_key, dims, jnp.float32) * deviation * loudness
    return jnp.minimum(jnp.maximum(drawn, -most), most).astype(held_as)


def setup_inputs(seed: int = 0) -> dict:
    splits = jax.random.split(jax.random.key(seed), 9)
    state = noise(splits[0], (2 * LEVELS + 1, COLS), 1.0, 6.0, ((1, 32),))
    held_orders = draw_held_orders(jax.random.fold_in(splits[8], 71), 0)
    pair_lows = jax.random.permutation(splits[2], HALF).astype(jnp.int32)
    inverses = draw_inverses(jax.random.fold_in(splits[8], 71), 0)
    height_operator = noise(splits[4], (LEVELS, LEVELS), LEVELS ** -0.5, 0.5)
    pressure_column = noise(splits[5], (LEVELS,), 1.0, 5.0)
    thermal_response_matrix = noise(splits[6], (LEVELS, LEVELS), LEVELS ** -0.5, 0.5)
    mass_row = noise(splits[7], (LEVELS,), LEVELS ** -0.5, 0.5)
    return {"state": state, "held_orders": held_orders, "pair_lows": pair_lows, "inverses": inverses, "height_operator": height_operator, "pressure_column": pressure_column, "thermal_response_matrix": thermal_response_matrix, "mass_row": mass_row}


def reference(state, held_orders, pair_lows, inverses, height_operator, pressure_column, thermal_response_matrix, mass_row):
    layer_heights_count = LEVELS
    truncation = TRUNC
    slot_width = WIDTH_SLOT
    slot_of = jnp.zeros((HALF,), jnp.int32).at[jnp.where(held_orders >= 0, held_orders, HALF)].set(
        jnp.arange(ORDER_SLOTS, dtype=jnp.int32), mode="drop")
    pair_of = jnp.zeros((HALF,), jnp.int32).at[pair_lows].set(jnp.arange(HALF, dtype=jnp.int32))
    coeff_index = jnp.arange(slot_width // 2, dtype=jnp.int32)
    denom = float(truncation * (truncation + 1))

    def pair_block(low_degree):
        high_degree = truncation - low_degree
        in_low = coeff_index <= low_degree
        degree = jnp.where(in_low, low_degree, high_degree)
        order_of = jnp.where(in_low, coeff_index, coeff_index - low_degree - 1)
        pair_m = jnp.minimum(order_of, truncation - order_of)
        position = jnp.where(order_of == pair_m, degree - order_of, degree + 1)
        first_col = slot_of[pair_m] * slot_width + 2 * position
        spectral_stacks = jnp.stack([first_col, first_col + 1], axis=1).reshape(-1).astype(jnp.int32)
        grouped_arrays = jnp.take(state, spectral_stacks, axis=1)
        divergence = grouped_arrays[:layer_heights_count]
        thermal_state_array = grouped_arrays[layer_heights_count:2 * layer_heights_count]
        pressure = grouped_arrays[2 * layer_heights_count]
        lap_scale = jnp.repeat((degree * (degree + 1)).astype(jnp.float32) / denom, 2)
        height_drive_term = jnp.dot(height_operator, thermal_state_array, preferred_element_type=jnp.float32)
        height_drive_term = height_drive_term + pressure_column.astype(jnp.float32)[:, None] * pressure.astype(jnp.float32)[None, :]
        right_side = (divergence.astype(jnp.float32) + lap_scale[None, :] * height_drive_term).astype(jnp.bfloat16)
        slot_pair = pair_of[low_degree]
        div_low = jnp.dot(inverses[slot_pair, 0], right_side, preferred_element_type=jnp.float32)
        div_high = jnp.dot(inverses[slot_pair, 1], right_side, preferred_element_type=jnp.float32)
        next_spreading_rate = jnp.where(jnp.repeat(in_low, 2)[None, :], div_low, div_high).astype(jnp.bfloat16)
        next_thermal_state = (thermal_state_array.astype(jnp.float32)
                    - jnp.dot(thermal_response_matrix, next_spreading_rate, preferred_element_type=jnp.float32)).astype(jnp.bfloat16)
        surface_mass_next = (pressure.astype(jnp.float32)
                     - jnp.dot(mass_row, next_spreading_rate, preferred_element_type=jnp.float32)).astype(jnp.bfloat16)
        return jnp.concatenate([next_spreading_rate, next_thermal_state, surface_mass_next[None, :]], axis=0), spectral_stacks

    blocks, spectral_stacks = lax.map(pair_block, jnp.arange(HALF, dtype=jnp.int32))
    rows = 2 * layer_heights_count + 1
    flat = jnp.transpose(blocks, (1, 0, 2)).reshape(rows, -1)
    result = jnp.zeros((rows, COLS), jnp.bfloat16)
    return result.at[:, spectral_stacks.reshape(-1)].set(flat)
```

```python
import functools

import jax
import jax.numpy as jnp
from jax import lax
from jax.experimental import pallas as pl
from jax.experimental.pallas import tpu as pltpu
from jax.sharding import PartitionSpec as P

MESH = pl.DeviceIdType.MESH
LANES = 128
ROWS_TILE = 16
TABLE_ROWS = 8
KEEP_BYTES = 24 << 20
scope = jax.named_scope


def ceil_to(value, step):
    return -(-value // step) * step


def kernel(
    size,
    held,
    lows,
    state_far,
    inverses,
    height_operator,
    pressure_column,
    thermal_response,
    mass_row,
    out,
    state,
    info,
    low_table,
    matrices,
    rest,
    right,
    pick,
    outgoing,
    arrived,
    solved,
    returned,
    total,
    info_send,
    info_recv,
    table_send,
    table_recv,
    z_send,
    z_recv,
    out_send,
    out_recv,
    back_send,
    back_recv,
    state_sem,
):
    Z, W, levels, slots, pairs = size
    half_count = Z * W * pairs
    truncation = 2 * half_count - 1
    slot_width = 2 * (truncation + 2)
    width = slots * slot_width
    denom = float(truncation * (truncation + 1))
    per_pair = 4 * slots
    block_pairs = 2 * pairs
    first_extra = block_pairs * per_pair
    moved = per_pair - 2
    last_slot = slots - 1
    stages = W.bit_length() - 1
    tail = levels - LANES
    keep = pick.shape[1] > 1
    z = lax.axis_index("grp")
    w = lax.axis_index("wave")
    middle = jnp.logical_and(z > 0, z < Z - 1)

    def wave_peer(i):
        return w + (1 << i) * (1 - 2 * lax.rem(w // (1 << i), 2))

    barrier = pltpu.get_barrier_semaphore()
    for i in range(stages):
        pl.semaphore_signal(barrier, inc=1, device_id=(z, wave_peer(i)), device_id_type=MESH)
    for i in range(1, Z):
        pl.semaphore_signal(barrier, inc=1, device_id=(lax.rem(z + i, Z), w), device_id_type=MESH)
    fetch = pltpu.make_async_copy(state_far, state, state_sem)
    fetch.start()

    lane = lax.broadcasted_iota(jnp.int32, (1, LANES), 1)
    lane_pair = lane // per_pair
    lane_member = lax.rem(lane, per_pair) // (2 * slots)
    lane_slot = lax.rem(lax.rem(lane, per_pair), 2 * slots) // 2
    lane_part = lax.rem(lane, 2)
    spare = lane >= first_extra
    is_moved = jnp.logical_and(lane >= moved, lane < moved + 2)
    orders = jnp.full((1, LANES), -1, jnp.int32)
    for s in range(slots):
        orders = jnp.where(lane_slot == s, held[s], orders)
    low_row = jnp.zeros((1, LANES), jnp.int32)
    for j in range(pairs):
        low_row = jnp.where(lax.rem(lane_pair, pairs) == j, lows[j], low_row)
    table_row = lax.broadcasted_iota(jnp.int32, (TABLE_ROWS, LANES), 0)
    info[w] = jnp.where(table_row == 0, low_row, orders)

    ends = []
    for i in range(2 * pairs):
        matrices[z, i, 0:levels, :] = inverses[i]
        ends.append(inverses[i, :, LANES:levels].astype(jnp.float32))
    ends = jnp.concatenate(ends, axis=1).astype(jnp.bfloat16)
    rest[z, 0:levels, 0 : 2 * pairs * tail] = ends

    with scope("barrier"):
        pl.semaphore_wait(barrier, stages + Z - 1)

    def z_copy(g, c, way):
        if c < pairs:
            ref = matrices.at[g, pl.ds(2 * c, 2), :, pl.ds(0, LANES)]
        else:
            ref = rest.at[g]
        step = 1 if way == 0 else -1
        return pltpu.make_async_remote_copy(
            src_ref=ref,
            dst_ref=ref,
            send_sem=z_send.at[g, c, way],
            recv_sem=z_recv.at[g, c],
            device_id=(z + step, w),
            device_id_type=MESH,
        )

    def forward(g, c):
        @pl.when(jnp.logical_and(g <= z, z < Z - 1))
        def _():
            z_copy(g, c, 0).start()

        @pl.when(jnp.logical_and(g >= z, z > 0))
        def _():
            z_copy(g, c, 1).start()

    def group_at(t):
        g = z
        for zz in range(Z):
            by_distance = sorted(range(Z), key=lambda a: abs(a - zz))
            g = jnp.where(z == zz, by_distance[t], g)
        return g

    def relay(*steps):
        @pl.when(middle)
        def _():
            for t, c in steps:
                g = group_at(t)
                z_copy(g, c, 0).wait_recv()
                forward(g, c)

    def arrive(*steps):
        @pl.when(jnp.logical_not(middle))
        def _():
            for t, c in steps:
                z_copy(group_at(t), c, 0).wait_recv()

    def info_copy(i, start):
        ref = info.at[pl.ds(start, 1 << i)]
        return pltpu.make_async_remote_copy(
            src_ref=ref,
            dst_ref=ref,
            send_sem=info_send.at[i],
            recv_sem=info_recv.at[i],
            device_id=(z, wave_peer(i)),
            device_id_type=MESH,
        )

    def block_start(who, i):
        return who // (1 << i) * (1 << i)

    def table_copy(k):
        return pltpu.make_async_remote_copy(
            src_ref=low_table.at[z],
            dst_ref=low_table.at[z],
            send_sem=table_send.at[k],
            recv_sem=table_recv.at[k],
            device_id=(lax.rem(z + k, Z), w),
            device_id_type=MESH,
        )

    def table_arrival(k):
        ref = low_table.at[lax.rem(z + Z - k, Z)]
        return pltpu.make_async_remote_copy(
            src_ref=ref,
            dst_ref=ref,
            send_sem=table_send.at[k],
            recv_sem=table_recv.at[k],
            device_id=(lax.rem(z + Z - k, Z), w),
            device_id_type=MESH,
        )

    forward(z, pairs)
    forward(z, 0)
    with scope("info0"):
        info_copy(0, block_start(w, 0)).start()

    column = lax.broadcasted_iota(jnp.int32, (1, width), 1)
    column_order = jnp.full((1, width), -1, jnp.int32)
    column_start = jnp.zeros((1, width), jnp.int32)
    for s in range(slots):
        inside = jnp.logical_and(column >= s * slot_width, column < (s + 1) * slot_width)
        column_order = jnp.where(inside, held[s], column_order)
        column_start = jnp.where(inside, s * slot_width, column_start)

    def drive_right():
        coefficient = (column - column_start) // 2
        degree = jnp.where(
            coefficient <= truncation - column_order, column_order + coefficient, coefficient - 1
        )
        lap_scale = (degree * (degree + 1)).astype(jnp.float32) / denom
        height = height_operator[...].astype(jnp.float32)
        pressure_row = jnp.broadcast_to(
            pressure_column[...].astype(jnp.float32).reshape(1, levels), height.shape
        )
        across = lax.broadcasted_iota(jnp.int32, height.shape, 1)
        down = lax.broadcasted_iota(jnp.int32, height.shape, 0)
        pressure_side = jnp.sum(
            jnp.where(across == down, pressure_row, 0.0), axis=1, keepdims=True
        )
        height = jnp.concatenate(
            [jnp.zeros((levels, tail), jnp.float32), height, pressure_side], axis=1
        ).astype(jnp.bfloat16)
        fetch.wait()
        drive = jnp.dot(height, state[LANES:, :], preferred_element_type=jnp.float32)
        right[0:levels, :] = (
            state[0:levels, :].astype(jnp.float32) + lap_scale * drive
        ).astype(jnp.bfloat16)

    for i in range(stages):
        with scope(f"info_wait{i}"):
            info_copy(i, block_start(wave_peer(i), i)).wait_recv()
        if i + 1 < stages:
            info_copy(i + 1, block_start(w, i + 1)).start()
        if i == 0:
            with scope("drive"):
                drive_right()
        if i == 1:
            for c in range(1, pairs - 1):
                forward(z, c)

    for d in range(W):
        low_table[z, d : d + 1, :] = info[d, 0:1, :]
    for k in range(1, Z):
        table_copy(k).start()
    for c in range(pairs - 1, pairs):
        forward(z, c)
    with scope("relay_a"):
        relay((1, pairs), (2, pairs), (1, 0), (2, 0))
    with scope("table_wait"):
        for k in range(1, Z):
            table_arrival(k).wait_recv()

    groups = [group_at(t) for t in range(Z)]

    def target_of(b, k):
        d = lax.rem(w + k, W)
        rows = [low_table[groups[t], pl.ds(d, 1), :] for t in range(Z)]
        low = jnp.where(lane < pairs * per_pair, rows[2 * b], rows[2 * b + 1])
        slot, member, order = lane_slot, lane_member, orders
        if b == 0:
            low = jnp.where(spare, rows[2], low)
            slot = jnp.where(spare, last_slot, slot)
            member = jnp.where(spare, 1, member)
            order = jnp.where(spare, held[last_slot], order)
        merged = jnp.where(order <= low, low - order, truncation + 1 - low)
        position = jnp.where(member == 0, merged, truncation - low - order)
        used = order >= 0
        if b == 0:
            used = jnp.logical_and(used, lane < first_extra + 2)
        else:
            extra = jnp.logical_or(spare, is_moved)
            position = jnp.where(extra, truncation + 1 - order, position)
        target = slot * slot_width + 2 * position + lane_part
        return jnp.where(used, target, -1)

    def build(b, i, place):
        at = lax.broadcasted_iota(jnp.int32, (width, LANES), 0)
        for h in range(2):
            pick[b, place, :, h * LANES : (h + 1) * LANES] = jnp.where(
                at == target_of(b, 2 * i + h), 1.0, 0.0
            ).astype(jnp.bfloat16)

    def place_of(i):
        return i if keep else 0

    def out_copy(b, k):
        return pltpu.make_async_remote_copy(
            src_ref=outgoing.at[b, k],
            dst_ref=arrived.at[b, k],
            send_sem=out_send.at[b, k],
            recv_sem=out_recv.at[b, k],
            device_id=(z, lax.rem(w + k, W)),
            device_id_type=MESH,
        )

    def back_copy(b, k):
        return pltpu.make_async_remote_copy(
            src_ref=solved.at[b, k],
            dst_ref=returned.at[b, k],
            send_sem=back_send.at[b, k],
            recv_sem=back_recv.at[b, k],
            device_id=(z, lax.rem(w + W - k, W)),
            device_id_type=MESH,
        )

    def send_block(b):
        def send(i, carry):
            build(b, i, place_of(i))
            message = jnp.dot(
                right[...], pick[b, place_of(i)], preferred_element_type=jnp.float32
            ).astype(jnp.bfloat16)
            k0, k1 = 2 * i, 2 * i + 1
            outgoing[b, k0] = message[:, :LANES]
            outgoing[b, k1] = message[:, LANES:]

            @pl.when(i > 0)
            def _():
                out_copy(b, k0).start()

            out_copy(b, k1).start()
            return carry

        lax.fori_loop(0, W // 2, send, 0)
        arrived[b, 0] = outgoing[b, 0]

    def wait_block(b):
        def wait_out(k, carry):
            out_copy(b, k).wait_recv()
            return carry

        lax.fori_loop(1, W, wait_out, 0)

    with scope("send0"):
        send_block(0)
    with scope("relay_b"):
        for c in range(1, pairs):
            relay((1, c), (2, c))
    with scope("send1"):
        send_block(1)
    with scope("relay_c"):
        relay((3, pairs), (3, 0))

    def low_values():
        rows = []
        for t in range(Z):
            row = low_table[groups[t], pl.ds(w, 1), :]
            for j in range(pairs):
                rows.append(jnp.where(lane_pair == j, row, -1).astype(jnp.float32))
        return jnp.max(jnp.concatenate(rows, axis=0), axis=1, keepdims=True).astype(jnp.int32)

    low_column = low_values()

    def low_at(t, j):
        return low_column[t * pairs + j : t * pairs + j + 1, :]

    def twice(row):
        return jnp.concatenate([row, row], axis=1)

    wide_pair = twice(lane_pair)
    wide_member = twice(lane_member)
    wide_spare = twice(spare)
    wide_extra = twice(jnp.logical_or(spare, is_moved))

    def fill_rest(t):
        g = groups[t]
        for i in range(2 * pairs):
            piece = rest[g].astype(jnp.float32)[:, i * tail : (i + 1) * tail]
            matrices[g, i, :, LANES:levels] = piece.astype(jnp.bfloat16)

    def columns(buffer, b, i, count):
        return jnp.concatenate(
            [buffer[b, 2 * i, 0:count, :], buffer[b, 2 * i + 1, 0:count, :]], axis=1
        )

    def store(b, i, y):
        y = y.astype(jnp.bfloat16)
        solved[b, 2 * i] = y[:, :LANES]
        solved[b, 2 * i + 1] = y[:, LANES:]

    def source_orders(i):
        s0 = lax.rem(w + W - 2 * i, W)
        s1 = lax.rem(w + W - 2 * i - 1, W)
        return jnp.concatenate([info[s0][1:2], info[s1][1:2]], axis=1)

    def times(t, j, member, x):
        return jnp.dot(
            matrices[groups[t], 2 * j + member], x, preferred_element_type=jnp.float32
        )

    rows = solved.shape[2]

    def regular(b, t, j, m, x, y):
        own = wide_pair == (t - 2 * b) * pairs + j
        low = low_at(t, j)
        if b == 1:
            extra = jnp.logical_and(wide_extra, m == low)
            own = jnp.logical_and(own, jnp.logical_not(wide_extra))
        use_low = jnp.logical_and(jnp.logical_and(own, wide_member == 0), m <= low)
        use_high = jnp.logical_or(own, extra) if b == 1 else own
        lower = times(t, j, 0, x)
        upper = times(t, j, 1, x)
        return jnp.where(use_low, lower, jnp.where(use_high, upper, y))

    def near(i, carry):
        m = source_orders(i)
        x = columns(arrived, 0, i, levels)
        y = jnp.zeros((rows, 2 * LANES), jnp.float32)
        for t in range(2):
            for j in range(pairs):
                y = regular(0, t, j, m, x, y)
        store(0, i, y)
        return carry

    def send_back(b, i):
        @pl.when(i > 0)
        def _():
            back_copy(b, 2 * i).start()

        back_copy(b, 2 * i + 1).start()

    def turn(i, carry):
        m = source_orders(i)
        x = columns(arrived, 1, i, levels)
        y = jnp.zeros((rows, 2 * LANES), jnp.float32)
        for t in range(2):
            for j in range(pairs):
                extra = jnp.logical_and(wide_extra, m == low_at(t, j))
                y = jnp.where(extra, times(t, j, 1, x), y)
        y = regular(1, 2, 0, m, x, y)
        store(1, i, y)
        y = columns(solved, 0, i, rows).astype(jnp.float32)
        y = jnp.where(wide_spare, times(2, 0, 1, columns(arrived, 0, i, levels)), y)
        store(0, i, y)
        send_back(0, i)
        return carry

    def late(steps, last):
        def body(i, carry):
            m = source_orders(i)
            x = columns(arrived, 1, i, levels)
            y = columns(solved, 1, i, rows).astype(jnp.float32)
            for t, j in steps:
                y = regular(1, t, j, m, x, y)
            store(1, i, y)
            if last:
                send_back(1, i)
            return carry

        lax.fori_loop(0, W // 2, body, 0)

    with scope("wait0"):
        wait_block(0)
        arrive((1, pairs), *[(1, c) for c in range(pairs)])
    fill_rest(1)
    with scope("near"):
        lax.fori_loop(0, W // 2, near, 0)
    with scope("relay_d"):
        relay(*[(3, c) for c in range(1, pairs)])
    with scope("wait1"):
        wait_block(1)
    with scope("arrive2"):
        arrive((2, pairs), (2, 0))
    fill_rest(2)
    with scope("turn"):
        lax.fori_loop(0, W // 2, turn, 0)
    with scope("arrive2b"):
        arrive(*[(2, c) for c in range(1, pairs)])
    with scope("late2"):
        late([(2, j) for j in range(1, pairs)], False)
    with scope("arrive3"):
        arrive((3, pairs), *[(3, c) for c in range(pairs - 1)])
    fill_rest(3)
    with scope("late3"):
        late([(3, j) for j in range(pairs - 1)], False)
    with scope("arrive3b"):
        arrive((3, pairs - 1))
    with scope("late3b"):
        late([(3, pairs - 1)], True)

    total[...] = jnp.zeros_like(total)
    through_row = lax.broadcasted_iota(jnp.int32, (tail, levels), 0)
    through_lane = lax.broadcasted_iota(jnp.int32, (tail, levels), 1)
    response = jnp.concatenate(
        [
            jnp.where(through_lane == through_row + LANES, -1.0, 0.0),
            thermal_response[...].astype(jnp.float32),
            mass_row[...].astype(jnp.float32).reshape(1, levels),
        ],
        axis=0,
    ).astype(jnp.bfloat16)

    def collect(b, i, first, second):
        if not keep:
            build(b, i, 0)
        total[...] += lax.dot_general(
            jnp.concatenate([first, second], axis=1),
            pick[b, place_of(i)],
            (((1,), (1,)), ((), ())),
            preferred_element_type=jnp.float32,
        )

    def gather_back(b):
        with scope(f"back{b}_0"):
            back_copy(b, 1).wait_recv()
            collect(b, 0, solved[b, 0], returned[b, 1])

        def step(i, carry):
            back_copy(b, 2 * i).wait_recv()
            back_copy(b, 2 * i + 1).wait_recv()
            collect(b, i, returned[b, 2 * i], returned[b, 2 * i + 1])
            return carry

        with scope(f"back{b}"):
            lax.fori_loop(1, W // 2, step, 0)

    gather_back(0)
    gather_back(1)

    with scope("final"):
        div = total[0:levels, :].astype(jnp.bfloat16)
        change = jnp.dot(response, div, preferred_element_type=jnp.float32)
        old = state[LANES:, :].astype(jnp.float32)
        below = lax.broadcasted_iota(jnp.int32, old.shape, 0) < tail
        new = jnp.where(below, 0.0, old) - change
        new = jnp.where(column_order >= 0, new, 0.0)
        out[0:LANES, :] = div[0:LANES, :]
        out[LANES:, :] = new.astype(jnp.bfloat16)

    def drain(k, carry):
        for b in range(2):
            out_copy(b, k).wait_send()
            back_copy(b, k).wait_send()
        return carry

    lax.fori_loop(1, W, drain, 0)
    for i in range(stages):
        info_copy(i, block_start(w, i)).wait_send()
    for k in range(1, Z):
        table_copy(k).wait_send()
    for g in range(Z):
        for c in range(pairs + 1):

            @pl.when(jnp.logical_and(g <= z, z < Z - 1))
            def _():
                z_copy(g, c, 0).wait_send()

            @pl.when(jnp.logical_and(g >= z, z > 0))
            def _():
                z_copy(g, c, 1).wait_send()


def shards(
    state,
    held_orders,
    pair_lows,
    inverses,
    height_operator,
    pressure_column,
    thermal_response_matrix,
    mass_row,
):
    levels = height_operator.shape[0]
    slots = held_orders.shape[0]
    pairs = pair_lows.shape[0]
    Z, W = lax.axis_size("grp"), lax.axis_size("wave")
    width = state.shape[1]
    rows = ceil_to(levels, ROWS_TILE)
    places = W // 2 if W * width * 4 * LANES <= KEEP_BYTES else 1
    stages = W.bit_length() - 1
    vmem = pl.BlockSpec(memory_space=pltpu.VMEM)
    smem = pl.BlockSpec(memory_space=pltpu.SMEM)
    block = pltpu.VMEM((2, W, rows, LANES), jnp.bfloat16)
    return pl.pallas_call(
        functools.partial(kernel, (Z, W, levels, slots, pairs)),
        out_shape=jax.ShapeDtypeStruct(state.shape, jnp.bfloat16),
        in_specs=[smem, smem, pl.BlockSpec(memory_space=pl.ANY)] + [vmem] * 5,
        out_specs=vmem,
        scratch_shapes=[
            pltpu.VMEM(state.shape, jnp.bfloat16),
            pltpu.VMEM((W, TABLE_ROWS, LANES), jnp.int32),
            pltpu.VMEM((Z, W, LANES), jnp.int32),
            pltpu.VMEM((Z, 2 * pairs, rows, levels), jnp.bfloat16),
            pltpu.VMEM((Z, rows, LANES), jnp.bfloat16),
            pltpu.VMEM((rows, width), jnp.bfloat16),
            pltpu.VMEM((2, places, width, 2 * LANES), jnp.bfloat16),
            block,
            block,
            block,
            block,
            pltpu.VMEM((rows, width), jnp.float32),
            pltpu.SemaphoreType.DMA((stages,)),
            pltpu.SemaphoreType.DMA((stages,)),
            pltpu.SemaphoreType.DMA((Z,)),
            pltpu.SemaphoreType.DMA((Z,)),
            pltpu.SemaphoreType.DMA((Z, pairs + 1, 2)),
            pltpu.SemaphoreType.DMA((Z, pairs + 1)),
            pltpu.SemaphoreType.DMA((2, W)),
            pltpu.SemaphoreType.DMA((2, W)),
            pltpu.SemaphoreType.DMA((2, W)),
            pltpu.SemaphoreType.DMA((2, W)),
            pltpu.SemaphoreType.DMA,
        ],
        compiler_params=pltpu.CompilerParams(
            collective_id=0, has_side_effects=True, vmem_limit_bytes=60 * 1024 * 1024
        ),
    )(
        held_orders,
        pair_lows,
        state,
        inverses.reshape(2 * pairs, levels, levels),
        height_operator,
        pressure_column,
        thermal_response_matrix,
        mass_row,
    )


def solution(mesh):
    placed = (
        P(None, ("grp", "wave")),
        P(("grp", "wave")),
        P(("grp", "wave")),
        P(("grp", "wave"), None, None, None),
        P(),
        P(),
        P(),
        P(),
    )
    return jax.shard_map(
        shards, mesh=mesh, in_specs=placed, out_specs=P(None, ("grp", "wave")), check_vma=False
    )
```

```python
import functools

import jax
import jax.numpy as jnp
from jax import lax
from jax.experimental import pallas as pl
from jax.experimental.pallas import tpu as pltpu
from jax.sharding import PartitionSpec as P

MESH = pl.DeviceIdType.MESH
LANES = 128
ROWS_TILE = 16
TABLE_ROWS = 8
KEEP_BYTES = 24 << 20
scope = jax.named_scope


def ceil_to(value, step):
    return -(-value // step) * step


def kernel(
    size,
    held_far,
    lows_far,
    state_far,
    inverses_far,
    height_far,
    pressure_far,
    thermal_far,
    mass_far,
    out,
    held,
    lows,
    state,
    inverses,
    height_operator,
    pressure_column,
    thermal_response,
    mass_row,
    low_rows,
    info,
    matrices,
    rest,
    right,
    pick,
    outgoing,
    arrived,
    solved,
    returned,
    total,
    row_send,
    row_recv,
    info_send,
    info_recv,
    z_send,
    z_recv,
    out_send,
    out_recv,
    back_send,
    back_recv,
    fetch_sem,
):
    Z, W, levels, slots, pairs = size
    half_count = Z * W * pairs
    truncation = 2 * half_count - 1
    slot_width = 2 * (truncation + 2)
    width = slots * slot_width
    denom = float(truncation * (truncation + 1))
    per_pair = 4 * slots
    block_pairs = 2 * pairs
    first_extra = block_pairs * per_pair
    moved = per_pair - 2
    last_slot = slots - 1
    tail = levels - LANES
    keep = pick.shape[1] > 1
    z = lax.axis_index("grp")
    w = lax.axis_index("wave")
    middle = jnp.logical_and(z > 0, z < Z - 1)

    barrier = pltpu.get_barrier_semaphore()

    def greet(k, carry):
        pl.semaphore_signal(
            barrier, inc=1, device_id=(z, lax.rem(w + k, W)), device_id_type=MESH
        )
        return carry

    fetches = [
        pltpu.make_async_copy(far, near, fetch_sem.at[i])
        for i, (far, near) in enumerate(
            [
                (lows_far, lows),
                (held_far, held),
                (inverses_far, inverses),
                (state_far, state),
                (height_far, height_operator),
                (pressure_far, pressure_column),
                (thermal_far, thermal_response),
                (mass_far, mass_row),
            ]
        )
    ]
    for k in range(1, Z):
        pl.semaphore_signal(barrier, inc=1, device_id=(lax.rem(z + k, Z), w), device_id_type=MESH)
    for fetch in fetches[:3]:
        fetch.start()
    lax.fori_loop(1, W, greet, 0)
    for fetch in fetches[3:]:
        fetch.start()

    lane = lax.broadcasted_iota(jnp.int32, (1, LANES), 1)
    lane_pair = lane // per_pair
    lane_member = lax.rem(lane, per_pair) // (2 * slots)
    lane_slot = lax.rem(lax.rem(lane, per_pair), 2 * slots) // 2
    lane_part = lax.rem(lane, 2)
    spare = lane >= first_extra
    is_moved = jnp.logical_and(lane >= moved, lane < moved + 2)
    with scope("small_fetch"):
        fetches[0].wait()
        fetches[1].wait()
    orders = jnp.full((1, LANES), -1, jnp.int32)
    for s in range(slots):
        orders = jnp.where(lane_slot == s, held[s], orders)
    low_row = jnp.zeros((1, LANES), jnp.int32)
    for j in range(pairs):
        low_row = jnp.where(lax.rem(lane_pair, pairs) == j, lows[j], low_row)
    low_rows[z] = jnp.broadcast_to(low_row, (TABLE_ROWS, LANES))

    with scope("inverse_fetch"):
        fetches[2].wait()
    rows = matrices.shape[2]
    with scope("split"):
        to_row = lax.broadcasted_iota(jnp.int32, (2 * rows, 2 * levels), 0)
        from_row = lax.broadcasted_iota(jnp.int32, (2 * rows, 2 * levels), 1)
        wanted = jnp.where(to_row < rows, 2 * to_row, 2 * (to_row - rows) + 1)
        split = jnp.where(wanted == from_row, 1.0, 0.0).astype(jnp.bfloat16)
        ends = []
        for j in range(pairs):
            both = jnp.dot(
                split,
                inverses[j].reshape(2 * levels, levels),
                preferred_element_type=jnp.float32,
            )
            for member in range(2):
                matrix = both[member * rows : (member + 1) * rows]
                matrices[z, 2 * j + member] = matrix.astype(jnp.bfloat16)
                ends.append(matrix[:, LANES:levels])
        rest[z, :, 0 : 2 * pairs * tail] = jnp.concatenate(ends, axis=1).astype(jnp.bfloat16)

    with scope("barrier"):
        pl.semaphore_wait(barrier, W + Z - 2)

    def z_copy(g, c, way):
        if c < pairs:
            ref = matrices.at[g, pl.ds(2 * c, 2), :, pl.ds(0, LANES)]
        else:
            ref = rest.at[g]
        step = 1 if way == 0 else -1
        return pltpu.make_async_remote_copy(
            src_ref=ref,
            dst_ref=ref,
            send_sem=z_send.at[g, c, way],
            recv_sem=z_recv.at[g, c],
            device_id=(z + step, w),
            device_id_type=MESH,
        )

    def forward(g, c):
        @pl.when(jnp.logical_and(g <= z, z < Z - 1))
        def _():
            z_copy(g, c, 0).start()

        @pl.when(jnp.logical_and(g >= z, z > 0))
        def _():
            z_copy(g, c, 1).start()

    def group_at(t):
        g = z
        for zz in range(Z):
            by_distance = sorted(range(Z), key=lambda a: abs(a - zz))
            g = jnp.where(z == zz, by_distance[t], g)
        return g

    def relay(*steps):
        @pl.when(middle)
        def _():
            for t, c in steps:
                g = group_at(t)
                z_copy(g, c, 0).wait_recv()
                forward(g, c)

    def arrive(*steps):
        @pl.when(jnp.logical_not(middle))
        def _():
            for t, c in steps:
                z_copy(group_at(t), c, 0).wait_recv()

    def row_copy(k):
        return pltpu.make_async_remote_copy(
            src_ref=low_rows.at[z],
            dst_ref=low_rows.at[z],
            send_sem=row_send.at[k],
            recv_sem=row_recv.at[k],
            device_id=(lax.rem(z + k, Z), w),
            device_id_type=MESH,
        )

    def row_arrival(k):
        source = lax.rem(z + Z - k, Z)
        return pltpu.make_async_remote_copy(
            src_ref=low_rows.at[source],
            dst_ref=low_rows.at[source],
            send_sem=row_send.at[k],
            recv_sem=row_recv.at[k],
            device_id=(source, w),
            device_id_type=MESH,
        )

    def info_copy(k):
        return pltpu.make_async_remote_copy(
            src_ref=info.at[w],
            dst_ref=info.at[w],
            send_sem=info_send.at[k],
            recv_sem=info_recv.at[k],
            device_id=(z, lax.rem(w + k, W)),
            device_id_type=MESH,
        )

    def info_arrival(k):
        source = lax.rem(w + W - k, W)
        return pltpu.make_async_remote_copy(
            src_ref=info.at[source],
            dst_ref=info.at[source],
            send_sem=info_send.at[k],
            recv_sem=info_recv.at[k],
            device_id=(z, source),
            device_id_type=MESH,
        )

    for k in range(1, Z):
        row_copy(k).start()
    for c in [pairs, *range(pairs)]:
        forward(z, c)

    column = lax.broadcasted_iota(jnp.int32, (1, width), 1)
    column_order = jnp.full((1, width), -1, jnp.int32)
    column_start = jnp.zeros((1, width), jnp.int32)
    for s in range(slots):
        inside = jnp.logical_and(column >= s * slot_width, column < (s + 1) * slot_width)
        column_order = jnp.where(inside, held[s], column_order)
        column_start = jnp.where(inside, s * slot_width, column_start)

    def drive_right():
        coefficient = (column - column_start) // 2
        degree = jnp.where(
            coefficient <= truncation - column_order, column_order + coefficient, coefficient - 1
        )
        lap_scale = (degree * (degree + 1)).astype(jnp.float32) / denom
        fetches[4].wait()
        fetches[5].wait()
        height = height_operator[...].astype(jnp.float32)
        pressure_row = jnp.broadcast_to(
            pressure_column[...].astype(jnp.float32).reshape(1, levels), height.shape
        )
        across = lax.broadcasted_iota(jnp.int32, height.shape, 1)
        down = lax.broadcasted_iota(jnp.int32, height.shape, 0)
        pressure_side = jnp.sum(
            jnp.where(across == down, pressure_row, 0.0), axis=1, keepdims=True
        )
        height = jnp.concatenate(
            [jnp.zeros((levels, tail), jnp.float32), height, pressure_side], axis=1
        ).astype(jnp.bfloat16)
        fetches[3].wait()
        drive = jnp.dot(height, state[LANES:, :], preferred_element_type=jnp.float32)
        right[0:levels, :] = (
            state[0:levels, :].astype(jnp.float32) + lap_scale * drive
        ).astype(jnp.bfloat16)

    with scope("rows_wait"):
        for k in range(1, Z):
            row_arrival(k).wait_recv()
    table = [low_rows[g][0:1] for g in range(Z)]
    table += [jnp.broadcast_to(orders, (TABLE_ROWS - Z, LANES))]
    info[w] = jnp.concatenate(table, axis=0)

    def start_info(k, carry):
        info_copy(k).start()
        return carry

    lax.fori_loop(1, W, start_info, 0)
    with scope("drive"):
        drive_right()

    def wait_info(k, carry):
        info_arrival(k).wait_recv()
        return carry

    with scope("info_wait"):
        lax.fori_loop(1, W, wait_info, 0)

    groups = [group_at(t) for t in range(Z)]

    def target_of(b, k):
        d = lax.rem(w + k, W)
        rows = [info[d, pl.ds(groups[t], 1), :] for t in range(Z)]
        low = jnp.where(lane < pairs * per_pair, rows[2 * b], rows[2 * b + 1])
        slot, member, order = lane_slot, lane_member, orders
        if b == 0:
            low = jnp.where(spare, rows[2], low)
            slot = jnp.where(spare, last_slot, slot)
            member = jnp.where(spare, 1, member)
            order = jnp.where(spare, held[last_slot], order)
        merged = jnp.where(order <= low, low - order, truncation + 1 - low)
        position = jnp.where(member == 0, merged, truncation - low - order)
        used = order >= 0
        if b == 0:
            used = jnp.logical_and(used, lane < first_extra + 2)
        else:
            extra = jnp.logical_or(spare, is_moved)
            position = jnp.where(extra, truncation + 1 - order, position)
        target = slot * slot_width + 2 * position + lane_part
        return jnp.where(used, target, -1)

    def build(b, i, place):
        at = lax.broadcasted_iota(jnp.int32, (width, LANES), 0)
        for h in range(2):
            pick[b, place, :, h * LANES : (h + 1) * LANES] = jnp.where(
                at == target_of(b, 2 * i + h), 1.0, 0.0
            ).astype(jnp.bfloat16)

    def place_of(i):
        return i if keep else 0

    def out_copy(b, k):
        return pltpu.make_async_remote_copy(
            src_ref=outgoing.at[b, k],
            dst_ref=arrived.at[b, k],
            send_sem=out_send.at[b, k],
            recv_sem=out_recv.at[b, k],
            device_id=(z, lax.rem(w + k, W)),
            device_id_type=MESH,
        )

    def back_copy(b, k):
        return pltpu.make_async_remote_copy(
            src_ref=solved.at[b, k],
            dst_ref=returned.at[b, k],
            send_sem=back_send.at[b, k],
            recv_sem=back_recv.at[b, k],
            device_id=(z, lax.rem(w + W - k, W)),
            device_id_type=MESH,
        )

    def send_block(b):
        def send(i, carry):
            build(b, i, place_of(i))
            message = jnp.dot(
                right[...], pick[b, place_of(i)], preferred_element_type=jnp.float32
            ).astype(jnp.bfloat16)
            k0, k1 = 2 * i, 2 * i + 1
            outgoing[b, k0] = message[:, :LANES]
            outgoing[b, k1] = message[:, LANES:]

            @pl.when(i > 0)
            def _():
                out_copy(b, k0).start()

            out_copy(b, k1).start()
            return carry

        lax.fori_loop(0, W // 2, send, 0)
        arrived[b, 0] = outgoing[b, 0]

    def wait_block(b):
        def wait_out(k, carry):
            out_copy(b, k).wait_recv()
            return carry

        lax.fori_loop(1, W, wait_out, 0)

    with scope("relay_a"):
        relay((1, pairs), (2, pairs), (1, 0), (2, 0))
    with scope("send0"):
        send_block(0)
    with scope("relay_b"):
        for c in range(1, pairs):
            relay((1, c), (2, c))
    with scope("send1"):
        send_block(1)
    with scope("relay_c"):
        relay((3, pairs), (3, 0))

    def low_values():
        rows = []
        for t in range(Z):
            row = info[w, pl.ds(groups[t], 1), :]
            for j in range(pairs):
                rows.append(jnp.where(lane_pair == j, row, -1).astype(jnp.float32))
        return jnp.max(jnp.concatenate(rows, axis=0), axis=1, keepdims=True).astype(jnp.int32)

    low_column = low_values()

    def low_at(t, j):
        return low_column[t * pairs + j : t * pairs + j + 1, :]

    def twice(row):
        return jnp.concatenate([row, row], axis=1)

    wide_pair = twice(lane_pair)
    wide_member = twice(lane_member)
    wide_spare = twice(spare)
    wide_extra = twice(jnp.logical_or(spare, is_moved))

    def fill_rest(t):
        g = groups[t]
        for i in range(2 * pairs):
            piece = rest[g].astype(jnp.float32)[:, i * tail : (i + 1) * tail]
            matrices[g, i, :, LANES:levels] = piece.astype(jnp.bfloat16)

    def columns(buffer, b, i, count):
        return jnp.concatenate(
            [buffer[b, 2 * i, 0:count, :], buffer[b, 2 * i + 1, 0:count, :]], axis=1
        )

    def store(b, i, y):
        y = y.astype(jnp.bfloat16)
        solved[b, 2 * i] = y[:, :LANES]
        solved[b, 2 * i + 1] = y[:, LANES:]

    def source_orders(i):
        s0 = lax.rem(w + W - 2 * i, W)
        s1 = lax.rem(w + W - 2 * i - 1, W)
        return jnp.concatenate([info[s0][Z : Z + 1], info[s1][Z : Z + 1]], axis=1)

    def times(t, j, member, x):
        return jnp.dot(
            matrices[groups[t], 2 * j + member], x, preferred_element_type=jnp.float32
        )

    def regular(b, t, j, m, x, y):
        own = wide_pair == (t - 2 * b) * pairs + j
        low = low_at(t, j)
        if b == 1:
            extra = jnp.logical_and(wide_extra, m == low)
            own = jnp.logical_and(own, jnp.logical_not(wide_extra))
        use_low = jnp.logical_and(jnp.logical_and(own, wide_member == 0), m <= low)
        use_high = jnp.logical_or(own, extra) if b == 1 else own
        lower = times(t, j, 0, x)
        upper = times(t, j, 1, x)
        return jnp.where(use_low, lower, jnp.where(use_high, upper, y))

    def near(i, carry):
        m = source_orders(i)
        x = columns(arrived, 0, i, levels)
        y = jnp.zeros((rows, 2 * LANES), jnp.float32)
        for t in range(2):
            for j in range(pairs):
                y = regular(0, t, j, m, x, y)
        store(0, i, y)
        return carry

    def send_back(b, i):
        @pl.when(i > 0)
        def _():
            back_copy(b, 2 * i).start()

        back_copy(b, 2 * i + 1).start()

    def turn(i, carry):
        m = source_orders(i)
        x = columns(arrived, 1, i, levels)
        y = jnp.zeros((rows, 2 * LANES), jnp.float32)
        for t in range(2):
            for j in range(pairs):
                extra = jnp.logical_and(wide_extra, m == low_at(t, j))
                y = jnp.where(extra, times(t, j, 1, x), y)
        y = regular(1, 2, 0, m, x, y)
        store(1, i, y)
        y = columns(solved, 0, i, rows).astype(jnp.float32)
        y = jnp.where(wide_spare, times(2, 0, 1, columns(arrived, 0, i, levels)), y)
        store(0, i, y)
        send_back(0, i)
        return carry

    def late(steps, last):
        def body(i, carry):
            m = source_orders(i)
            x = columns(arrived, 1, i, levels)
            y = columns(solved, 1, i, rows).astype(jnp.float32)
            for t, j in steps:
                y = regular(1, t, j, m, x, y)
            store(1, i, y)
            if last:
                send_back(1, i)
            return carry

        lax.fori_loop(0, W // 2, body, 0)

    with scope("wait0"):
        wait_block(0)
        arrive((1, pairs), *[(1, c) for c in range(pairs)])
    fill_rest(1)
    with scope("near"):
        lax.fori_loop(0, W // 2, near, 0)
    with scope("relay_d"):
        relay(*[(3, c) for c in range(1, pairs)])
    with scope("wait1"):
        wait_block(1)
    with scope("arrive2"):
        arrive((2, pairs), (2, 0))
    fill_rest(2)
    with scope("turn"):
        lax.fori_loop(0, W // 2, turn, 0)
    with scope("arrive2b"):
        arrive(*[(2, c) for c in range(1, pairs)])
    with scope("late2"):
        late([(2, j) for j in range(1, pairs)], False)
    with scope("arrive3"):
        arrive((3, pairs), *[(3, c) for c in range(pairs - 1)])
    fill_rest(3)
    with scope("late3"):
        late([(3, j) for j in range(pairs - 1)], False)
    with scope("arrive3b"):
        arrive((3, pairs - 1))
    with scope("late3b"):
        late([(3, pairs - 1)], True)

    fetches[6].wait()
    fetches[7].wait()
    total[...] = jnp.zeros_like(total)
    through_row = lax.broadcasted_iota(jnp.int32, (tail, levels), 0)
    through_lane = lax.broadcasted_iota(jnp.int32, (tail, levels), 1)
    response = jnp.concatenate(
        [
            jnp.where(through_lane == through_row + LANES, -1.0, 0.0),
            thermal_response[...].astype(jnp.float32),
            mass_row[...].astype(jnp.float32).reshape(1, levels),
        ],
        axis=0,
    ).astype(jnp.bfloat16)

    def collect(b, i, first, second):
        if not keep:
            build(b, i, 0)
        total[...] += lax.dot_general(
            jnp.concatenate([first, second], axis=1),
            pick[b, place_of(i)],
            (((1,), (1,)), ((), ())),
            preferred_element_type=jnp.float32,
        )

    def gather_back(b):
        with scope(f"back{b}_0"):
            back_copy(b, 1).wait_recv()
            collect(b, 0, solved[b, 0], returned[b, 1])

        def step(i, carry):
            back_copy(b, 2 * i).wait_recv()
            back_copy(b, 2 * i + 1).wait_recv()
            collect(b, i, returned[b, 2 * i], returned[b, 2 * i + 1])
            return carry

        with scope(f"back{b}"):
            lax.fori_loop(1, W // 2, step, 0)

    gather_back(0)
    gather_back(1)

    with scope("final"):
        div = total[0:levels, :].astype(jnp.bfloat16)
        change = jnp.dot(response, div, preferred_element_type=jnp.float32)
        old = state[LANES:, :].astype(jnp.float32)
        below = lax.broadcasted_iota(jnp.int32, old.shape, 0) < tail
        new = jnp.where(below, 0.0, old) - change
        new = jnp.where(column_order >= 0, new, 0.0)
        out[0:LANES, :] = div[0:LANES, :]
        out[LANES:, :] = new.astype(jnp.bfloat16)

    def drain(k, carry):
        for b in range(2):
            out_copy(b, k).wait_send()
            back_copy(b, k).wait_send()
        return carry

    lax.fori_loop(1, W, drain, 0)
    for k in range(1, Z):
        row_copy(k).wait_send()

    def drain_info(k, carry):
        info_copy(k).wait_send()
        return carry

    lax.fori_loop(1, W, drain_info, 0)
    for g in range(Z):
        for c in range(pairs + 1):

            @pl.when(jnp.logical_and(g <= z, z < Z - 1))
            def _():
                z_copy(g, c, 0).wait_send()

            @pl.when(jnp.logical_and(g >= z, z > 0))
            def _():
                z_copy(g, c, 1).wait_send()


def shards(
    state,
    held_orders,
    pair_lows,
    inverses,
    height_operator,
    pressure_column,
    thermal_response_matrix,
    mass_row,
):
    levels = height_operator.shape[0]
    slots = held_orders.shape[0]
    pairs = pair_lows.shape[0]
    Z, W = lax.axis_size("grp"), lax.axis_size("wave")
    width = state.shape[1]
    rows = ceil_to(levels, ROWS_TILE)
    places = W // 2 if W * width * 4 * LANES <= KEEP_BYTES else 1
    block = pltpu.VMEM((2, W, rows, LANES), jnp.bfloat16)
    return pl.pallas_call(
        functools.partial(kernel, (Z, W, levels, slots, pairs)),
        out_shape=jax.ShapeDtypeStruct(state.shape, jnp.bfloat16),
        in_specs=[pl.BlockSpec(memory_space=pl.ANY)] * 8,
        out_specs=pl.BlockSpec(memory_space=pltpu.VMEM),
        scratch_shapes=[
            pltpu.SMEM(held_orders.shape, jnp.int32),
            pltpu.SMEM(pair_lows.shape, jnp.int32),
            pltpu.VMEM(state.shape, jnp.bfloat16),
            pltpu.VMEM((pairs, levels, 2, levels), jnp.bfloat16),
            pltpu.VMEM(height_operator.shape, jnp.bfloat16),
            pltpu.VMEM(pressure_column.shape, jnp.bfloat16),
            pltpu.VMEM(thermal_response_matrix.shape, jnp.bfloat16),
            pltpu.VMEM(mass_row.shape, jnp.bfloat16),
            pltpu.VMEM((Z, TABLE_ROWS, LANES), jnp.int32),
            pltpu.VMEM((W, TABLE_ROWS, LANES), jnp.int32),
            pltpu.VMEM((Z, 2 * pairs, rows, levels), jnp.bfloat16),
            pltpu.VMEM((Z, rows, LANES), jnp.bfloat16),
            pltpu.VMEM((rows, width), jnp.bfloat16),
            pltpu.VMEM((2, places, width, 2 * LANES), jnp.bfloat16),
            block,
            block,
            block,
            block,
            pltpu.VMEM((rows, width), jnp.float32),
            pltpu.SemaphoreType.DMA((Z,)),
            pltpu.SemaphoreType.DMA((Z,)),
            pltpu.SemaphoreType.DMA((W,)),
            pltpu.SemaphoreType.DMA((W,)),
            pltpu.SemaphoreType.DMA((Z, pairs + 1, 2)),
            pltpu.SemaphoreType.DMA((Z, pairs + 1)),
            pltpu.SemaphoreType.DMA((2, W)),
            pltpu.SemaphoreType.DMA((2, W)),
            pltpu.SemaphoreType.DMA((2, W)),
            pltpu.SemaphoreType.DMA((2, W)),
            pltpu.SemaphoreType.DMA((8,)),
        ],
        compiler_params=pltpu.CompilerParams(
            collective_id=0, has_side_effects=True, vmem_limit_bytes=60 * 1024 * 1024
        ),
    )(
        held_orders,
        pair_lows,
        state,
        jnp.transpose(inverses, (0, 2, 1, 3)),
        height_operator,
        pressure_column,
        thermal_response_matrix,
        mass_row,
    )


def solution(mesh):
    placed = (
        P(None, ("grp", "wave")),
        P(("grp", "wave")),
        P(("grp", "wave")),
        P(("grp", "wave"), None, None, None),
        P(),
        P(),
        P(),
        P(),
    )
    return jax.shard_map(
        shards, mesh=mesh, in_specs=placed, out_specs=P(None, ("grp", "wave")), check_vma=False
    )
```

```python
import functools

import jax
import jax.numpy as jnp
from jax import lax
from jax.experimental import pallas as pl
from jax.experimental.pallas import tpu as pltpu
from jax.sharding import PartitionSpec as P

MESH = pl.DeviceIdType.MESH
LANES = 128
ROWS_TILE = 16
TABLE_ROWS = 8
NEAR_ROWS = 16
KEEP_BYTES = 24 << 20
scope = jax.named_scope


def ceil_to(value, step):
    return -(-value // step) * step


def kernel(
    size,
    held_far,
    lows_far,
    state_far,
    inverses_far,
    height_far,
    pressure_far,
    thermal_far,
    mass_far,
    out,
    held,
    lows,
    state,
    inverses,
    height_operator,
    pressure_column,
    thermal_response,
    mass_row,
    low_rows,
    info,
    far_info,
    matrices,
    rest,
    right,
    pick,
    outgoing,
    arrived,
    solved,
    returned,
    packed,
    packed_orders,
    pick_moved,
    pick_extra,
    extra_in,
    extra_out,
    total,
    row_send,
    row_recv,
    info_send,
    info_recv,
    z_send,
    z_recv,
    out_send,
    out_recv,
    back_send,
    back_recv,
    fetch_sem,
):
    Z, W, levels, slots, pairs = size
    half_count = Z * W * pairs
    truncation = 2 * half_count - 1
    slot_width = 2 * (truncation + 2)
    width = slots * slot_width
    denom = float(truncation * (truncation + 1))
    per_pair = 4 * slots
    block_pairs = 2 * pairs
    first_extra = block_pairs * per_pair
    moved = per_pair - 2
    tiles = packed.shape[2] // LANES
    last_slot = slots - 1
    tail = levels - LANES
    keep = pick.shape[1] > 1
    z = lax.axis_index("grp")
    w = lax.axis_index("wave")
    middle = jnp.logical_and(z > 0, z < Z - 1)

    barrier = pltpu.get_barrier_semaphore()

    def greet(k, carry):
        pl.semaphore_signal(
            barrier, inc=1, device_id=(z, lax.rem(w + k, W)), device_id_type=MESH
        )
        return carry

    fetches = [
        pltpu.make_async_copy(far, near, fetch_sem.at[i])
        for i, (far, near) in enumerate(
            [
                (lows_far, lows),
                (held_far, held),
                (inverses_far, inverses),
                (state_far, state),
                (height_far, height_operator),
                (pressure_far, pressure_column),
                (thermal_far, thermal_response),
                (mass_far, mass_row),
            ]
        )
    ]
    for k in range(1, Z):
        pl.semaphore_signal(barrier, inc=1, device_id=(lax.rem(z + k, Z), w), device_id_type=MESH)
    for fetch in fetches[:3]:
        fetch.start()
    lax.fori_loop(1, W, greet, 0)
    for fetch in fetches[3:]:
        fetch.start()

    lane = lax.broadcasted_iota(jnp.int32, (1, LANES), 1)
    lane_pair = lane // per_pair
    lane_member = lax.rem(lane, per_pair) // (2 * slots)
    lane_slot = lax.rem(lax.rem(lane, per_pair), 2 * slots) // 2
    lane_part = lax.rem(lane, 2)
    spare = lane >= first_extra
    table_row = lax.broadcasted_iota(jnp.int32, (TABLE_ROWS, LANES), 0)
    with scope("small_fetch"):
        fetches[0].wait()
        fetches[1].wait()
    orders = jnp.full((1, LANES), -1, jnp.int32)
    for s in range(slots):
        orders = jnp.where(lane_slot == s, held[s], orders)
    low_tile = jnp.zeros((TABLE_ROWS, LANES), jnp.int32)
    for j in range(pairs):
        low_tile = jnp.where(table_row == j, lows[j], low_tile)
    low_rows[z] = low_tile

    rows = matrices.shape[2]

    def split_inverses():
        fetches[2].wait()
        to_row = lax.broadcasted_iota(jnp.int32, (2 * rows, 2 * levels), 0)
        from_row = lax.broadcasted_iota(jnp.int32, (2 * rows, 2 * levels), 1)
        wanted = jnp.where(to_row < rows, 2 * to_row, 2 * (to_row - rows) + 1)
        split = jnp.where(wanted == from_row, 1.0, 0.0).astype(jnp.bfloat16)
        ends = []
        for j in range(pairs):
            both = jnp.dot(
                split,
                inverses[j].reshape(2 * levels, levels),
                preferred_element_type=jnp.float32,
            )
            for member in range(2):
                matrix = both[member * rows : (member + 1) * rows]
                matrices[z, 2 * j + member] = matrix.astype(jnp.bfloat16)
                ends.append(matrix[:, LANES:levels])
        rest[z, :, 0 : 2 * pairs * tail] = jnp.concatenate(ends, axis=1).astype(jnp.bfloat16)

    @pl.when(middle)
    def _():
        with scope("split"):
            split_inverses()

    with scope("barrier"):
        pl.semaphore_wait(barrier, W + Z - 2)

    def z_copy(g, c, way):
        if c < pairs:
            ref = matrices.at[g, pl.ds(2 * c, 2), :, pl.ds(0, LANES)]
        else:
            ref = rest.at[g]
        step = 1 if way == 0 else -1
        return pltpu.make_async_remote_copy(
            src_ref=ref,
            dst_ref=ref,
            send_sem=z_send.at[0 if c < pairs else 1, way],
            recv_sem=z_recv.at[g, c],
            device_id=(z + step, w),
            device_id_type=MESH,
        )

    def forward(g, c):
        @pl.when(jnp.logical_and(g <= z, z < Z - 1))
        def _():
            z_copy(g, c, 0).start()

        @pl.when(jnp.logical_and(g >= z, z > 0))
        def _():
            z_copy(g, c, 1).start()

    def group_at(t):
        g = z
        for zz in range(Z):
            by_distance = sorted(range(Z), key=lambda a: abs(a - zz))
            g = jnp.where(z == zz, by_distance[t], g)
        return g

    def relay_now(*steps):
        for t, c in steps:
            g = group_at(t)
            z_copy(g, c, 0).wait_recv()
            forward(g, c)

    def relay(*steps):
        @pl.when(middle)
        def _():
            relay_now(*steps)

    def arrive(*steps):
        @pl.when(jnp.logical_not(middle))
        def _():
            for t, c in steps:
                z_copy(group_at(t), c, 0).wait_recv()

    groups = [group_at(t) for t in range(Z)]

    def row_copy(k):
        return pltpu.make_async_remote_copy(
            src_ref=low_rows.at[z],
            dst_ref=low_rows.at[z],
            send_sem=row_send,
            recv_sem=row_recv.at[k],
            device_id=(lax.rem(z + k, Z), w),
            device_id_type=MESH,
        )

    def wait_row(g):
        pltpu.make_async_remote_copy(
            src_ref=low_rows.at[g],
            dst_ref=low_rows.at[g],
            send_sem=row_send,
            recv_sem=row_recv.at[lax.rem(z + Z - g, Z)],
            device_id=(g, w),
            device_id_type=MESH,
        ).wait_recv()

    def table_copy(table, b, k):
        return pltpu.make_async_remote_copy(
            src_ref=table.at[w],
            dst_ref=table.at[w],
            send_sem=info_send.at[b],
            recv_sem=info_recv.at[b],
            device_id=(z, lax.rem(w + k, W)),
            device_id_type=MESH,
        )

    def send_table(table, b):
        def start(k, carry):
            table_copy(table, b, k).start()
            return carry

        lax.fori_loop(1, W, start, 0)

    def all_tables(table, b):
        return pltpu.make_async_remote_copy(
            src_ref=table.at[pl.ds(0, W - 1)],
            dst_ref=table.at[pl.ds(0, W - 1)],
            send_sem=info_send.at[b],
            recv_sem=info_recv.at[b],
            device_id=(z, lax.rem(w + 1, W)),
            device_id_type=MESH,
        )

    for k in range(1, Z):
        row_copy(k).start()

    @pl.when(jnp.logical_not(middle))
    def _():
        with scope("split_end"):
            split_inverses()

    for c in [pairs, *range(pairs)]:
        forward(z, c)

    column = lax.broadcasted_iota(jnp.int32, (1, width), 1)
    column_order = jnp.full((1, width), -1, jnp.int32)
    column_start = jnp.zeros((1, width), jnp.int32)
    for s in range(slots):
        inside = jnp.logical_and(column >= s * slot_width, column < (s + 1) * slot_width)
        column_order = jnp.where(inside, held[s], column_order)
        column_start = jnp.where(inside, s * slot_width, column_start)

    def drive_right():
        coefficient = (column - column_start) // 2
        degree = jnp.where(
            coefficient <= truncation - column_order, column_order + coefficient, coefficient - 1
        )
        lap_scale = (degree * (degree + 1)).astype(jnp.float32) / denom
        fetches[4].wait()
        fetches[5].wait()
        height = height_operator[...].astype(jnp.float32)
        pressure_row = jnp.broadcast_to(
            pressure_column[...].astype(jnp.float32).reshape(1, levels), height.shape
        )
        across = lax.broadcasted_iota(jnp.int32, height.shape, 1)
        down = lax.broadcasted_iota(jnp.int32, height.shape, 0)
        pressure_side = jnp.sum(
            jnp.where(across == down, pressure_row, 0.0), axis=1, keepdims=True
        )
        height = jnp.concatenate(
            [jnp.zeros((levels, tail), jnp.float32), height, pressure_side], axis=1
        ).astype(jnp.bfloat16)
        fetches[3].wait()
        drive = jnp.dot(height, state[LANES:, :], preferred_element_type=jnp.float32)
        right[0:levels, :] = (
            state[0:levels, :].astype(jnp.float32) + lap_scale * drive
        ).astype(jnp.bfloat16)

    with scope("drive"):
        drive_right()
    with scope("rows_wait"):
        for t in range(1, 3):
            wait_row(groups[t])
    table = [low_rows[groups[t]][0:pairs] for t in range(3)]
    table += [jnp.broadcast_to(orders, (NEAR_ROWS - 3 * pairs, LANES))]
    info[w] = jnp.concatenate(table, axis=0)
    send_table(info, 0)
    with scope("row_far"):
        wait_row(groups[3])
    far_info[w] = low_rows[groups[3]]
    send_table(far_info, 1)

    @pl.when(middle)
    def _():
        with scope("relay_a"):
            relay_now((1, pairs), (2, pairs), (1, 0), (2, 0))

    with scope("info_wait"):
        all_tables(info, 0).wait_recv()

    def low_of(d, t, j):
        if t < 3:
            return info[d][t * pairs + j : t * pairs + j + 1]
        return far_info[d][j : j + 1]

    def target_of(b, k):
        d = lax.rem(w + k, W)
        pair = lax.rem(lane_pair + block_pairs - lax.rem(k, block_pairs), block_pairs)
        low = jnp.zeros((1, LANES), jnp.int32)
        for p in range(block_pairs):
            low = jnp.where(pair == p, low_of(d, 2 * b + p // pairs, p % pairs), low)
        slot, member, order = lane_slot, lane_member, orders
        if b == 0:
            low = jnp.where(spare, low_of(d, 2, 0), low)
            slot = jnp.where(spare, last_slot, slot)
            member = jnp.where(spare, 1, member)
            order = jnp.where(spare, held[last_slot], order)
        merged = jnp.where(order <= low, low - order, truncation + 1 - low)
        position = jnp.where(member == 0, merged, truncation - low - order)
        used = order >= 0
        if b == 0:
            used = jnp.logical_and(used, lane < first_extra + 2)
        else:
            hole = jnp.logical_and(pair == 0, lax.rem(lane, per_pair) >= moved)
            extra = jnp.logical_or(spare, hole)
            position = jnp.where(extra, truncation + 1 - order, position)
        target = slot * slot_width + 2 * position + lane_part
        return jnp.where(used, target, -1)

    def build(b, i, place):
        at = lax.broadcasted_iota(jnp.int32, (width, LANES), 0)
        for h in range(2):
            pick[b, place, :, h * LANES : (h + 1) * LANES] = jnp.where(
                at == target_of(b, 2 * i + h), 1.0, 0.0
            ).astype(jnp.bfloat16)

    def place_of(i):
        return i if keep else 0

    def out_copy(b, k):
        return pltpu.make_async_remote_copy(
            src_ref=outgoing.at[b, k],
            dst_ref=arrived.at[b, k],
            send_sem=out_send.at[b],
            recv_sem=out_recv.at[b],
            device_id=(z, lax.rem(w + k, W)),
            device_id_type=MESH,
        )

    def back_copy(b, k):
        return pltpu.make_async_remote_copy(
            src_ref=solved.at[b, k],
            dst_ref=returned.at[b, k],
            send_sem=back_send.at[b],
            recv_sem=back_recv.at[b, k // 2],
            device_id=(z, lax.rem(w + W - k, W)),
            device_id_type=MESH,
        )

    def send_block(b):
        def send(i, carry):
            build(b, i, place_of(i))
            message = jnp.dot(
                right[...], pick[b, place_of(i)], preferred_element_type=jnp.float32
            ).astype(jnp.bfloat16)
            k0, k1 = 2 * i, 2 * i + 1
            outgoing[b, k0] = message[:, :LANES]
            outgoing[b, k1] = message[:, LANES:]

            @pl.when(i > 0)
            def _():
                out_copy(b, k0).start()

            out_copy(b, k1).start()
            return carry

        lax.fori_loop(0, W // 2, send, 0)
        arrived[b, 0] = outgoing[b, 0]

    def all_out(b):
        return pltpu.make_async_remote_copy(
            src_ref=outgoing.at[b, pl.ds(1, W - 1)],
            dst_ref=arrived.at[b, pl.ds(1, W - 1)],
            send_sem=out_send.at[b],
            recv_sem=out_recv.at[b],
            device_id=(z, lax.rem(w + 1, W)),
            device_id_type=MESH,
        )

    def some_back(b, first, count):
        return pltpu.make_async_remote_copy(
            src_ref=solved.at[b, pl.ds(first, count)],
            dst_ref=returned.at[b, pl.ds(first, count)],
            send_sem=back_send.at[b],
            recv_sem=back_recv.at[b, first // 2],
            device_id=(z, lax.rem(w + 1, W)),
            device_id_type=MESH,
        )

    with scope("send0"):
        send_block(0)
    with scope("relay_b"):
        for c in range(1, pairs):
            relay((1, c), (2, c))
    with scope("far_wait"):
        all_tables(far_info, 1).wait_recv()
    with scope("send1"):
        send_block(1)
    with scope("relay_c"):
        relay((3, pairs), (3, 0))

    def fill_rest(t):
        g = groups[t]
        for i in range(2 * pairs):
            piece = rest[g].astype(jnp.float32)[:, i * tail : (i + 1) * tail]
            matrices[g, i, :, LANES:levels] = piece.astype(jnp.bfloat16)

    def spread(row):
        return jnp.concatenate([row] * tiles, axis=1)

    source_orders = [
        info[lax.rem(w + W - k, W)][3 * pairs : 3 * pairs + 1] for k in range(W)
    ]

    def place(p, k):
        return lane_pair == (p + k) % block_pairs

    def pack(b, p):
        for v in range(tiles):
            first = v * block_pairs
            columns = arrived[b, first, 0:levels, :]
            order = source_orders[first]
            for k in range(first + 1, min(first + block_pairs, W)):
                columns = jnp.where(place(p, k), arrived[b, k, 0:levels, :], columns)
                order = jnp.where(place(p, k), source_orders[k], order)
            part = slice(v * LANES, (v + 1) * LANES)
            packed[b * block_pairs + p, 0:levels, part] = columns
            if b == 0:
                packed_orders[p : p + 1, part] = order

    wide_member = spread(lane_member)

    def times(t, j, member, x):
        return jnp.dot(
            matrices[groups[t], 2 * j + member], x, preferred_element_type=jnp.float32
        )

    def solve(b, p):
        t, j = 2 * b + p // pairs, p % pairs
        x = packed[b * block_pairs + p, 0:levels, :]
        low = spread(low_of(w, t, j))
        use_low = jnp.logical_and(wide_member == 0, packed_orders[p : p + 1, :] <= low)
        y = jnp.where(use_low, times(t, j, 0, x), times(t, j, 1, x))
        return y.astype(jnp.bfloat16)

    def deal(b, ps, answers, fresh):
        for k in range(W):
            v = k // block_pairs
            parts = [y[:, v * LANES : (v + 1) * LANES] for y in answers]
            block = parts[0] if fresh else solved[b, k]
            for p, part in list(zip(ps, parts))[1 if fresh else 0 :]:
                block = jnp.where(place(p, k), part, block)
            solved[b, k] = block

    def start_back(b):
        for k in range(1, W):
            back_copy(b, k).start()

    def gather_spare(b, chosen):
        columns = jnp.concatenate([arrived[b, k, 0:levels, :] for k in range(W)], axis=1)
        return jnp.dot(columns, chosen[...], preferred_element_type=jnp.float32).astype(
            jnp.bfloat16
        )

    def scatter_spare(b, answer, chosen, where):
        back = lax.dot_general(
            answer, chosen[...], (((1,), (1,)), ((), ())), preferred_element_type=jnp.float32
        ).astype(jnp.bfloat16)
        for k in range(W):
            part = back[:, k * LANES : (k + 1) * LANES]
            solved[b, k] = jnp.where(where(k), part, solved[b, k])

    def is_extra(k):
        start = per_pair * (k % block_pairs) + moved
        return jnp.logical_or(spare, jnp.logical_and(lane >= start, lane < start + 2))

    def choose():
        for b, ref in ((0, pick_moved), (1, pick_extra)):
            row = lax.broadcasted_iota(jnp.int32, ref.shape, 0)
            at = lax.broadcasted_iota(jnp.int32, ref.shape, 1)
            k, own = row // LANES, lax.rem(row, LANES)
            if b == 0:
                wanted = 2 * k + own - first_extra
                valid = jnp.logical_and(own >= first_extra, own < first_extra + 2)
            else:
                start = per_pair * lax.rem(k, block_pairs) + moved
                hole = jnp.logical_and(own >= start, own < start + 2)
                last = 2 * last_slot + own - start
                wanted = 2 * slots * k + jnp.where(hole, last, own - first_extra)
                valid = jnp.logical_or(hole, own >= first_extra)
            ref[...] = jnp.where(jnp.logical_and(valid, at == wanted), 1.0, 0.0).astype(
                jnp.bfloat16
            )

    extra_width = extra_in.shape[1]

    def along(row):
        return jnp.concatenate([row] * (extra_width // LANES), axis=1)

    extra_lane = lax.broadcasted_iota(jnp.int32, (1, extra_width), 1)
    extra_slot = lax.rem(extra_lane, 2 * slots) // 2
    extra_order = jnp.full((1, extra_width), -1, jnp.int32)
    for k in range(W):
        for s in range(slots):
            here = jnp.logical_and(extra_lane // (2 * slots) == k, extra_slot == s)
            value = source_orders[k][:, 2 * s : 2 * s + 1]
            extra_order = jnp.where(here, value, extra_order)

    def solve_extra(steps):
        x = extra_in[0:levels, :]
        y = extra_out[...]
        for t, j in steps:
            hit = extra_order == along(low_of(w, t, j))
            y = jnp.where(hit, times(t, j, 1, x).astype(jnp.bfloat16), y)
        extra_out[...] = y

    def late(ps):
        deal(1, ps, [solve(1, p) for p in ps], False)
        solve_extra([(2 + p // pairs, p % pairs) for p in ps])

    with scope("choose"):
        choose()
    with scope("wait0"):
        all_out(0).wait_recv()
    with scope("pack0"):
        for p in range(block_pairs):
            pack(0, p)
    with scope("moved"):
        moved_in = gather_spare(0, pick_moved)
    with scope("arrive1"):
        arrive((1, pairs), *[(1, c) for c in range(pairs)])
    fill_rest(1)
    with scope("near"):
        every = list(range(block_pairs))
        deal(0, every, [solve(0, p) for p in every], True)
    with scope("arrive2"):
        relay(*[(3, c) for c in range(1, pairs)])
        arrive((2, pairs), (2, 0))
    fill_rest(2)
    with scope("moved_back"):
        answer = times(2, 0, 1, moved_in).astype(jnp.bfloat16)
        scatter_spare(0, answer, pick_moved, lambda k: spare)
        start_back(0)
    with scope("wait1"):
        all_out(1).wait_recv()
    with scope("pack1"):
        for p in range(block_pairs):
            pack(1, p)
        extra_in[0:levels, :] = gather_spare(1, pick_extra)
        extra_out[...] = jnp.zeros_like(extra_out)
    with scope("extra"):
        solve_extra([(t, j) for t in range(2) for j in range(pairs)])
    with scope("late2a"):
        deal(1, [0], [solve(1, 0)], True)
        solve_extra([(2, 0)])
    with scope("arrive2b"):
        arrive(*[(2, c) for c in range(1, pairs)])
    with scope("late2b"):
        late(list(range(1, pairs)))
    with scope("arrive3"):
        arrive((3, pairs), *[(3, c) for c in range(pairs - 1)])
    fill_rest(3)
    with scope("late3a"):
        late(list(range(pairs, block_pairs - 1)))
    with scope("arrive3b"):
        arrive((3, pairs - 1))
    with scope("late3b"):
        late([block_pairs - 1])
        scatter_spare(1, extra_out[...], pick_extra, is_extra)
        start_back(1)

    fetches[6].wait()
    fetches[7].wait()
    total[...] = jnp.zeros_like(total)
    through_row = lax.broadcasted_iota(jnp.int32, (tail, levels), 0)
    through_lane = lax.broadcasted_iota(jnp.int32, (tail, levels), 1)
    response = jnp.concatenate(
        [
            jnp.where(through_lane == through_row + LANES, -1.0, 0.0),
            thermal_response[...].astype(jnp.float32),
            mass_row[...].astype(jnp.float32).reshape(1, levels),
        ],
        axis=0,
    ).astype(jnp.bfloat16)

    def collect(b, i, first, second):
        if not keep:
            build(b, i, 0)
        total[...] += lax.dot_general(
            jnp.concatenate([first, second], axis=1),
            pick[b, place_of(i)],
            (((1,), (1,)), ((), ())),
            preferred_element_type=jnp.float32,
        )

    def gather_back(b):
        with scope(f"back{b}_0"):
            some_back(b, 1, 1).wait_recv()
            collect(b, 0, solved[b, 0], returned[b, 1])

        def step(i, carry):
            some_back(b, 2 * i, 2).wait_recv()
            collect(b, i, returned[b, 2 * i], returned[b, 2 * i + 1])
            return carry

        with scope(f"back{b}"):
            lax.fori_loop(1, W // 2, step, 0)

    gather_back(0)
    gather_back(1)

    with scope("final"):
        div = total[0:levels, :].astype(jnp.bfloat16)
        change = jnp.dot(response, div, preferred_element_type=jnp.float32)
        old = state[LANES:, :].astype(jnp.float32)
        below = lax.broadcasted_iota(jnp.int32, old.shape, 0) < tail
        new = jnp.where(below, 0.0, old) - change
        new = jnp.where(column_order >= 0, new, 0.0)
        out[0:LANES, :] = div[0:LANES, :]
        out[LANES:, :] = new.astype(jnp.bfloat16)

    for b, table in ((0, info), (1, far_info)):
        all_out(b).wait_send()
        pltpu.make_async_remote_copy(
            src_ref=solved.at[b, pl.ds(1, W - 1)],
            dst_ref=returned.at[b, pl.ds(1, W - 1)],
            send_sem=back_send.at[b],
            recv_sem=back_recv.at[b, 0],
            device_id=(z, lax.rem(w + 1, W)),
            device_id_type=MESH,
        ).wait_send()
        all_tables(table, b).wait_send()
    pltpu.make_async_remote_copy(
        src_ref=low_rows.at[pl.ds(0, Z - 1)],
        dst_ref=low_rows.at[pl.ds(0, Z - 1)],
        send_sem=row_send,
        recv_sem=row_recv.at[1],
        device_id=(lax.rem(z + 1, Z), w),
        device_id_type=MESH,
    ).wait_send()

    def wait_relayed(count, way):
        for kind, ref in (
            (0, matrices.at[pl.ds(0, count), :, :, pl.ds(0, LANES)]),
            (1, rest.at[pl.ds(0, count)]),
        ):
            pltpu.make_async_remote_copy(
                src_ref=ref,
                dst_ref=ref,
                send_sem=z_send.at[kind, way],
                recv_sem=z_recv.at[0, 0],
                device_id=(lax.rem(z + 1, Z), w),
                device_id_type=MESH,
            ).wait_send()

    for zz in range(Z):

        @pl.when(z == zz)
        def _():
            if zz < Z - 1:
                wait_relayed(zz + 1, 0)
            if zz > 0:
                wait_relayed(Z - zz, 1)


def shards(
    state,
    held_orders,
    pair_lows,
    inverses,
    height_operator,
    pressure_column,
    thermal_response_matrix,
    mass_row,
):
    levels = height_operator.shape[0]
    slots = held_orders.shape[0]
    pairs = pair_lows.shape[0]
    Z, W = lax.axis_size("grp"), lax.axis_size("wave")
    width = state.shape[1]
    rows = ceil_to(levels, ROWS_TILE)
    places = W // 2 if W * width * 4 * LANES <= KEEP_BYTES else 1
    tiles = -(-W // (2 * pairs))
    extra_width = ceil_to(2 * slots * W, LANES)
    block = pltpu.VMEM((2, W, rows, LANES), jnp.bfloat16)
    return pl.pallas_call(
        functools.partial(kernel, (Z, W, levels, slots, pairs)),
        out_shape=pltpu.VMEM(state.shape, jnp.bfloat16),
        in_specs=[pl.BlockSpec(memory_space=pl.ANY)] * 8,
        out_specs=pl.BlockSpec(memory_space=pltpu.VMEM),
        scratch_shapes=[
            pltpu.SMEM(held_orders.shape, jnp.int32),
            pltpu.SMEM(pair_lows.shape, jnp.int32),
            pltpu.VMEM(state.shape, jnp.bfloat16),
            pltpu.VMEM((pairs, levels, 2, levels), jnp.bfloat16),
            pltpu.VMEM(height_operator.shape, jnp.bfloat16),
            pltpu.VMEM(pressure_column.shape, jnp.bfloat16),
            pltpu.VMEM(thermal_response_matrix.shape, jnp.bfloat16),
            pltpu.VMEM(mass_row.shape, jnp.bfloat16),
            pltpu.VMEM((Z, TABLE_ROWS, LANES), jnp.int32),
            pltpu.VMEM((W, NEAR_ROWS, LANES), jnp.int32),
            pltpu.VMEM((W, TABLE_ROWS, LANES), jnp.int32),
            pltpu.VMEM((Z, 2 * pairs, rows, levels), jnp.bfloat16),
            pltpu.VMEM((Z, rows, LANES), jnp.bfloat16),
            pltpu.VMEM((rows, width), jnp.bfloat16),
            pltpu.VMEM((2, places, width, 2 * LANES), jnp.bfloat16),
            block,
            block,
            block,
            block,
            pltpu.VMEM((4 * pairs, rows, tiles * LANES), jnp.bfloat16),
            pltpu.VMEM((ceil_to(2 * pairs, TABLE_ROWS), tiles * LANES), jnp.int32),
            pltpu.VMEM((W * LANES, ceil_to(2 * W, LANES)), jnp.bfloat16),
            pltpu.VMEM((W * LANES, extra_width), jnp.bfloat16),
            pltpu.VMEM((rows, extra_width), jnp.bfloat16),
            pltpu.VMEM((rows, extra_width), jnp.bfloat16),
            pltpu.VMEM((rows, width), jnp.float32),
            pltpu.SemaphoreType.DMA,
            pltpu.SemaphoreType.DMA((Z,)),
            pltpu.SemaphoreType.DMA((2,)),
            pltpu.SemaphoreType.DMA((2,)),
            pltpu.SemaphoreType.DMA((2, 2)),
            pltpu.SemaphoreType.DMA((Z, pairs + 1)),
            pltpu.SemaphoreType.DMA((2,)),
            pltpu.SemaphoreType.DMA((2,)),
            pltpu.SemaphoreType.DMA((2,)),
            pltpu.SemaphoreType.DMA((2, W // 2)),
            pltpu.SemaphoreType.DMA((8,)),
        ],
        compiler_params=pltpu.CompilerParams(
            collective_id=0, has_side_effects=True, vmem_limit_bytes=52 * 1024 * 1024
        ),
    )(
        *[
            pltpu.with_memory_space_constraint(array, pltpu.HBM)
            for array in (
                held_orders,
                pair_lows,
                state,
                jnp.transpose(inverses, (0, 2, 1, 3)),
                height_operator,
                pressure_column,
                thermal_response_matrix,
                mass_row,
            )
        ]
    )


def solution(mesh):
    placed = (
        P(None, ("grp", "wave")),
        P(("grp", "wave")),
        P(("grp", "wave")),
        P(("grp", "wave"), None, None, None),
        P(),
        P(),
        P(),
        P(),
    )
    return jax.shard_map(
        shards, mesh=mesh, in_specs=placed, out_specs=P(None, ("grp", "wave")), check_vma=False
    )
```

```python
import functools

import jax
import jax.numpy as jnp
from jax import lax
from jax.experimental import pallas as pl
from jax.experimental.pallas import tpu as pltpu
from jax.sharding import PartitionSpec as P

MESH = pl.DeviceIdType.MESH
LANES = 128
ROWS_TILE = 16
TABLE_ROWS = 8
NEAR_ROWS = 16
KEEP_BYTES = 24 << 20
scope = jax.named_scope


def ceil_to(value, step):
    return -(-value // step) * step


def kernel(
    size,
    held_far,
    lows_far,
    state_far,
    inverses_far,
    height_far,
    pressure_far,
    thermal_far,
    mass_far,
    out,
    held,
    lows,
    state,
    inverses,
    height_operator,
    pressure_column,
    thermal_response,
    mass_row,
    low_rows,
    info,
    far_info,
    matrices,
    edges,
    right,
    pick,
    outgoing,
    arrived,
    solved,
    returned,
    packed,
    packed_orders,
    pick_moved,
    pick_extra,
    extra_in,
    extra_out,
    total,
    row_send,
    row_recv,
    info_send,
    info_recv,
    z_send,
    z_recv,
    out_send,
    out_recv,
    back_send,
    back_recv,
    fetch_sem,
):
    Z, W, levels, slots, pairs = size
    half_count = Z * W * pairs
    truncation = 2 * half_count - 1
    slot_width = 2 * (truncation + 2)
    width = slots * slot_width
    denom = float(truncation * (truncation + 1))
    per_pair = 4 * slots
    block_pairs = 2 * pairs
    first_extra = block_pairs * per_pair
    moved = per_pair - 2
    tiles = packed.shape[2] // LANES
    last_slot = slots - 1
    tail = levels - LANES
    border = 2 * pairs * tail
    keep = pick.shape[1] > 1
    z = lax.axis_index("grp")
    w = lax.axis_index("wave")
    middle = jnp.logical_and(z > 0, z < Z - 1)

    barrier = pltpu.get_barrier_semaphore()

    def greet(k, carry):
        pl.semaphore_signal(
            barrier, inc=1, device_id=(z, lax.rem(w + k, W)), device_id_type=MESH
        )
        return carry

    fetches = [
        pltpu.make_async_copy(far, near, fetch_sem.at[i])
        for i, (far, near) in enumerate(
            [
                (lows_far, lows),
                (held_far, held),
                (inverses_far, inverses),
                (state_far, state),
                (height_far, height_operator),
                (pressure_far, pressure_column),
                (thermal_far, thermal_response),
                (mass_far, mass_row),
            ]
        )
    ]
    for k in range(1, Z):
        pl.semaphore_signal(barrier, inc=1, device_id=(lax.rem(z + k, Z), w), device_id_type=MESH)
    for fetch in fetches[:3]:
        fetch.start()
    lax.fori_loop(1, W, greet, 0)
    for fetch in fetches[3:]:
        fetch.start()

    lane = lax.broadcasted_iota(jnp.int32, (1, LANES), 1)
    lane_pair = lane // per_pair
    lane_member = lax.rem(lane, per_pair) // (2 * slots)
    lane_slot = lax.rem(lax.rem(lane, per_pair), 2 * slots) // 2
    lane_part = lax.rem(lane, 2)
    spare = lane >= first_extra
    table_row = lax.broadcasted_iota(jnp.int32, (TABLE_ROWS, LANES), 0)
    with scope("small_fetch"):
        fetches[0].wait()
        fetches[1].wait()
    orders = jnp.full((1, LANES), -1, jnp.int32)
    for s in range(slots):
        orders = jnp.where(lane_slot == s, held[s], orders)
    low_tile = jnp.zeros((TABLE_ROWS, LANES), jnp.int32)
    for j in range(pairs):
        low_tile = jnp.where(table_row == j, lows[j], low_tile)
    low_rows[z] = low_tile

    rows = matrices.shape[2]

    def split_inverses():
        fetches[2].wait()
        to_row = lax.broadcasted_iota(jnp.int32, (2 * rows, 2 * levels), 0)
        from_row = lax.broadcasted_iota(jnp.int32, (2 * rows, 2 * levels), 1)
        wanted = jnp.where(to_row < rows, 2 * to_row, 2 * (to_row - rows) + 1)
        split = jnp.where(wanted == from_row, 1.0, 0.0).astype(jnp.bfloat16)
        parts = []
        for j in range(pairs):
            both = jnp.dot(
                split,
                inverses[j].reshape(2 * levels, levels),
                preferred_element_type=jnp.float32,
            )
            for member in range(2):
                matrix = both[member * rows : (member + 1) * rows]
                matrices[z, 2 * j + member] = matrix.astype(jnp.bfloat16)
                parts.append(matrix)
        blank = jnp.zeros((LANES, LANES - border), jnp.float32)
        under = [matrix[LANES:levels, 0:LANES] for matrix in parts]
        aside = jnp.concatenate([m[0:LANES, LANES:levels] for m in parts] + [blank], axis=1)
        corner = [m[LANES:levels, LANES:levels] for m in parts] + [blank[0:tail]]
        corner = jnp.concatenate(corner, axis=1)
        filler = jnp.zeros((LANES - 2 * border - tail, LANES), jnp.float32)
        edge = jnp.concatenate([*under, aside.T[0:border], corner, filler], axis=0)
        edges[z] = edge.astype(jnp.bfloat16)

    @pl.when(z < Z - 1)
    def _():
        with scope("split"):
            split_inverses()

    with scope("barrier"):
        pl.semaphore_wait(barrier, W + Z - 2)

    def z_copy(g, c, way):
        if c < pairs:
            ref = matrices.at[g, pl.ds(2 * c, 2), pl.ds(0, LANES), pl.ds(0, LANES)]
        else:
            ref = edges.at[g]
        step = 1 if way == 0 else -1
        return pltpu.make_async_remote_copy(
            src_ref=ref,
            dst_ref=ref,
            send_sem=z_send.at[0 if c < pairs else 1, way],
            recv_sem=z_recv.at[g, c],
            device_id=(z + step, w),
            device_id_type=MESH,
        )

    def forward(g, c):
        @pl.when(jnp.logical_and(g <= z, z < Z - 1))
        def _():
            z_copy(g, c, 0).start()

        @pl.when(jnp.logical_and(g >= z, z > 0))
        def _():
            z_copy(g, c, 1).start()

    def group_at(t):
        g = z
        for zz in range(Z):
            by_distance = sorted(range(Z), key=lambda a: (abs(a - zz), abs(2 * a - Z + 1)))
            g = jnp.where(z == zz, by_distance[t], g)
        return g

    def relay_now(*steps):
        for t, c in steps:
            g = group_at(t)
            z_copy(g, c, 0).wait_recv()
            forward(g, c)

    def relay(*steps):
        @pl.when(middle)
        def _():
            relay_now(*steps)

    def arrive(*steps):
        @pl.when(jnp.logical_not(middle))
        def _():
            for t, c in steps:
                z_copy(group_at(t), c, 0).wait_recv()

    groups = [group_at(t) for t in range(Z)]

    def row_copy(k):
        return pltpu.make_async_remote_copy(
            src_ref=low_rows.at[z],
            dst_ref=low_rows.at[z],
            send_sem=row_send,
            recv_sem=row_recv.at[k],
            device_id=(lax.rem(z + k, Z), w),
            device_id_type=MESH,
        )

    def wait_row(g):
        pltpu.make_async_remote_copy(
            src_ref=low_rows.at[g],
            dst_ref=low_rows.at[g],
            send_sem=row_send,
            recv_sem=row_recv.at[lax.rem(z + Z - g, Z)],
            device_id=(g, w),
            device_id_type=MESH,
        ).wait_recv()

    def table_copy(table, b, k):
        return pltpu.make_async_remote_copy(
            src_ref=table.at[w],
            dst_ref=table.at[w],
            send_sem=info_send.at[b],
            recv_sem=info_recv.at[b],
            device_id=(z, lax.rem(w + k, W)),
            device_id_type=MESH,
        )

    def send_table(table, b):
        def start(k, carry):
            table_copy(table, b, k).start()
            return carry

        lax.fori_loop(1, W, start, 0)

    def all_tables(table, b):
        return pltpu.make_async_remote_copy(
            src_ref=table.at[pl.ds(0, W - 1)],
            dst_ref=table.at[pl.ds(0, W - 1)],
            send_sem=info_send.at[b],
            recv_sem=info_recv.at[b],
            device_id=(z, lax.rem(w + 1, W)),
            device_id_type=MESH,
        )

    for k in range(1, Z):
        row_copy(k).start()

    @pl.when(z == Z - 1)
    def _():
        with scope("split_end"):
            split_inverses()

    for c in [pairs, *range(pairs)]:
        forward(z, c)

    column = lax.broadcasted_iota(jnp.int32, (1, width), 1)
    column_order = jnp.full((1, width), -1, jnp.int32)
    column_start = jnp.zeros((1, width), jnp.int32)
    for s in range(slots):
        inside = jnp.logical_and(column >= s * slot_width, column < (s + 1) * slot_width)
        column_order = jnp.where(inside, held[s], column_order)
        column_start = jnp.where(inside, s * slot_width, column_start)

    def drive_right():
        coefficient = (column - column_start) // 2
        degree = jnp.where(
            coefficient <= truncation - column_order, column_order + coefficient, coefficient - 1
        )
        lap_scale = (degree * (degree + 1)).astype(jnp.float32) / denom
        fetches[4].wait()
        fetches[5].wait()
        height = height_operator[...].astype(jnp.float32)
        pressure_row = jnp.broadcast_to(
            pressure_column[...].astype(jnp.float32).reshape(1, levels), height.shape
        )
        across = lax.broadcasted_iota(jnp.int32, height.shape, 1)
        down = lax.broadcasted_iota(jnp.int32, height.shape, 0)
        pressure_side = jnp.sum(
            jnp.where(across == down, pressure_row, 0.0), axis=1, keepdims=True
        )
        height = jnp.concatenate(
            [jnp.zeros((levels, tail), jnp.float32), height, pressure_side], axis=1
        ).astype(jnp.bfloat16)
        fetches[3].wait()
        drive = jnp.dot(height, state[LANES:, :], preferred_element_type=jnp.float32)
        right[0:levels, :] = (
            state[0:levels, :].astype(jnp.float32) + lap_scale * drive
        ).astype(jnp.bfloat16)

    with scope("drive"):
        drive_right()
    with scope("rows_wait"):
        for t in range(1, 3):
            wait_row(groups[t])
    table = [low_rows[groups[t]][0:pairs] for t in range(3)]
    table += [jnp.broadcast_to(orders, (NEAR_ROWS - 3 * pairs, LANES))]
    info[w] = jnp.concatenate(table, axis=0)
    send_table(info, 0)
    with scope("row_far"):
        wait_row(groups[3])
    far_info[w] = low_rows[groups[3]]
    send_table(far_info, 1)

    @pl.when(middle)
    def _():
        with scope("relay_a"):
            relay_now((1, pairs), (1, 0), (2, pairs), (2, 0), (1, 1))

    with scope("info_wait"):
        all_tables(info, 0).wait_recv()

    def low_of(d, t, j):
        if t < 3:
            return info[d][t * pairs + j : t * pairs + j + 1]
        return far_info[d][j : j + 1]

    def target_of(b, k):
        d = lax.rem(w + k, W)
        pair = lax.rem(lane_pair + block_pairs - lax.rem(k, block_pairs), block_pairs)
        low = jnp.zeros((1, LANES), jnp.int32)
        for p in range(block_pairs):
            low = jnp.where(pair == p, low_of(d, 2 * b + p // pairs, p % pairs), low)
        slot, member, order = lane_slot, lane_member, orders
        if b == 0:
            low = jnp.where(spare, low_of(d, 2, 0), low)
            slot = jnp.where(spare, last_slot, slot)
            member = jnp.where(spare, 1, member)
            order = jnp.where(spare, held[last_slot], order)
        merged = jnp.where(order <= low, low - order, truncation + 1 - low)
        position = jnp.where(member == 0, merged, truncation - low - order)
        used = order >= 0
        if b == 0:
            used = jnp.logical_and(used, lane < first_extra + 2)
        else:
            hole = jnp.logical_and(pair == 0, lax.rem(lane, per_pair) >= moved)
            extra = jnp.logical_or(spare, hole)
            position = jnp.where(extra, truncation + 1 - order, position)
        target = slot * slot_width + 2 * position + lane_part
        return jnp.where(used, target, -1)

    def build(b, i, place):
        at = lax.broadcasted_iota(jnp.int32, (width, LANES), 0)
        for h in range(2):
            pick[b, place, :, h * LANES : (h + 1) * LANES] = jnp.where(
                at == target_of(b, 2 * i + h), 1.0, 0.0
            ).astype(jnp.bfloat16)

    def place_of(i):
        return i if keep else 0

    def out_copy(b, k):
        return pltpu.make_async_remote_copy(
            src_ref=outgoing.at[b, k],
            dst_ref=arrived.at[b, k],
            send_sem=out_send.at[b],
            recv_sem=out_recv.at[b],
            device_id=(z, lax.rem(w + k, W)),
            device_id_type=MESH,
        )

    def back_copy(b, k):
        return pltpu.make_async_remote_copy(
            src_ref=solved.at[b, k],
            dst_ref=returned.at[b, k],
            send_sem=back_send.at[b],
            recv_sem=back_recv.at[b, k // 2],
            device_id=(z, lax.rem(w + W - k, W)),
            device_id_type=MESH,
        )

    def send_block(b, start, stop):
        def send(i, carry):
            build(b, i, place_of(i))
            message = jnp.dot(
                right[...], pick[b, place_of(i)], preferred_element_type=jnp.float32
            ).astype(jnp.bfloat16)
            k0, k1 = 2 * i, 2 * i + 1
            outgoing[b, k0] = message[:, :LANES]
            outgoing[b, k1] = message[:, LANES:]

            @pl.when(i > 0)
            def _():
                out_copy(b, k0).start()

            out_copy(b, k1).start()
            return carry

        lax.fori_loop(start, stop, send, 0)

    def all_out(b):
        return pltpu.make_async_remote_copy(
            src_ref=outgoing.at[b, pl.ds(1, W - 1)],
            dst_ref=arrived.at[b, pl.ds(1, W - 1)],
            send_sem=out_send.at[b],
            recv_sem=out_recv.at[b],
            device_id=(z, lax.rem(w + 1, W)),
            device_id_type=MESH,
        )

    def some_back(b, first, count):
        return pltpu.make_async_remote_copy(
            src_ref=solved.at[b, pl.ds(first, count)],
            dst_ref=returned.at[b, pl.ds(first, count)],
            send_sem=back_send.at[b],
            recv_sem=back_recv.at[b, first // 2],
            device_id=(z, lax.rem(w + 1, W)),
            device_id_type=MESH,
        )

    with scope("send0"):
        send_block(0, 0, W // 4)
    with scope("relay_b"):
        relay((1, 2), (2, 1))
    with scope("send0b"):
        send_block(0, W // 4, W // 2)
    with scope("relay_c"):
        relay((2, 2), (3, pairs))
    with scope("far_wait"):
        all_tables(far_info, 1).wait_recv()
    with scope("send1"):
        send_block(1, 0, W // 4)
    with scope("relay_d"):
        relay((3, 0))
    with scope("send1b"):
        send_block(1, W // 4, W // 2)
    with scope("relay_e"):
        relay((3, 1))
    for b in range(2):
        arrived[b, 0] = outgoing[b, 0]

    def fill_edges(t):
        g = groups[t]
        edge = edges[g].astype(jnp.float32)
        across = edge.T
        for i in range(2 * pairs):
            at = i * tail
            side = across[:, border + at : border + at + tail]
            below = jnp.concatenate(
                [edge[at : at + tail], edge[2 * border : 2 * border + tail, at : at + tail]],
                axis=1,
            )
            matrices[g, i, 0:LANES, LANES:levels] = side.astype(jnp.bfloat16)
            matrices[g, i, LANES:levels, :] = below.astype(jnp.bfloat16)

    def spread(row):
        return jnp.concatenate([row] * tiles, axis=1)

    source_orders = [
        info[lax.rem(w + W - k, W)][3 * pairs : 3 * pairs + 1] for k in range(W)
    ]

    def place(p, k):
        return lane_pair == (p + k) % block_pairs

    def pack(b, p):
        for v in range(tiles):
            first = v * block_pairs
            columns = arrived[b, first, 0:levels, :]
            order = source_orders[first]
            for k in range(first + 1, min(first + block_pairs, W)):
                columns = jnp.where(place(p, k), arrived[b, k, 0:levels, :], columns)
                order = jnp.where(place(p, k), source_orders[k], order)
            part = slice(v * LANES, (v + 1) * LANES)
            packed[b * block_pairs + p, 0:levels, part] = columns
            if b == 0:
                packed_orders[p : p + 1, part] = order

    wide_member = spread(lane_member)

    def times(t, j, member, x):
        return jnp.dot(
            matrices[groups[t], 2 * j + member], x, preferred_element_type=jnp.float32
        )

    def solve(b, p):
        t, j = 2 * b + p // pairs, p % pairs
        x = packed[b * block_pairs + p, 0:levels, :]
        low = spread(low_of(w, t, j))
        use_low = jnp.logical_and(wide_member == 0, packed_orders[p : p + 1, :] <= low)
        y = jnp.where(use_low, times(t, j, 0, x), times(t, j, 1, x))
        return y.astype(jnp.bfloat16)

    def deal(b, ps, answers, fresh):
        for k in range(W):
            v = k // block_pairs
            parts = [y[:, v * LANES : (v + 1) * LANES] for y in answers]
            block = parts[0] if fresh else solved[b, k]
            for p, part in list(zip(ps, parts))[1 if fresh else 0 :]:
                block = jnp.where(place(p, k), part, block)
            solved[b, k] = block

    def start_back(b):
        for k in range(1, W):
            back_copy(b, k).start()

    def gather_spare(b, chosen):
        columns = jnp.concatenate([arrived[b, k, 0:levels, :] for k in range(W)], axis=1)
        return jnp.dot(columns, chosen[...], preferred_element_type=jnp.float32).astype(
            jnp.bfloat16
        )

    def scatter_spare(b, answer, chosen, where):
        back = lax.dot_general(
            answer, chosen[...], (((1,), (1,)), ((), ())), preferred_element_type=jnp.float32
        ).astype(jnp.bfloat16)
        for k in range(W):
            part = back[:, k * LANES : (k + 1) * LANES]
            solved[b, k] = jnp.where(where(k), part, solved[b, k])

    def is_extra(k):
        start = per_pair * (k % block_pairs) + moved
        return jnp.logical_or(spare, jnp.logical_and(lane >= start, lane < start + 2))

    def choose():
        for b, ref in ((0, pick_moved), (1, pick_extra)):
            row = lax.broadcasted_iota(jnp.int32, ref.shape, 0)
            at = lax.broadcasted_iota(jnp.int32, ref.shape, 1)
            k, own = row // LANES, lax.rem(row, LANES)
            if b == 0:
                wanted = 2 * k + own - first_extra
                valid = jnp.logical_and(own >= first_extra, own < first_extra + 2)
            else:
                start = per_pair * lax.rem(k, block_pairs) + moved
                hole = jnp.logical_and(own >= start, own < start + 2)
                last = 2 * last_slot + own - start
                wanted = 2 * slots * k + jnp.where(hole, last, own - first_extra)
                valid = jnp.logical_or(hole, own >= first_extra)
            ref[...] = jnp.where(jnp.logical_and(valid, at == wanted), 1.0, 0.0).astype(
                jnp.bfloat16
            )

    extra_width = extra_in.shape[1]

    def along(row):
        return jnp.concatenate([row] * (extra_width // LANES), axis=1)

    extra_lane = lax.broadcasted_iota(jnp.int32, (1, extra_width), 1)
    extra_slot = lax.rem(extra_lane, 2 * slots) // 2
    extra_order = jnp.full((1, extra_width), -1, jnp.int32)
    for k in range(W):
        for s in range(slots):
            here = jnp.logical_and(extra_lane // (2 * slots) == k, extra_slot == s)
            value = source_orders[k][:, 2 * s : 2 * s + 1]
            extra_order = jnp.where(here, value, extra_order)

    def solve_extra(steps):
        x = extra_in[0:levels, :]
        y = extra_out[...]
        for t, j in steps:
            hit = extra_order == along(low_of(w, t, j))
            y = jnp.where(hit, times(t, j, 1, x).astype(jnp.bfloat16), y)
        extra_out[...] = y

    def late(ps):
        deal(1, ps, [solve(1, p) for p in ps], False)
        solve_extra([(2 + p // pairs, p % pairs) for p in ps])

    with scope("choose"):
        choose()
    with scope("wait0"):
        all_out(0).wait_recv()
    with scope("pack0"):
        for p in range(block_pairs):
            pack(0, p)
    with scope("moved"):
        moved_in = gather_spare(0, pick_moved)
    with scope("arrive1"):
        arrive((1, pairs), *[(1, c) for c in range(pairs)])
    fill_edges(1)
    with scope("near"):
        every = list(range(block_pairs))
        deal(0, every, [solve(0, p) for p in every], True)
    with scope("arrive2"):
        relay((3, 2))
        arrive((2, pairs), (2, 0))
    fill_edges(2)
    with scope("moved_back"):
        answer = times(2, 0, 1, moved_in).astype(jnp.bfloat16)
        scatter_spare(0, answer, pick_moved, lambda k: spare)
        start_back(0)
    with scope("wait1"):
        all_out(1).wait_recv()
    with scope("pack1"):
        for p in range(block_pairs):
            pack(1, p)
        extra_in[0:levels, :] = gather_spare(1, pick_extra)
        extra_out[...] = jnp.zeros_like(extra_out)
    with scope("extra"):
        solve_extra([(t, j) for t in range(2) for j in range(pairs)])
    with scope("late2a"):
        deal(1, [0], [solve(1, 0)], True)
        solve_extra([(2, 0)])
    with scope("arrive2b"):
        arrive(*[(2, c) for c in range(1, pairs)])
    with scope("late2b"):
        late(list(range(1, pairs)))
    with scope("arrive3"):
        arrive((3, pairs), *[(3, c) for c in range(pairs - 1)])
    fill_edges(3)
    with scope("late3a"):
        late(list(range(pairs, block_pairs - 1)))
    with scope("arrive3b"):
        arrive((3, pairs - 1))
    with scope("late3b"):
        late([block_pairs - 1])
        scatter_spare(1, extra_out[...], pick_extra, is_extra)
        start_back(1)

    fetches[6].wait()
    fetches[7].wait()
    total[...] = jnp.zeros_like(total)
    through_row = lax.broadcasted_iota(jnp.int32, (tail, levels), 0)
    through_lane = lax.broadcasted_iota(jnp.int32, (tail, levels), 1)
    response = jnp.concatenate(
        [
            jnp.where(through_lane == through_row + LANES, -1.0, 0.0),
            thermal_response[...].astype(jnp.float32),
            mass_row[...].astype(jnp.float32).reshape(1, levels),
        ],
        axis=0,
    ).astype(jnp.bfloat16)

    def collect(b, i, first, second):
        if not keep:
            build(b, i, 0)
        total[...] += lax.dot_general(
            jnp.concatenate([first, second], axis=1),
            pick[b, place_of(i)],
            (((1,), (1,)), ((), ())),
            preferred_element_type=jnp.float32,
        )

    def gather_back(b):
        with scope(f"back{b}_0"):
            some_back(b, 1, 1).wait_recv()
            collect(b, 0, solved[b, 0], returned[b, 1])

        def step(i, carry):
            some_back(b, 2 * i, 2).wait_recv()
            collect(b, i, returned[b, 2 * i], returned[b, 2 * i + 1])
            return carry

        with scope(f"back{b}"):
            lax.fori_loop(1, W // 2, step, 0)

    gather_back(0)
    gather_back(1)

    with scope("final"):
        div = total[0:levels, :].astype(jnp.bfloat16)
        change = jnp.dot(response, div, preferred_element_type=jnp.float32)
        old = state[LANES:, :].astype(jnp.float32)
        below = lax.broadcasted_iota(jnp.int32, old.shape, 0) < tail
        new = jnp.where(below, 0.0, old) - change
        new = jnp.where(column_order >= 0, new, 0.0)
        out[0:LANES, :] = div[0:LANES, :]
        out[LANES:, :] = new.astype(jnp.bfloat16)

    for b, table in ((0, info), (1, far_info)):
        all_out(b).wait_send()
        pltpu.make_async_remote_copy(
            src_ref=solved.at[b, pl.ds(1, W - 1)],
            dst_ref=returned.at[b, pl.ds(1, W - 1)],
            send_sem=back_send.at[b],
            recv_sem=back_recv.at[b, 0],
            device_id=(z, lax.rem(w + 1, W)),
            device_id_type=MESH,
        ).wait_send()
        all_tables(table, b).wait_send()
    pltpu.make_async_remote_copy(
        src_ref=low_rows.at[pl.ds(0, Z - 1)],
        dst_ref=low_rows.at[pl.ds(0, Z - 1)],
        send_sem=row_send,
        recv_sem=row_recv.at[1],
        device_id=(lax.rem(z + 1, Z), w),
        device_id_type=MESH,
    ).wait_send()

    def wait_relayed(count, way):
        for kind, ref in (
            (0, matrices.at[pl.ds(0, count), :, pl.ds(0, LANES), pl.ds(0, LANES)]),
            (1, edges.at[pl.ds(0, count)]),
        ):
            pltpu.make_async_remote_copy(
                src_ref=ref,
                dst_ref=ref,
                send_sem=z_send.at[kind, way],
                recv_sem=z_recv.at[0, 0],
                device_id=(lax.rem(z + 1, Z), w),
                device_id_type=MESH,
            ).wait_send()

    for zz in range(Z):

        @pl.when(z == zz)
        def _():
            if zz < Z - 1:
                wait_relayed(zz + 1, 0)
            if zz > 0:
                wait_relayed(Z - zz, 1)


def shards(
    state,
    held_orders,
    pair_lows,
    inverses,
    height_operator,
    pressure_column,
    thermal_response_matrix,
    mass_row,
):
    levels = height_operator.shape[0]
    slots = held_orders.shape[0]
    pairs = pair_lows.shape[0]
    Z, W = lax.axis_size("grp"), lax.axis_size("wave")
    width = state.shape[1]
    rows = ceil_to(levels, ROWS_TILE)
    places = W // 2 if W * width * 4 * LANES <= KEEP_BYTES else 1
    tiles = -(-W // (2 * pairs))
    extra_width = ceil_to(2 * slots * W, LANES)
    block = pltpu.VMEM((2, W, rows, LANES), jnp.bfloat16)
    return pl.pallas_call(
        functools.partial(kernel, (Z, W, levels, slots, pairs)),
        out_shape=pltpu.VMEM(state.shape, jnp.bfloat16),
        in_specs=[pl.BlockSpec(memory_space=pl.ANY)] * 8,
        out_specs=pl.BlockSpec(memory_space=pltpu.VMEM),
        scratch_shapes=[
            pltpu.SMEM(held_orders.shape, jnp.int32),
            pltpu.SMEM(pair_lows.shape, jnp.int32),
            pltpu.VMEM(state.shape, jnp.bfloat16),
            pltpu.VMEM((pairs, levels, 2, levels), jnp.bfloat16),
            pltpu.VMEM(height_operator.shape, jnp.bfloat16),
            pltpu.VMEM(pressure_column.shape, jnp.bfloat16),
            pltpu.VMEM(thermal_response_matrix.shape, jnp.bfloat16),
            pltpu.VMEM(mass_row.shape, jnp.bfloat16),
            pltpu.VMEM((Z, TABLE_ROWS, LANES), jnp.int32),
            pltpu.VMEM((W, NEAR_ROWS, LANES), jnp.int32),
            pltpu.VMEM((W, TABLE_ROWS, LANES), jnp.int32),
            pltpu.VMEM((Z, 2 * pairs, rows, levels), jnp.bfloat16),
            pltpu.VMEM((Z, LANES, LANES), jnp.bfloat16),
            pltpu.VMEM((rows, width), jnp.bfloat16),
            pltpu.VMEM((2, places, width, 2 * LANES), jnp.bfloat16),
            block,
            block,
            block,
            block,
            pltpu.VMEM((4 * pairs, rows, tiles * LANES), jnp.bfloat16),
            pltpu.VMEM((ceil_to(2 * pairs, TABLE_ROWS), tiles * LANES), jnp.int32),
            pltpu.VMEM((W * LANES, ceil_to(2 * W, LANES)), jnp.bfloat16),
            pltpu.VMEM((W * LANES, extra_width), jnp.bfloat16),
            pltpu.VMEM((rows, extra_width), jnp.bfloat16),
            pltpu.VMEM((rows, extra_width), jnp.bfloat16),
            pltpu.VMEM((rows, width), jnp.float32),
            pltpu.SemaphoreType.DMA,
            pltpu.SemaphoreType.DMA((Z,)),
            pltpu.SemaphoreType.DMA((2,)),
            pltpu.SemaphoreType.DMA((2,)),
            pltpu.SemaphoreType.DMA((2, 2)),
            pltpu.SemaphoreType.DMA((Z, pairs + 1)),
            pltpu.SemaphoreType.DMA((2,)),
            pltpu.SemaphoreType.DMA((2,)),
            pltpu.SemaphoreType.DMA((2,)),
            pltpu.SemaphoreType.DMA((2, W // 2)),
            pltpu.SemaphoreType.DMA((8,)),
        ],
        compiler_params=pltpu.CompilerParams(
            collective_id=0, has_side_effects=True, vmem_limit_bytes=52 * 1024 * 1024
        ),
    )(
        *[
            pltpu.with_memory_space_constraint(array, pltpu.HBM)
            for array in (
                held_orders,
                pair_lows,
                state,
                jnp.transpose(inverses, (0, 2, 1, 3)),
                height_operator,
                pressure_column,
                thermal_response_matrix,
                mass_row,
            )
        ]
    )


def solution(mesh):
    placed = (
        P(None, ("grp", "wave")),
        P(("grp", "wave")),
        P(("grp", "wave")),
        P(("grp", "wave"), None, None, None),
        P(),
        P(),
        P(),
        P(),
    )
    return jax.shard_map(
        shards, mesh=mesh, in_specs=placed, out_specs=P(None, ("grp", "wave")), check_vma=False
    )
```

```python
import functools

import jax
import jax.numpy as jnp
from jax import lax
from jax.experimental import pallas as pl
from jax.experimental.pallas import tpu as pltpu
from jax.sharding import PartitionSpec as P

MESH = pl.DeviceIdType.MESH
LANES = 128
ROWS_TILE = 16
TABLE_ROWS = 8
NEAR_ROWS = 16
KEEP_BYTES = 24 << 20
scope = jax.named_scope


def ceil_to(value, step):
    return -(-value // step) * step


def kernel(
    size,
    held_far,
    lows_far,
    state_far,
    inverses_far,
    height_far,
    pressure_far,
    thermal_far,
    mass_far,
    out,
    held,
    lows,
    state,
    inverses,
    height_operator,
    pressure_column,
    thermal_response,
    mass_row,
    low_rows,
    info,
    far_info,
    matrices,
    edges,
    right,
    pick,
    outgoing,
    arrived,
    solved,
    returned,
    packed,
    packed_orders,
    pick_extra,
    extra_in,
    extra_out,
    total,
    row_send,
    row_recv,
    info_send,
    info_recv,
    z_send,
    z_recv,
    out_send,
    out_recv,
    back_send,
    back_recv,
    fetch_sem,
):
    Z, W, levels, slots, pairs = size
    half_count = Z * W * pairs
    truncation = 2 * half_count - 1
    slot_width = 2 * (truncation + 2)
    width = slots * slot_width
    denom = float(truncation * (truncation + 1))
    per_pair = 4 * slots
    block_pairs = 2 * pairs
    first_extra = block_pairs * per_pair
    moved = per_pair - 2
    tiles = packed.shape[2] // LANES
    last_slot = slots - 1
    tail = levels - LANES
    border = 2 * pairs * tail
    keep = pick.shape[1] > 1
    z = lax.axis_index("grp")
    w = lax.axis_index("wave")
    middle = jnp.logical_and(z > 0, z < Z - 1)

    barrier = pltpu.get_barrier_semaphore()

    def peer(k):
        other = 0
        for i in range(W.bit_length() - 1):
            mine, flip = lax.rem(w // (1 << i), 2), lax.rem(k // (1 << i), 2)
            other = other + (1 << i) * (mine + flip - 2 * mine * flip)
        return other

    def greet(k, carry):
        pl.semaphore_signal(barrier, inc=1, device_id=(z, peer(k)), device_id_type=MESH)
        return carry

    fetches = [
        pltpu.make_async_copy(far, near, fetch_sem.at[i])
        for i, (far, near) in enumerate(
            [
                (lows_far, lows),
                (held_far, held),
                (inverses_far, inverses),
                (state_far, state),
                (height_far, height_operator),
                (pressure_far, pressure_column),
                (thermal_far, thermal_response),
                (mass_far, mass_row),
            ]
        )
    ]
    for k in range(1, Z):
        pl.semaphore_signal(barrier, inc=1, device_id=(lax.rem(z + k, Z), w), device_id_type=MESH)
    for fetch in fetches[:3]:
        fetch.start()
    lax.fori_loop(1, W, greet, 0)
    for fetch in fetches[3:]:
        fetch.start()

    lane = lax.broadcasted_iota(jnp.int32, (1, LANES), 1)
    lane_pair = lane // per_pair
    lane_member = lax.rem(lane, per_pair) // (2 * slots)
    lane_slot = lax.rem(lax.rem(lane, per_pair), 2 * slots) // 2
    lane_part = lax.rem(lane, 2)
    spare = lane >= first_extra
    table_row = lax.broadcasted_iota(jnp.int32, (TABLE_ROWS, LANES), 0)
    with scope("small_fetch"):
        fetches[0].wait()
        fetches[1].wait()
    orders = jnp.full((1, LANES), -1, jnp.int32)
    for s in range(slots):
        orders = jnp.where(lane_slot == s, held[s], orders)
    low_tile = jnp.zeros((TABLE_ROWS, LANES), jnp.int32)
    for j in range(pairs):
        low_tile = jnp.where(table_row == j, lows[j], low_tile)
    low_rows[z] = low_tile

    rows = matrices.shape[2]

    def split_inverses():
        fetches[2].wait()
        to_row = lax.broadcasted_iota(jnp.int32, (2 * rows, 2 * levels), 0)
        from_row = lax.broadcasted_iota(jnp.int32, (2 * rows, 2 * levels), 1)
        wanted = jnp.where(to_row < rows, 2 * to_row, 2 * (to_row - rows) + 1)
        split = jnp.where(wanted == from_row, 1.0, 0.0).astype(jnp.bfloat16)
        parts = []
        for j in range(pairs):
            both = jnp.dot(
                split,
                inverses[j].reshape(2 * levels, levels),
                preferred_element_type=jnp.float32,
            )
            for member in range(2):
                matrix = both[member * rows : (member + 1) * rows]
                matrices[z, 2 * j + member] = matrix.astype(jnp.bfloat16)
                parts.append(matrix)
        blank = jnp.zeros((LANES, LANES - border), jnp.float32)
        under = [matrix[LANES:levels, 0:LANES] for matrix in parts]
        aside = jnp.concatenate([m[0:LANES, LANES:levels] for m in parts] + [blank], axis=1)
        corner = [m[LANES:levels, LANES:levels] for m in parts] + [blank[0:tail]]
        corner = jnp.concatenate(corner, axis=1)
        filler = jnp.zeros((LANES - 2 * border - tail, LANES), jnp.float32)
        edge = jnp.concatenate([*under, aside.T[0:border], corner, filler], axis=0)
        edges[z] = edge.astype(jnp.bfloat16)

    @pl.when(z < Z - 1)
    def _():
        with scope("split"):
            split_inverses()

    with scope("barrier"):
        pl.semaphore_wait(barrier, W + Z - 2)

    def z_copy(g, c, way):
        if c < pairs:
            ref = matrices.at[g, pl.ds(2 * c, 2), pl.ds(0, LANES), pl.ds(0, LANES)]
        else:
            ref = edges.at[g]
        step = 1 if way == 0 else -1
        return pltpu.make_async_remote_copy(
            src_ref=ref,
            dst_ref=ref,
            send_sem=z_send.at[0 if c < pairs else 1, way],
            recv_sem=z_recv.at[g, c],
            device_id=(z + step, w),
            device_id_type=MESH,
        )

    def forward(g, c):
        @pl.when(jnp.logical_and(g <= z, z < Z - 1))
        def _():
            z_copy(g, c, 0).start()

        @pl.when(jnp.logical_and(g >= z, z > 0))
        def _():
            z_copy(g, c, 1).start()

    def group_at(t):
        g = z
        for zz in range(Z):
            by_distance = sorted(range(Z), key=lambda a: (abs(a - zz), abs(2 * a - Z + 1)))
            g = jnp.where(z == zz, by_distance[t], g)
        return g

    def relay_now(*steps):
        for t, c in steps:
            g = group_at(t)
            z_copy(g, c, 0).wait_recv()
            forward(g, c)

    def relay(*steps):
        @pl.when(middle)
        def _():
            relay_now(*steps)

    def arrive(*steps):
        @pl.when(jnp.logical_not(middle))
        def _():
            for t, c in steps:
                z_copy(group_at(t), c, 0).wait_recv()

    groups = [group_at(t) for t in range(Z)]

    def row_copy(g):
        return pltpu.make_async_remote_copy(
            src_ref=low_rows.at[z],
            dst_ref=low_rows.at[z],
            send_sem=row_send,
            recv_sem=row_recv.at[z],
            device_id=(g, w),
            device_id_type=MESH,
        )

    def send_rows(distance):
        for step in (-distance, distance):

            @pl.when(jnp.logical_and(z + step >= 0, z + step < Z))
            def _():
                row_copy(z + step).start()

    def wait_row(g):
        pltpu.make_async_remote_copy(
            src_ref=low_rows.at[g],
            dst_ref=low_rows.at[g],
            send_sem=row_send,
            recv_sem=row_recv.at[g],
            device_id=(g, w),
            device_id_type=MESH,
        ).wait_recv()

    def table_copy(table, b, k):
        return pltpu.make_async_remote_copy(
            src_ref=table.at[w],
            dst_ref=table.at[w],
            send_sem=info_send.at[b],
            recv_sem=info_recv.at[b],
            device_id=(z, peer(k)),
            device_id_type=MESH,
        )

    def send_table(table, b):
        def start(n, carry):
            table_copy(table, b, W - n).start()
            return carry

        lax.fori_loop(1, W, start, 0)

    def all_tables(table, b):
        return pltpu.make_async_remote_copy(
            src_ref=table.at[pl.ds(0, W - 1)],
            dst_ref=table.at[pl.ds(0, W - 1)],
            send_sem=info_send.at[b],
            recv_sem=info_recv.at[b],
            device_id=(z, peer(1)),
            device_id_type=MESH,
        )

    for distance in range(1, Z):
        send_rows(distance)

    @pl.when(z == Z - 1)
    def _():
        with scope("split_end"):
            split_inverses()

    for c in [pairs, *range(pairs)]:
        forward(z, c)

    column = lax.broadcasted_iota(jnp.int32, (1, width), 1)
    column_order = jnp.full((1, width), -1, jnp.int32)
    column_start = jnp.zeros((1, width), jnp.int32)
    for s in range(slots):
        inside = jnp.logical_and(column >= s * slot_width, column < (s + 1) * slot_width)
        column_order = jnp.where(inside, held[s], column_order)
        column_start = jnp.where(inside, s * slot_width, column_start)

    def choose():
        row = lax.broadcasted_iota(jnp.int32, pick_extra.shape, 0)
        at = lax.broadcasted_iota(jnp.int32, pick_extra.shape, 1)
        k, own = row // LANES, lax.rem(row, LANES)
        start = per_pair * lax.rem(k, block_pairs) + moved
        hole = jnp.logical_and(own >= start, own < start + 2)
        last = 2 * last_slot + own - start
        wanted = 2 * slots * k + jnp.where(hole, last, own - first_extra)
        valid = jnp.logical_or(hole, own >= first_extra)
        pick_extra[...] = jnp.where(jnp.logical_and(valid, at == wanted), 1.0, 0.0).astype(
            jnp.bfloat16
        )

    def drive_right():
        coefficient = (column - column_start) // 2
        degree = jnp.where(
            coefficient <= truncation - column_order, column_order + coefficient, coefficient - 1
        )
        lap_scale = (degree * (degree + 1)).astype(jnp.float32) / denom
        fetches[4].wait()
        fetches[5].wait()
        height = height_operator[...].astype(jnp.float32)
        pressure_row = jnp.broadcast_to(
            pressure_column[...].astype(jnp.float32).reshape(1, levels), height.shape
        )
        across = lax.broadcasted_iota(jnp.int32, height.shape, 1)
        down = lax.broadcasted_iota(jnp.int32, height.shape, 0)
        pressure_side = jnp.sum(
            jnp.where(across == down, pressure_row, 0.0), axis=1, keepdims=True
        )
        height = jnp.concatenate(
            [jnp.zeros((levels, tail), jnp.float32), height, pressure_side], axis=1
        ).astype(jnp.bfloat16)
        fetches[3].wait()
        drive = jnp.dot(height, state[LANES:, :], preferred_element_type=jnp.float32)
        right[0:levels, :] = (
            state[0:levels, :].astype(jnp.float32) + lap_scale * drive
        ).astype(jnp.bfloat16)

    with scope("drive"):
        drive_right()
    choose()
    with scope("rows_wait"):
        for t in range(1, 3):
            wait_row(groups[t])
    table = [low_rows[groups[t]][0:pairs] for t in range(3)]
    table += [jnp.broadcast_to(orders, (NEAR_ROWS - 3 * pairs, LANES))]
    info[w] = jnp.concatenate(table, axis=0)
    send_table(info, 0)
    with scope("row_far"):
        wait_row(groups[3])
    far_info[w] = low_rows[groups[3]]
    send_table(far_info, 1)

    @pl.when(middle)
    def _():
        with scope("relay_a"):
            relay_now((1, pairs), (1, 0), (2, pairs), (2, 0), (1, 1))

    with scope("info_wait"):
        all_tables(info, 0).wait_recv()

    def low_of(d, t, j):
        if t < 3:
            return info[d][t * pairs + j : t * pairs + j + 1]
        return far_info[d][j : j + 1]

    def target_of(b, k):
        d = peer(k)
        pair = lax.rem(lane_pair + block_pairs - lax.rem(k, block_pairs), block_pairs)
        low = jnp.zeros((1, LANES), jnp.int32)
        for p in range(block_pairs):
            low = jnp.where(pair == p, low_of(d, 2 * b + p // pairs, p % pairs), low)
        slot, member, order = lane_slot, lane_member, orders
        if b == 0:
            low = jnp.where(spare, low_of(d, 2, 0), low)
            slot = jnp.where(spare, last_slot, slot)
            member = jnp.where(spare, 1, member)
            order = jnp.where(spare, held[last_slot], order)
        merged = jnp.where(order <= low, low - order, truncation + 1 - low)
        position = jnp.where(member == 0, merged, truncation - low - order)
        used = order >= 0
        if b == 0:
            used = jnp.logical_and(used, lane < first_extra + 2)
        else:
            hole = jnp.logical_and(pair == 0, lax.rem(lane, per_pair) >= moved)
            extra = jnp.logical_or(spare, hole)
            position = jnp.where(extra, truncation + 1 - order, position)
        target = slot * slot_width + 2 * position + lane_part
        return jnp.where(used, target, -1)

    def build(b, i, place):
        at = lax.broadcasted_iota(jnp.int32, (width, LANES), 0)
        for h in range(2):
            pick[b, place, :, h * LANES : (h + 1) * LANES] = jnp.where(
                at == target_of(b, 2 * i + h), 1.0, 0.0
            ).astype(jnp.bfloat16)

    def place_of(i):
        return i if keep else 0

    def out_copy(b, k):
        return pltpu.make_async_remote_copy(
            src_ref=outgoing.at[b, k],
            dst_ref=arrived.at[b, k],
            send_sem=out_send.at[b],
            recv_sem=out_recv.at[b],
            device_id=(z, peer(k)),
            device_id_type=MESH,
        )

    def back_copy(b, k):
        return pltpu.make_async_remote_copy(
            src_ref=solved.at[b, k],
            dst_ref=returned.at[b, k],
            send_sem=back_send.at[b],
            recv_sem=back_recv.at[b, k // 2],
            device_id=(z, peer(k)),
            device_id_type=MESH,
        )

    def send_block(b, start, stop):
        def send(step, carry):
            i = W // 2 - 1 - step
            build(b, i, place_of(i))
            message = jnp.dot(
                right[...], pick[b, place_of(i)], preferred_element_type=jnp.float32
            ).astype(jnp.bfloat16)
            k0, k1 = 2 * i, 2 * i + 1
            outgoing[b, k0] = message[:, :LANES]
            outgoing[b, k1] = message[:, LANES:]

            @pl.when(i > 0)
            def _():
                out_copy(b, k0).start()

            out_copy(b, k1).start()
            return carry

        lax.fori_loop(start, stop, send, 0)

    def all_out(b):
        return pltpu.make_async_remote_copy(
            src_ref=outgoing.at[b, pl.ds(1, W - 1)],
            dst_ref=arrived.at[b, pl.ds(1, W - 1)],
            send_sem=out_send.at[b],
            recv_sem=out_recv.at[b],
            device_id=(z, peer(1)),
            device_id_type=MESH,
        )

    def some_back(b, first, count):
        return pltpu.make_async_remote_copy(
            src_ref=solved.at[b, pl.ds(first, count)],
            dst_ref=returned.at[b, pl.ds(first, count)],
            send_sem=back_send.at[b],
            recv_sem=back_recv.at[b, first // 2],
            device_id=(z, peer(1)),
            device_id_type=MESH,
        )

    with scope("send0"):
        send_block(0, 0, W // 4)
    with scope("relay_b"):
        relay((1, 2), (2, 1))
    with scope("send0b"):
        send_block(0, W // 4, W // 2)
    with scope("relay_c"):
        relay((2, 2), (3, pairs))
    with scope("far_wait"):
        all_tables(far_info, 1).wait_recv()
    with scope("send1"):
        send_block(1, 0, W // 4)
    with scope("relay_d"):
        relay((3, 0))
    with scope("send1b"):
        send_block(1, W // 4, W // 2)
    with scope("relay_e"):
        relay((3, 1))
    for b in range(2):
        arrived[b, 0] = outgoing[b, 0]

    def fill_edges(t):
        g = groups[t]
        edge = edges[g].astype(jnp.float32)
        across = edge.T
        for i in range(2 * pairs):
            at = i * tail
            side = across[:, border + at : border + at + tail]
            below = jnp.concatenate(
                [edge[at : at + tail], edge[2 * border : 2 * border + tail, at : at + tail]],
                axis=1,
            )
            matrices[g, i, 0:LANES, LANES:levels] = side.astype(jnp.bfloat16)
            matrices[g, i, LANES:levels, :] = below.astype(jnp.bfloat16)

    def spread(row):
        return jnp.concatenate([row] * tiles, axis=1)

    source_orders = [
        info[peer(k)][3 * pairs : 3 * pairs + 1] for k in range(W)
    ]

    def place(p, k):
        return lane_pair == (p + k) % block_pairs

    def pack(b, p):
        for v in range(tiles):
            first = v * block_pairs
            columns = arrived[b, first, 0:levels, :]
            order = source_orders[first]
            for k in range(first + 1, min(first + block_pairs, W)):
                columns = jnp.where(place(p, k), arrived[b, k, 0:levels, :], columns)
                order = jnp.where(place(p, k), source_orders[k], order)
            part = slice(v * LANES, (v + 1) * LANES)
            packed[b * block_pairs + p, 0:levels, part] = columns
            if b == 0:
                packed_orders[p : p + 1, part] = order

    wide_member = spread(lane_member)

    def times(t, j, member, x):
        return jnp.dot(
            matrices[groups[t], 2 * j + member], x, preferred_element_type=jnp.float32
        )

    def solve(b, p):
        t, j = 2 * b + p // pairs, p % pairs
        x = packed[b * block_pairs + p, 0:levels, :]
        low = spread(low_of(w, t, j))
        use_low = jnp.logical_and(wide_member == 0, packed_orders[p : p + 1, :] <= low)
        y = jnp.where(use_low, times(t, j, 0, x), times(t, j, 1, x))
        return y.astype(jnp.bfloat16)

    def deal(b, ps, answers, fresh):
        for k in range(W):
            v = k // block_pairs
            parts = [y[:, v * LANES : (v + 1) * LANES] for y in answers]
            block = parts[0] if fresh else solved[b, k]
            for p, part in list(zip(ps, parts))[1 if fresh else 0 :]:
                block = jnp.where(place(p, k), part, block)
            solved[b, k] = block

    def start_back(b):
        for k in range(W - 1, 0, -1):
            back_copy(b, k).start()

    def gather_spare(b, chosen):
        columns = jnp.concatenate([arrived[b, k, 0:levels, :] for k in range(W)], axis=1)
        return jnp.dot(columns, chosen[...], preferred_element_type=jnp.float32).astype(
            jnp.bfloat16
        )

    def scatter_spare(b, answer, chosen, where):
        back = lax.dot_general(
            answer, chosen[...], (((1,), (1,)), ((), ())), preferred_element_type=jnp.float32
        ).astype(jnp.bfloat16)
        for k in range(W):
            part = back[:, k * LANES : (k + 1) * LANES]
            solved[b, k] = jnp.where(where(k), part, solved[b, k])

    def is_extra(k):
        start = per_pair * (k % block_pairs) + moved
        return jnp.logical_or(spare, jnp.logical_and(lane >= start, lane < start + 2))

    extra_width = extra_in.shape[1]

    def along(row):
        return jnp.concatenate([row] * (extra_width // LANES), axis=1)

    extra_lane = lax.broadcasted_iota(jnp.int32, (1, extra_width), 1)
    extra_slot = lax.rem(extra_lane, 2 * slots) // 2
    extra_order = jnp.full((1, extra_width), -1, jnp.int32)
    for k in range(W):
        for s in range(slots):
            here = jnp.logical_and(extra_lane // (2 * slots) == k, extra_slot == s)
            value = source_orders[k][:, 2 * s : 2 * s + 1]
            extra_order = jnp.where(here, value, extra_order)

    def solve_extra(steps):
        x = extra_in[0:levels, :]
        y = extra_out[...]
        for t, j in steps:
            hit = extra_order == along(low_of(w, t, j))
            y = jnp.where(hit, times(t, j, 1, x).astype(jnp.bfloat16), y)
        extra_out[...] = y

    def late(ps):
        deal(1, ps, [solve(1, p) for p in ps], False)
        solve_extra([(2 + p // pairs, p % pairs) for p in ps])

    with scope("arrive1"):
        relay((3, 2))
        arrive((1, pairs), *[(1, c) for c in range(pairs)], (2, pairs))
    fill_edges(1)
    fill_edges(2)
    with scope("wait0"):
        all_out(0).wait_recv()
    with scope("pack0"):
        for p in range(block_pairs):
            pack(0, p)
    with scope("near"):
        every = list(range(block_pairs))
        deal(0, every, [solve(0, p) for p in every], True)
    with scope("arrive2"):
        arrive((2, 0))
    with scope("moved_back"):
        for k in range(W - 2, -1, -2):
            x = [arrived[0, k + h, 0:levels, :] for h in range(2)]
            y = times(2, 0, 1, jnp.concatenate(x, axis=1)).astype(jnp.bfloat16)
            for h in range(2):
                part = y[:, h * LANES : (h + 1) * LANES]
                solved[0, k + h] = jnp.where(spare, part, solved[0, k + h])
                if k + h > 0:
                    back_copy(0, k + h).start()
    with scope("edges3"):
        arrive((3, pairs))
        fill_edges(3)
    with scope("wait1"):
        all_out(1).wait_recv()
    with scope("pack1"):
        for p in range(block_pairs):
            pack(1, p)
        extra_in[0:levels, :] = gather_spare(1, pick_extra)
        extra_out[...] = jnp.zeros_like(extra_out)
    with scope("extra"):
        solve_extra([(t, j) for t in range(2) for j in range(pairs)])
    with scope("late2a"):
        deal(1, [0], [solve(1, 0)], True)
        solve_extra([(2, 0)])
    with scope("arrive2b"):
        arrive(*[(2, c) for c in range(1, pairs)])
    with scope("late2b"):
        late(list(range(1, pairs)))
    with scope("arrive3"):
        arrive(*[(3, c) for c in range(pairs - 1)])
    with scope("late3a"):
        late(list(range(pairs, block_pairs - 1)))
    with scope("arrive3b"):
        arrive((3, pairs - 1))
    with scope("late3b"):
        late([block_pairs - 1])
        scatter_spare(1, extra_out[...], pick_extra, is_extra)
        start_back(1)

    fetches[6].wait()
    fetches[7].wait()
    total[...] = jnp.zeros_like(total)
    through_row = lax.broadcasted_iota(jnp.int32, (tail, levels), 0)
    through_lane = lax.broadcasted_iota(jnp.int32, (tail, levels), 1)
    response = jnp.concatenate(
        [
            jnp.where(through_lane == through_row + LANES, -1.0, 0.0),
            thermal_response[...].astype(jnp.float32),
            mass_row[...].astype(jnp.float32).reshape(1, levels),
        ],
        axis=0,
    ).astype(jnp.bfloat16)

    def collect(b, i, first, second):
        if not keep:
            build(b, i, 0)
        total[...] += lax.dot_general(
            jnp.concatenate([first, second], axis=1),
            pick[b, place_of(i)],
            (((1,), (1,)), ((), ())),
            preferred_element_type=jnp.float32,
        )

    def gather_back(b):
        def step(n, carry):
            i = W // 2 - 1 - n
            some_back(b, 2 * i, 2).wait_recv()
            collect(b, i, returned[b, 2 * i], returned[b, 2 * i + 1])
            return carry

        with scope(f"back{b}"):
            lax.fori_loop(0, W // 2 - 1, step, 0)
        with scope(f"back{b}_0"):
            some_back(b, 1, 1).wait_recv()
            collect(b, 0, solved[b, 0], returned[b, 1])

    gather_back(0)
    gather_back(1)

    with scope("final"):
        div = total[0:levels, :].astype(jnp.bfloat16)
        change = jnp.dot(response, div, preferred_element_type=jnp.float32)
        old = state[LANES:, :].astype(jnp.float32)
        below = lax.broadcasted_iota(jnp.int32, old.shape, 0) < tail
        new = jnp.where(below, 0.0, old) - change
        new = jnp.where(column_order >= 0, new, 0.0)
        out[0:LANES, :] = div[0:LANES, :]
        out[LANES:, :] = new.astype(jnp.bfloat16)

    for b, table in ((0, info), (1, far_info)):
        all_out(b).wait_send()
        pltpu.make_async_remote_copy(
            src_ref=solved.at[b, pl.ds(1, W - 1)],
            dst_ref=returned.at[b, pl.ds(1, W - 1)],
            send_sem=back_send.at[b],
            recv_sem=back_recv.at[b, 0],
            device_id=(z, peer(1)),
            device_id_type=MESH,
        ).wait_send()
        all_tables(table, b).wait_send()
    pltpu.make_async_remote_copy(
        src_ref=low_rows.at[pl.ds(0, Z - 1)],
        dst_ref=low_rows.at[pl.ds(0, Z - 1)],
        send_sem=row_send,
        recv_sem=row_recv.at[1],
        device_id=(lax.rem(z + 1, Z), w),
        device_id_type=MESH,
    ).wait_send()

    def wait_relayed(count, way):
        for kind, ref in (
            (0, matrices.at[pl.ds(0, count), :, pl.ds(0, LANES), pl.ds(0, LANES)]),
            (1, edges.at[pl.ds(0, count)]),
        ):
            pltpu.make_async_remote_copy(
                src_ref=ref,
                dst_ref=ref,
                send_sem=z_send.at[kind, way],
                recv_sem=z_recv.at[0, 0],
                device_id=(lax.rem(z + 1, Z), w),
                device_id_type=MESH,
            ).wait_send()

    for zz in range(Z):

        @pl.when(z == zz)
        def _():
            if zz < Z - 1:
                wait_relayed(zz + 1, 0)
            if zz > 0:
                wait_relayed(Z - zz, 1)


def shards(
    state,
    held_orders,
    pair_lows,
    inverses,
    height_operator,
    pressure_column,
    thermal_response_matrix,
    mass_row,
):
    levels = height_operator.shape[0]
    slots = held_orders.shape[0]
    pairs = pair_lows.shape[0]
    Z, W = lax.axis_size("grp"), lax.axis_size("wave")
    width = state.shape[1]
    rows = ceil_to(levels, ROWS_TILE)
    places = W // 2 if W * width * 4 * LANES <= KEEP_BYTES else 1
    tiles = -(-W // (2 * pairs))
    extra_width = ceil_to(2 * slots * W, LANES)
    block = pltpu.VMEM((2, W, rows, LANES), jnp.bfloat16)
    return pl.pallas_call(
        functools.partial(kernel, (Z, W, levels, slots, pairs)),
        out_shape=pltpu.VMEM(state.shape, jnp.bfloat16),
        in_specs=[pl.BlockSpec(memory_space=pl.ANY)] * 8,
        out_specs=pl.BlockSpec(memory_space=pltpu.VMEM),
        scratch_shapes=[
            pltpu.SMEM(held_orders.shape, jnp.int32),
            pltpu.SMEM(pair_lows.shape, jnp.int32),
            pltpu.VMEM(state.shape, jnp.bfloat16),
            pltpu.VMEM((pairs, levels, 2, levels), jnp.bfloat16),
            pltpu.VMEM(height_operator.shape, jnp.bfloat16),
            pltpu.VMEM(pressure_column.shape, jnp.bfloat16),
            pltpu.VMEM(thermal_response_matrix.shape, jnp.bfloat16),
            pltpu.VMEM(mass_row.shape, jnp.bfloat16),
            pltpu.VMEM((Z, TABLE_ROWS, LANES), jnp.int32),
            pltpu.VMEM((W, NEAR_ROWS, LANES), jnp.int32),
            pltpu.VMEM((W, TABLE_ROWS, LANES), jnp.int32),
            pltpu.VMEM((Z, 2 * pairs, rows, levels), jnp.bfloat16),
            pltpu.VMEM((Z, LANES, LANES), jnp.bfloat16),
            pltpu.VMEM((rows, width), jnp.bfloat16),
            pltpu.VMEM((2, places, width, 2 * LANES), jnp.bfloat16),
            block,
            block,
            block,
            block,
            pltpu.VMEM((4 * pairs, rows, tiles * LANES), jnp.bfloat16),
            pltpu.VMEM((ceil_to(2 * pairs, TABLE_ROWS), tiles * LANES), jnp.int32),
            pltpu.VMEM((W * LANES, extra_width), jnp.bfloat16),
            pltpu.VMEM((rows, extra_width), jnp.bfloat16),
            pltpu.VMEM((rows, extra_width), jnp.bfloat16),
            pltpu.VMEM((rows, width), jnp.float32),
            pltpu.SemaphoreType.DMA,
            pltpu.SemaphoreType.DMA((Z,)),
            pltpu.SemaphoreType.DMA((2,)),
            pltpu.SemaphoreType.DMA((2,)),
            pltpu.SemaphoreType.DMA((2, 2)),
            pltpu.SemaphoreType.DMA((Z, pairs + 1)),
            pltpu.SemaphoreType.DMA((2,)),
            pltpu.SemaphoreType.DMA((2,)),
            pltpu.SemaphoreType.DMA((2,)),
            pltpu.SemaphoreType.DMA((2, W // 2)),
            pltpu.SemaphoreType.DMA((8,)),
        ],
        compiler_params=pltpu.CompilerParams(
            collective_id=0, has_side_effects=True, vmem_limit_bytes=52 * 1024 * 1024
        ),
    )(
        *[
            pltpu.with_memory_space_constraint(array, pltpu.HBM)
            for array in (
                held_orders,
                pair_lows,
                state,
                jnp.transpose(inverses, (0, 2, 1, 3)),
                height_operator,
                pressure_column,
                thermal_response_matrix,
                mass_row,
            )
        ]
    )


def solution(mesh):
    placed = (
        P(None, ("grp", "wave")),
        P(("grp", "wave")),
        P(("grp", "wave")),
        P(("grp", "wave"), None, None, None),
        P(),
        P(),
        P(),
        P(),
    )
    return jax.shard_map(
        shards, mesh=mesh, in_specs=placed, out_specs=P(None, ("grp", "wave")), check_vma=False
    )
```

```python
import functools

import jax
import jax.numpy as jnp
from jax import lax
from jax.experimental import pallas as pl
from jax.experimental.pallas import tpu as pltpu
from jax.sharding import PartitionSpec as P

MESH = pl.DeviceIdType.MESH
LANES = 128
ROWS_TILE = 16
TABLE_ROWS = 8
NEAR_ROWS = 16
CHUNK = 256
KEEP_BYTES = 24 << 20
scope = jax.named_scope


def ceil_to(value, step):
    return -(-value // step) * step


def kernel(
    size,
    held_far,
    lows_far,
    state_far,
    inverses_far,
    height_far,
    pressure_far,
    thermal_far,
    mass_far,
    out,
    held,
    lows,
    state,
    inverses,
    height_operator,
    pressure_column,
    thermal_response,
    mass_row,
    low_rows,
    info,
    far_info,
    matrices,
    edges,
    right,
    pick,
    outgoing,
    arrived,
    solved,
    returned,
    packed,
    packed_orders,
    pick_extra,
    extra_in,
    put_extra,
    last_pick,
    total,
    row_send,
    row_recv,
    info_send,
    info_recv,
    z_send,
    z_recv,
    out_send,
    out_recv,
    back_send,
    back_recv,
    fetch_sem,
):
    Z, W, levels, slots, pairs = size
    half_count = Z * W * pairs
    truncation = 2 * half_count - 1
    slot_width = 2 * (truncation + 2)
    width = slots * slot_width
    denom = float(truncation * (truncation + 1))
    per_pair = 4 * slots
    block_pairs = 2 * pairs
    first_extra = block_pairs * per_pair
    moved = per_pair - 2
    tiles = packed.shape[2] // LANES
    last_slot = slots - 1
    tail = levels - LANES
    border = 2 * pairs * tail
    keep = pick.shape[1] > 1
    z = lax.axis_index("grp")
    w = lax.axis_index("wave")
    middle = jnp.logical_and(z > 0, z < Z - 1)

    barrier = pltpu.get_barrier_semaphore()

    def peer(k):
        other = 0
        for i in range(W.bit_length() - 1):
            mine, flip = lax.rem(w // (1 << i), 2), lax.rem(k // (1 << i), 2)
            other = other + (1 << i) * (mine + flip - 2 * mine * flip)
        return other

    def greet(k, carry):
        pl.semaphore_signal(barrier, inc=1, device_id=(z, peer(k)), device_id_type=MESH)
        return carry

    fetches = [
        pltpu.make_async_copy(far, near, fetch_sem.at[i])
        for i, (far, near) in enumerate(
            [
                (lows_far, lows),
                (held_far, held),
                (inverses_far, inverses),
                (state_far, state),
                (height_far, height_operator),
                (pressure_far, pressure_column),
                (thermal_far, thermal_response),
                (mass_far, mass_row),
            ]
        )
    ]
    for k in range(1, Z):
        pl.semaphore_signal(barrier, inc=1, device_id=(lax.rem(z + k, Z), w), device_id_type=MESH)
    for fetch in fetches[:3]:
        fetch.start()
    lax.fori_loop(1, W, greet, 0)
    for fetch in fetches[3:]:
        fetch.start()

    lane = lax.broadcasted_iota(jnp.int32, (1, LANES), 1)
    lane_pair = lane // per_pair
    lane_member = lax.rem(lane, per_pair) // (2 * slots)
    lane_slot = lax.rem(lax.rem(lane, per_pair), 2 * slots) // 2
    lane_part = lax.rem(lane, 2)
    spare = lane >= first_extra
    table_row = lax.broadcasted_iota(jnp.int32, (TABLE_ROWS, LANES), 0)
    with scope("small_fetch"):
        fetches[0].wait()
        fetches[1].wait()
    orders = jnp.full((1, LANES), -1, jnp.int32)
    for s in range(slots):
        orders = jnp.where(lane_slot == s, held[s], orders)
    low_tile = jnp.zeros((TABLE_ROWS, LANES), jnp.int32)
    for j in range(pairs):
        low_tile = jnp.where(table_row == j, lows[j], low_tile)
    low_rows[z] = low_tile

    rows = matrices.shape[2]

    def split_inverses():
        fetches[2].wait()
        to_row = lax.broadcasted_iota(jnp.int32, (2 * rows, 2 * levels), 0)
        from_row = lax.broadcasted_iota(jnp.int32, (2 * rows, 2 * levels), 1)
        wanted = jnp.where(to_row < rows, 2 * to_row, 2 * (to_row - rows) + 1)
        split = jnp.where(wanted == from_row, 1.0, 0.0).astype(jnp.bfloat16)
        parts = []
        for j in range(pairs):
            both = jnp.dot(
                split,
                inverses[j].reshape(2 * levels, levels),
                preferred_element_type=jnp.float32,
            )
            for member in range(2):
                matrix = both[member * rows : (member + 1) * rows]
                matrices[z, 2 * j + member] = matrix.astype(jnp.bfloat16)
                parts.append(matrix)
        blank = jnp.zeros((LANES, LANES - border), jnp.float32)
        under = [matrix[LANES:levels, 0:LANES] for matrix in parts]
        aside = jnp.concatenate([m[0:LANES, LANES:levels] for m in parts] + [blank], axis=1)
        corner = [m[LANES:levels, LANES:levels] for m in parts] + [blank[0:tail]]
        corner = jnp.concatenate(corner, axis=1)
        filler = jnp.zeros((LANES - 2 * border - tail, LANES), jnp.float32)
        edge = jnp.concatenate([*under, aside.T[0:border], corner, filler], axis=0)
        edges[z] = edge.astype(jnp.bfloat16)

    @pl.when(z < Z - 1)
    def _():
        with scope("split"):
            split_inverses()

    with scope("barrier"):
        pl.semaphore_wait(barrier, W + Z - 2)

    def z_copy(g, c, way):
        if c < pairs:
            ref = matrices.at[g, pl.ds(2 * c, 2), pl.ds(0, LANES), pl.ds(0, LANES)]
        else:
            ref = edges.at[g]
        step = 1 if way == 0 else -1
        return pltpu.make_async_remote_copy(
            src_ref=ref,
            dst_ref=ref,
            send_sem=z_send.at[0 if c < pairs else 1, way],
            recv_sem=z_recv.at[g, c],
            device_id=(z + step, w),
            device_id_type=MESH,
        )

    def forward(g, c):
        @pl.when(jnp.logical_and(g <= z, z < Z - 1))
        def _():
            z_copy(g, c, 0).start()

        @pl.when(jnp.logical_and(g >= z, z > 0))
        def _():
            z_copy(g, c, 1).start()

    def group_at(t):
        g = z
        for zz in range(Z):
            by_distance = sorted(range(Z), key=lambda a: (abs(a - zz), abs(2 * a - Z + 1)))
            g = jnp.where(z == zz, by_distance[t], g)
        return g

    def relay_now(*steps):
        for t, c in steps:
            g = group_at(t)
            z_copy(g, c, 0).wait_recv()
            forward(g, c)

    def relay(*steps):
        @pl.when(middle)
        def _():
            relay_now(*steps)

    def arrive(*steps):
        @pl.when(jnp.logical_not(middle))
        def _():
            for t, c in steps:
                z_copy(group_at(t), c, 0).wait_recv()

    groups = [group_at(t) for t in range(Z)]

    def row_copy(g):
        return pltpu.make_async_remote_copy(
            src_ref=low_rows.at[z],
            dst_ref=low_rows.at[z],
            send_sem=row_send,
            recv_sem=row_recv.at[z],
            device_id=(g, w),
            device_id_type=MESH,
        )

    def send_rows(distance):
        for step in (-distance, distance):

            @pl.when(jnp.logical_and(z + step >= 0, z + step < Z))
            def _():
                row_copy(z + step).start()

    def wait_row(g):
        pltpu.make_async_remote_copy(
            src_ref=low_rows.at[g],
            dst_ref=low_rows.at[g],
            send_sem=row_send,
            recv_sem=row_recv.at[g],
            device_id=(g, w),
            device_id_type=MESH,
        ).wait_recv()

    def table_copy(table, b, k):
        return pltpu.make_async_remote_copy(
            src_ref=table.at[w],
            dst_ref=table.at[w],
            send_sem=info_send.at[b],
            recv_sem=info_recv.at[b],
            device_id=(z, peer(k)),
            device_id_type=MESH,
        )

    def send_table(table, b):
        def start(n, carry):
            table_copy(table, b, W - n).start()
            return carry

        lax.fori_loop(1, W, start, 0)

    def all_tables(table, b):
        return pltpu.make_async_remote_copy(
            src_ref=table.at[pl.ds(0, W - 1)],
            dst_ref=table.at[pl.ds(0, W - 1)],
            send_sem=info_send.at[b],
            recv_sem=info_recv.at[b],
            device_id=(z, peer(1)),
            device_id_type=MESH,
        )

    for distance in range(1, Z):
        send_rows(distance)

    @pl.when(z == Z - 1)
    def _():
        with scope("split_end"):
            split_inverses()

    for c in [pairs, *range(pairs)]:
        forward(z, c)

    column = lax.broadcasted_iota(jnp.int32, (1, width), 1)
    column_order = jnp.full((1, width), -1, jnp.int32)
    column_start = jnp.zeros((1, width), jnp.int32)
    for s in range(slots):
        inside = jnp.logical_and(column >= s * slot_width, column < (s + 1) * slot_width)
        column_order = jnp.where(inside, held[s], column_order)
        column_start = jnp.where(inside, s * slot_width, column_start)

    def choose():
        for ref, dimension in ((pick_extra, 0), (put_extra, 1)):
            row = lax.broadcasted_iota(jnp.int32, ref.shape, dimension)
            at = lax.broadcasted_iota(jnp.int32, ref.shape, 1 - dimension)
            k, own = row // LANES, lax.rem(row, LANES)
            start = per_pair * lax.rem(k, block_pairs) + moved
            hole = jnp.logical_and(own >= start, own < start + 2)
            last = 2 * last_slot + own - start
            wanted = 2 * slots * k + jnp.where(hole, last, own - first_extra)
            valid = jnp.logical_or(hole, own >= first_extra)
            ref[...] = jnp.where(jnp.logical_and(valid, at == wanted), 1.0, 0.0).astype(
                jnp.bfloat16
            )

    def drive_right():
        coefficient = (column - column_start) // 2
        degree = jnp.where(
            coefficient <= truncation - column_order, column_order + coefficient, coefficient - 1
        )
        lap_scale = (degree * (degree + 1)).astype(jnp.float32) / denom
        fetches[4].wait()
        fetches[5].wait()
        height = height_operator[...].astype(jnp.float32)
        pressure_row = jnp.broadcast_to(
            pressure_column[...].astype(jnp.float32).reshape(1, levels), height.shape
        )
        across = lax.broadcasted_iota(jnp.int32, height.shape, 1)
        down = lax.broadcasted_iota(jnp.int32, height.shape, 0)
        pressure_side = jnp.sum(
            jnp.where(across == down, pressure_row, 0.0), axis=1, keepdims=True
        )
        height = jnp.concatenate(
            [jnp.zeros((levels, tail), jnp.float32), height, pressure_side], axis=1
        ).astype(jnp.bfloat16)
        fetches[3].wait()
        drive = jnp.dot(height, state[LANES:, :], preferred_element_type=jnp.float32)
        right[0:levels, :] = (
            state[0:levels, :].astype(jnp.float32) + lap_scale * drive
        ).astype(jnp.bfloat16)

    with scope("drive"):
        drive_right()
    choose()
    with scope("rows_wait"):
        for t in range(1, 3):
            wait_row(groups[t])
    table = [low_rows[groups[t]][0:pairs] for t in range(3)]
    table += [jnp.broadcast_to(orders, (NEAR_ROWS - 3 * pairs, LANES))]
    info[w] = jnp.concatenate(table, axis=0)
    send_table(info, 0)
    with scope("row_far"):
        wait_row(groups[3])
    far_info[w] = low_rows[groups[3]]
    send_table(far_info, 1)

    @pl.when(middle)
    def _():
        with scope("relay_a"):
            relay_now((1, pairs), (1, 0), (2, pairs), (2, 0), (1, 1))

    with scope("info_wait"):
        all_tables(info, 0).wait_recv()

    def low_of(d, t, j):
        if t < 3:
            return info[d][t * pairs + j : t * pairs + j + 1]
        return far_info[d][j : j + 1]

    def target_of(b, k):
        d = peer(k)
        pair = lax.rem(lane_pair + block_pairs - lax.rem(k, block_pairs), block_pairs)
        low = jnp.zeros((1, LANES), jnp.int32)
        for p in range(block_pairs):
            low = jnp.where(pair == p, low_of(d, 2 * b + p // pairs, p % pairs), low)
        slot, member, order = lane_slot, lane_member, orders
        if b == 0:
            low = jnp.where(spare, low_of(d, 2, 0), low)
            slot = jnp.where(spare, last_slot, slot)
            member = jnp.where(spare, 1, member)
            order = jnp.where(spare, held[last_slot], order)
        merged = jnp.where(order <= low, low - order, truncation + 1 - low)
        position = jnp.where(member == 0, merged, truncation - low - order)
        used = order >= 0
        if b == 0:
            used = jnp.logical_and(used, lane < first_extra + 2)
        else:
            hole = jnp.logical_and(pair == 0, lax.rem(lane, per_pair) >= moved)
            extra = jnp.logical_or(spare, hole)
            position = jnp.where(extra, truncation + 1 - order, position)
        target = slot * slot_width + 2 * position + lane_part
        return jnp.where(used, target, -1)

    def build(b, i, place):
        at = lax.broadcasted_iota(jnp.int32, (width, LANES), 0)
        for h in range(2):
            pick[b, place, :, h * LANES : (h + 1) * LANES] = jnp.where(
                at == target_of(b, 2 * i + h), 1.0, 0.0
            ).astype(jnp.bfloat16)

    def place_of(i):
        return i if keep else 0

    def out_copy(b, k):
        return pltpu.make_async_remote_copy(
            src_ref=outgoing.at[b, k],
            dst_ref=arrived.at[b, k],
            send_sem=out_send.at[b],
            recv_sem=out_recv.at[b],
            device_id=(z, peer(k)),
            device_id_type=MESH,
        )

    def back_copy(b, k):
        return pltpu.make_async_remote_copy(
            src_ref=solved.at[b, k],
            dst_ref=returned.at[b, k],
            send_sem=back_send.at[b],
            recv_sem=back_recv.at[b, k // 2],
            device_id=(z, peer(k)),
            device_id_type=MESH,
        )

    def send_block(b, first, stop):
        def send(step, carry):
            i = W // 2 - 1 - step
            targets = jnp.concatenate([target_of(b, 2 * i), target_of(b, 2 * i + 1)], axis=1)
            message = jnp.zeros((rows, 2 * LANES), jnp.float32)
            for start in range(0, width, CHUNK):
                count = min(CHUNK, width - start)
                at = lax.broadcasted_iota(jnp.int32, (count, 2 * LANES), 0) + start
                chosen = jnp.where(at == targets, 1.0, 0.0).astype(jnp.bfloat16)
                pick[b, place_of(i), start : start + count, :] = chosen
                message += jnp.dot(
                    right[:, start : start + count], chosen, preferred_element_type=jnp.float32
                )
            message = message.astype(jnp.bfloat16)
            k0, k1 = 2 * i, 2 * i + 1
            outgoing[b, k0] = message[:, :LANES]
            outgoing[b, k1] = message[:, LANES:]

            @pl.when(i > 0)
            def _():
                out_copy(b, k0).start()

            out_copy(b, k1).start()
            return carry

        lax.fori_loop(first, stop, send, 0)

    def all_out(b):
        return pltpu.make_async_remote_copy(
            src_ref=outgoing.at[b, pl.ds(1, W - 1)],
            dst_ref=arrived.at[b, pl.ds(1, W - 1)],
            send_sem=out_send.at[b],
            recv_sem=out_recv.at[b],
            device_id=(z, peer(1)),
            device_id_type=MESH,
        )

    def some_back(b, first, count):
        return pltpu.make_async_remote_copy(
            src_ref=solved.at[b, pl.ds(first, count)],
            dst_ref=returned.at[b, pl.ds(first, count)],
            send_sem=back_send.at[b],
            recv_sem=back_recv.at[b, first // 2],
            device_id=(z, peer(1)),
            device_id_type=MESH,
        )

    with scope("send0"):
        send_block(0, 0, W // 4)
    with scope("relay_b"):
        relay((1, 2), (2, 1))
    with scope("send0b"):
        send_block(0, W // 4, W // 2)
    with scope("relay_c"):
        relay((2, 2), (3, pairs))
    with scope("far_wait"):
        all_tables(far_info, 1).wait_recv()
    with scope("send1"):
        send_block(1, 0, W // 4)
    with scope("relay_d"):
        relay((3, 0))
    with scope("send1b"):
        send_block(1, W // 4, W // 2)
    with scope("relay_e"):
        relay((3, 1))
    for b in range(2):
        arrived[b, 0] = outgoing[b, 0]

    def fill_edges(t):
        g = groups[t]
        edge = edges[g].astype(jnp.float32)
        across = edge.T
        for i in range(2 * pairs):
            at = i * tail
            side = across[:, border + at : border + at + tail]
            below = jnp.concatenate(
                [edge[at : at + tail], edge[2 * border : 2 * border + tail, at : at + tail]],
                axis=1,
            )
            matrices[g, i, 0:LANES, LANES:levels] = side.astype(jnp.bfloat16)
            matrices[g, i, LANES:levels, :] = below.astype(jnp.bfloat16)

    def spread(row):
        return jnp.concatenate([row] * tiles, axis=1)

    source_orders = [
        info[peer(k)][3 * pairs : 3 * pairs + 1] for k in range(W)
    ]

    def place(p, k):
        return lane_pair == (p + k) % block_pairs

    def pack(b, p):
        for v in range(tiles):
            first = v * block_pairs
            columns = arrived[b, first, 0:levels, :]
            order = source_orders[first]
            for k in range(first + 1, min(first + block_pairs, W)):
                columns = jnp.where(place(p, k), arrived[b, k, 0:levels, :], columns)
                order = jnp.where(place(p, k), source_orders[k], order)
            part = slice(v * LANES, (v + 1) * LANES)
            packed[b * block_pairs + p, 0:levels, part] = columns
            if b == 0:
                packed_orders[p : p + 1, part] = order

    wide_member = spread(lane_member)

    def times(t, j, member, x):
        return jnp.dot(
            matrices[groups[t], 2 * j + member], x, preferred_element_type=jnp.float32
        )

    def solve(b, p):
        t, j = 2 * b + p // pairs, p % pairs
        x = packed[b * block_pairs + p, 0:levels, :]
        low = spread(low_of(w, t, j))
        use_low = jnp.logical_and(wide_member == 0, packed_orders[p : p + 1, :] <= low)
        y = jnp.where(use_low, times(t, j, 0, x), times(t, j, 1, x))
        return y.astype(jnp.bfloat16)

    def deal(answers, k):
        part = slice(k // block_pairs * LANES, (k // block_pairs + 1) * LANES)
        block = answers[0][:, part]
        for p in range(1, block_pairs):
            block = jnp.where(place(p, k), answers[p][:, part], block)
        return block

    def gather_extra():
        columns = jnp.concatenate([arrived[1, k, 0:levels, :] for k in range(W)], axis=1)
        return jnp.dot(columns, pick_extra[...], preferred_element_type=jnp.float32).astype(
            jnp.bfloat16
        )

    def is_extra(k):
        start = per_pair * (k % block_pairs) + moved
        return jnp.logical_or(spare, jnp.logical_and(lane >= start, lane < start + 2))

    extra_width = extra_in.shape[1]

    def along(row):
        return jnp.concatenate([row] * (extra_width // LANES), axis=1)

    extra_lane = lax.broadcasted_iota(jnp.int32, (1, extra_width), 1)
    extra_slot = lax.rem(extra_lane, 2 * slots) // 2
    extra_order = jnp.full((1, extra_width), -1, jnp.int32)
    for k in range(W):
        for s in range(slots):
            here = jnp.logical_and(extra_lane // (2 * slots) == k, extra_slot == s)
            value = source_orders[k][:, 2 * s : 2 * s + 1]
            extra_order = jnp.where(here, value, extra_order)

    def solve_extra(y, steps):
        x = extra_in[0:levels, :]
        for t, j in steps:
            hit = extra_order == along(low_of(w, t, j))
            y = jnp.where(hit, times(t, j, 1, x).astype(jnp.bfloat16), y)
        return y

    with scope("arrive1"):
        relay((3, 2))
        arrive((1, pairs), *[(1, c) for c in range(pairs)], (2, pairs))
    fill_edges(1)
    fill_edges(2)
    with scope("wait0"):
        all_out(0).wait_recv()
    with scope("pack0"):
        for p in range(block_pairs):
            pack(0, p)
    with scope("near"):
        answers = [solve(0, p) for p in range(block_pairs)]
        for k in range(W):
            solved[0, k] = deal(answers, k)
    with scope("arrive2"):
        arrive((2, 0))
    with scope("moved_back"):
        for k in range(W - 2, -1, -2):
            x = [arrived[0, k + h, 0:levels, :] for h in range(2)]
            y = times(2, 0, 1, jnp.concatenate(x, axis=1)).astype(jnp.bfloat16)
            for h in range(2):
                part = y[:, h * LANES : (h + 1) * LANES]
                solved[0, k + h] = jnp.where(spare, part, solved[0, k + h])
                if k + h > 0:
                    back_copy(0, k + h).start()
    with scope("edges3"):
        arrive((3, pairs))
        fill_edges(3)
    with scope("wait1"):
        all_out(1).wait_recv()
    with scope("arrive2"):
        arrive(*[(2, c) for c in range(1, pairs)], *[(3, c) for c in range(pairs - 1)])
    with scope("pack1"):
        extra_in[0:levels, :] = gather_extra()
        for p in range(block_pairs):
            pack(1, p)
    with scope("late"):
        answers = [solve(1, p) for p in range(block_pairs - 1)]
        steps = [(t, j) for t in range(Z) for j in range(pairs)]
        extra = jnp.zeros(extra_in.shape, jnp.bfloat16)
        extra = solve_extra(extra, steps[:-1])
    with scope("arrive3"):
        arrive((3, pairs - 1))
    with scope("last"):
        extra = solve_extra(extra, steps[-1:])
        answers.append(solve(1, block_pairs - 1))
        extra_back = jnp.dot(
            extra, put_extra[...], preferred_element_type=jnp.float32
        ).astype(jnp.bfloat16)
        for k in range(W - 1, -1, -1):
            block = deal(answers, k)
            solved[1, k] = jnp.where(
                is_extra(k), extra_back[:, k * LANES : (k + 1) * LANES], block
            )
            if k > 0:
                back_copy(1, k).start()

    fetches[6].wait()
    fetches[7].wait()
    total[...] = jnp.zeros_like(total)
    through_row = lax.broadcasted_iota(jnp.int32, (tail, levels), 0)
    through_lane = lax.broadcasted_iota(jnp.int32, (tail, levels), 1)
    response = jnp.concatenate(
        [
            jnp.where(through_lane == through_row + LANES, -1.0, 0.0),
            thermal_response[...].astype(jnp.float32),
            mass_row[...].astype(jnp.float32).reshape(1, levels),
        ],
        axis=0,
    ).astype(jnp.bfloat16)

    def collect(b, i, first, second):
        if not keep:
            build(b, i, 0)
        total[...] += lax.dot_general(
            jnp.concatenate([first, second], axis=1),
            pick[b, place_of(i)],
            (((1,), (1,)), ((), ())),
            preferred_element_type=jnp.float32,
        )

    def gather_back(b):
        def step(n, carry):
            i = W // 2 - 1 - n
            some_back(b, 2 * i, 2).wait_recv()
            collect(b, i, returned[b, 2 * i], returned[b, 2 * i + 1])
            return carry

        with scope(f"back{b}"):
            lax.fori_loop(0, W // 2 - 1, step, 0)
        with scope(f"back{b}_0"):
            some_back(b, 1, 1).wait_recv()
            if b == 0:
                collect(b, 0, solved[b, 0], returned[b, 1])
            else:
                total[...] += jnp.dot(
                    jnp.concatenate([solved[b, 0], returned[b, 1]], axis=1),
                    last_pick[...],
                    preferred_element_type=jnp.float32,
                )

    gather_back(0)
    with scope("last_pick"):
        targets = jnp.concatenate([target_of(1, 0), target_of(1, 1)], axis=1)
        targets = jnp.broadcast_to(targets.astype(jnp.float32), (TABLE_ROWS, 2 * LANES))
        targets = targets.T[:, 0:1].astype(jnp.int32)
        at = lax.broadcasted_iota(jnp.int32, (2 * LANES, width), 1)
        last_pick[...] = jnp.where(at == targets, 1.0, 0.0).astype(jnp.bfloat16)
    gather_back(1)

    with scope("final"):
        div = total[0:levels, :].astype(jnp.bfloat16)
        change = jnp.dot(response, div, preferred_element_type=jnp.float32)
        old = state[LANES:, :].astype(jnp.float32)
        below = lax.broadcasted_iota(jnp.int32, old.shape, 0) < tail
        new = jnp.where(below, 0.0, old) - change
        new = jnp.where(column_order >= 0, new, 0.0)
        out[0:LANES, :] = div[0:LANES, :]
        out[LANES:, :] = new.astype(jnp.bfloat16)

    for b, table in ((0, info), (1, far_info)):
        all_out(b).wait_send()
        pltpu.make_async_remote_copy(
            src_ref=solved.at[b, pl.ds(1, W - 1)],
            dst_ref=returned.at[b, pl.ds(1, W - 1)],
            send_sem=back_send.at[b],
            recv_sem=back_recv.at[b, 0],
            device_id=(z, peer(1)),
            device_id_type=MESH,
        ).wait_send()
        all_tables(table, b).wait_send()
    pltpu.make_async_remote_copy(
        src_ref=low_rows.at[pl.ds(0, Z - 1)],
        dst_ref=low_rows.at[pl.ds(0, Z - 1)],
        send_sem=row_send,
        recv_sem=row_recv.at[1],
        device_id=(lax.rem(z + 1, Z), w),
        device_id_type=MESH,
    ).wait_send()

    def wait_relayed(count, way):
        for kind, ref in (
            (0, matrices.at[pl.ds(0, count), :, pl.ds(0, LANES), pl.ds(0, LANES)]),
            (1, edges.at[pl.ds(0, count)]),
        ):
            pltpu.make_async_remote_copy(
                src_ref=ref,
                dst_ref=ref,
                send_sem=z_send.at[kind, way],
                recv_sem=z_recv.at[0, 0],
                device_id=(lax.rem(z + 1, Z), w),
                device_id_type=MESH,
            ).wait_send()

    for zz in range(Z):

        @pl.when(z == zz)
        def _():
            if zz < Z - 1:
                wait_relayed(zz + 1, 0)
            if zz > 0:
                wait_relayed(Z - zz, 1)


def shards(
    state,
    held_orders,
    pair_lows,
    inverses,
    height_operator,
    pressure_column,
    thermal_response_matrix,
    mass_row,
):
    levels = height_operator.shape[0]
    slots = held_orders.shape[0]
    pairs = pair_lows.shape[0]
    Z, W = lax.axis_size("grp"), lax.axis_size("wave")
    width = state.shape[1]
    rows = ceil_to(levels, ROWS_TILE)
    places = W // 2 if W * width * 4 * LANES <= KEEP_BYTES else 1
    tiles = -(-W // (2 * pairs))
    extra_width = ceil_to(2 * slots * W, LANES)
    block = pltpu.VMEM((2, W, rows, LANES), jnp.bfloat16)
    return pl.pallas_call(
        functools.partial(kernel, (Z, W, levels, slots, pairs)),
        out_shape=pltpu.VMEM(state.shape, jnp.bfloat16),
        in_specs=[pl.BlockSpec(memory_space=pl.ANY)] * 8,
        out_specs=pl.BlockSpec(memory_space=pltpu.VMEM),
        scratch_shapes=[
            pltpu.SMEM(held_orders.shape, jnp.int32),
            pltpu.SMEM(pair_lows.shape, jnp.int32),
            pltpu.VMEM(state.shape, jnp.bfloat16),
            pltpu.VMEM((pairs, levels, 2, levels), jnp.bfloat16),
            pltpu.VMEM(height_operator.shape, jnp.bfloat16),
            pltpu.VMEM(pressure_column.shape, jnp.bfloat16),
            pltpu.VMEM(thermal_response_matrix.shape, jnp.bfloat16),
            pltpu.VMEM(mass_row.shape, jnp.bfloat16),
            pltpu.VMEM((Z, TABLE_ROWS, LANES), jnp.int32),
            pltpu.VMEM((W, NEAR_ROWS, LANES), jnp.int32),
            pltpu.VMEM((W, TABLE_ROWS, LANES), jnp.int32),
            pltpu.VMEM((Z, 2 * pairs, rows, levels), jnp.bfloat16),
            pltpu.VMEM((Z, LANES, LANES), jnp.bfloat16),
            pltpu.VMEM((rows, width), jnp.bfloat16),
            pltpu.VMEM((2, places, width, 2 * LANES), jnp.bfloat16),
            block,
            block,
            block,
            block,
            pltpu.VMEM((4 * pairs, rows, tiles * LANES), jnp.bfloat16),
            pltpu.VMEM((ceil_to(2 * pairs, TABLE_ROWS), tiles * LANES), jnp.int32),
            pltpu.VMEM((W * LANES, extra_width), jnp.bfloat16),
            pltpu.VMEM((rows, extra_width), jnp.bfloat16),
            pltpu.VMEM((extra_width, W * LANES), jnp.bfloat16),
            pltpu.VMEM((2 * LANES, width), jnp.bfloat16),
            pltpu.VMEM((rows, width), jnp.float32),
            pltpu.SemaphoreType.DMA,
            pltpu.SemaphoreType.DMA((Z,)),
            pltpu.SemaphoreType.DMA((2,)),
            pltpu.SemaphoreType.DMA((2,)),
            pltpu.SemaphoreType.DMA((2, 2)),
            pltpu.SemaphoreType.DMA((Z, pairs + 1)),
            pltpu.SemaphoreType.DMA((2,)),
            pltpu.SemaphoreType.DMA((2,)),
            pltpu.SemaphoreType.DMA((2,)),
            pltpu.SemaphoreType.DMA((2, W // 2)),
            pltpu.SemaphoreType.DMA((8,)),
        ],
        compiler_params=pltpu.CompilerParams(
            collective_id=0, has_side_effects=True, vmem_limit_bytes=58 * 1024 * 1024
        ),
    )(
        *[
            pltpu.with_memory_space_constraint(array, pltpu.HBM)
            for array in (
                held_orders,
                pair_lows,
                state,
                jnp.transpose(inverses, (0, 2, 1, 3)),
                height_operator,
                pressure_column,
                thermal_response_matrix,
                mass_row,
            )
        ]
    )


def solution(mesh):
    placed = (
        P(None, ("grp", "wave")),
        P(("grp", "wave")),
        P(("grp", "wave")),
        P(("grp", "wave"), None, None, None),
        P(),
        P(),
        P(),
        P(),
    )
    return jax.shard_map(
        shards, mesh=mesh, in_specs=placed, out_specs=P(None, ("grp", "wave")), check_vma=False
    )
```

```python
import functools

import jax
import jax.numpy as jnp
from jax import lax
from jax.experimental import pallas as pl
from jax.experimental.pallas import tpu as pltpu
from jax.sharding import PartitionSpec as P

MESH = pl.DeviceIdType.MESH
LANES = 128
ROWS_TILE = 16
TABLE_ROWS = 8
CHUNK = 256
KEEP_BYTES = 24 << 20
scope = jax.named_scope


def ceil_to(value, step):
    return -(-value // step) * step


def kernel(
    size,
    held_far,
    lows_far,
    state_far,
    inverses_far,
    height_far,
    pressure_far,
    thermal_far,
    mass_far,
    out,
    held,
    lows,
    state,
    inverses,
    height_operator,
    pressure_column,
    thermal_response,
    mass_row,
    low_rows,
    info,
    far_info,
    matrices,
    edges,
    right,
    pick,
    outgoing,
    arrived,
    solved,
    returned,
    packed,
    packed_orders,
    pick_extra,
    extra_in,
    put_extra,
    last_pick,
    total,
    row_send,
    row_recv,
    info_send,
    info_recv,
    z_send,
    z_recv,
    out_send,
    out_recv,
    back_send,
    back_recv,
    fetch_sem,
    known,
):
    Z, W, levels, slots, pairs = size
    half_count = Z * W * pairs
    truncation = 2 * half_count - 1
    slot_width = 2 * (truncation + 2)
    width = slots * slot_width
    rows = solved.shape[2]
    denom = float(truncation * (truncation + 1))
    per_pair = 4 * slots
    block_pairs = 2 * pairs
    first_extra = block_pairs * per_pair
    fold = rows - levels
    spans = -(-levels // fold)
    tiles = packed.shape[2] // LANES
    last_slot = slots - 1
    stages = W.bit_length() - 1
    rounds = max(stages, Z - 1)
    tail = levels - LANES
    border = 2 * pairs * tail
    keep = pick.shape[1] > 1
    z = lax.axis_index("grp")
    w = lax.axis_index("wave")
    middle = jnp.logical_and(z > 0, z < Z - 1)

    barrier = pltpu.get_barrier_semaphore()

    def peer(k):
        other = 0
        for i in range(W.bit_length() - 1):
            mine, flip = lax.rem(w // (1 << i), 2), lax.rem(k // (1 << i), 2)
            other = other + (1 << i) * (mine + flip - 2 * mine * flip)
        return other

    def tell(semaphore):
        for i in range(stages):
            pl.semaphore_signal(
                semaphore, inc=1, device_id=(z, peer(1 << i)), device_id_type=MESH
            )

        @pl.when(z > 0)
        def _():
            pl.semaphore_signal(
                semaphore, inc=1, device_id=(lax.rem(z + Z - 1, Z), w), device_id_type=MESH
            )

        @pl.when(z < Z - 1)
        def _():
            pl.semaphore_signal(
                semaphore, inc=1, device_id=(lax.rem(z + 1, Z), w), device_id_type=MESH
            )

    near_count = stages + jnp.where(z > 0, 1, 0) + jnp.where(z < Z - 1, 1, 0)

    fetches = [
        pltpu.make_async_copy(far, near, fetch_sem.at[i])
        for i, (far, near) in enumerate(
            [
                (lows_far, lows),
                (held_far, held),
                (inverses_far, inverses),
                (state_far, state),
                (height_far, height_operator),
                (pressure_far, pressure_column),
                (thermal_far, thermal_response),
                (mass_far, mass_row),
            ]
        )
    ]
    tell(barrier)
    for fetch in fetches:
        fetch.start()

    lane = lax.broadcasted_iota(jnp.int32, (1, LANES), 1)
    lane_pair = lane // per_pair
    lane_member = lax.rem(lane, per_pair) // (2 * slots)
    lane_slot = lax.rem(lax.rem(lane, per_pair), 2 * slots) // 2
    lane_part = lax.rem(lane, 2)
    spare = lane >= first_extra
    table_row = lax.broadcasted_iota(jnp.int32, (TABLE_ROWS, LANES), 0)
    with scope("small_fetch"):
        fetches[0].wait()
        fetches[1].wait()
    orders = jnp.full((1, LANES), -1, jnp.int32)
    for s in range(slots):
        orders = jnp.where(lane_slot == s, held[s], orders)
    low_tile = jnp.zeros((TABLE_ROWS, LANES), jnp.int32)
    for j in range(pairs):
        low_tile = jnp.where(table_row == j, lows[j], low_tile)
    low_rows[z] = low_tile

    def split_inverses():
        fetches[2].wait()
        to_row = lax.broadcasted_iota(jnp.int32, (2 * rows, 2 * levels), 0)
        from_row = lax.broadcasted_iota(jnp.int32, (2 * rows, 2 * levels), 1)
        wanted = jnp.where(to_row < rows, 2 * to_row, 2 * (to_row - rows) + 1)
        split = jnp.where(wanted == from_row, 1.0, 0.0).astype(jnp.bfloat16)
        parts = []
        for j in range(pairs):
            both = jnp.dot(
                split,
                inverses[j].reshape(2 * levels, levels),
                preferred_element_type=jnp.float32,
            )
            for member in range(2):
                matrix = both[member * rows : (member + 1) * rows]
                matrices[z, 2 * j + member] = matrix.astype(jnp.bfloat16)
                parts.append(matrix)
        blank = jnp.zeros((LANES, LANES - border), jnp.float32)
        under = [matrix[LANES:levels, 0:LANES] for matrix in parts]
        aside = jnp.concatenate([m[0:LANES, LANES:levels] for m in parts] + [blank], axis=1)
        corner = [m[LANES:levels, LANES:levels] for m in parts] + [blank[0:tail]]
        corner = jnp.concatenate(corner, axis=1)
        filler = jnp.zeros((LANES - 2 * border - tail, LANES), jnp.float32)
        edge = jnp.concatenate([*under, aside.T[0:border], corner, filler], axis=0)
        edges[z] = edge.astype(jnp.bfloat16)

    @pl.when(z < Z - 1)
    def _():
        with scope("split"):
            split_inverses()

    with scope("barrier"):
        pl.semaphore_wait(barrier, near_count)

    def z_copy(g, c, way):
        if c < pairs:
            ref = matrices.at[g, pl.ds(2 * c, 2), pl.ds(0, LANES), pl.ds(0, LANES)]
        else:
            ref = edges.at[g]
        step = 1 if way == 0 else -1
        return pltpu.make_async_remote_copy(
            src_ref=ref,
            dst_ref=ref,
            send_sem=z_send.at[0 if c < pairs else 1, way],
            recv_sem=z_recv.at[g, c],
            device_id=(z + step, w),
            device_id_type=MESH,
        )

    def forward(g, c):
        @pl.when(jnp.logical_and(g <= z, z < Z - 1))
        def _():
            z_copy(g, c, 0).start()

        @pl.when(jnp.logical_and(g >= z, z > 0))
        def _():
            z_copy(g, c, 1).start()

    def group_at(t):
        g = z
        for zz in range(Z):
            by_distance = sorted(range(Z), key=lambda a: (abs(a - zz), abs(2 * a - Z + 1)))
            g = jnp.where(z == zz, by_distance[t], g)
        return g

    def relay_now(*steps):
        for t, c in steps:
            g = group_at(t)
            z_copy(g, c, 0).wait_recv()
            forward(g, c)

    def relay(*steps):
        @pl.when(middle)
        def _():
            relay_now(*steps)

    def arrive(*steps):
        @pl.when(jnp.logical_not(middle))
        def _():
            for t, c in steps:
                z_copy(group_at(t), c, 0).wait_recv()

    groups = [group_at(t) for t in range(Z)]

    def row_copy(g):
        return pltpu.make_async_remote_copy(
            src_ref=low_rows.at[z],
            dst_ref=low_rows.at[z],
            send_sem=row_send,
            recv_sem=row_recv.at[z],
            device_id=(g, w),
            device_id_type=MESH,
        )

    def send_rows(distance):
        for step in (-distance, distance):

            @pl.when(jnp.logical_and(z + step >= 0, z + step < Z))
            def _():
                row_copy(z + step).start()

    def wait_row(g):
        pltpu.make_async_remote_copy(
            src_ref=low_rows.at[g],
            dst_ref=low_rows.at[g],
            send_sem=row_send,
            recv_sem=row_recv.at[g],
            device_id=(g, w),
            device_id_type=MESH,
        ).wait_recv()

    def table_copy(table, b, k):
        return pltpu.make_async_remote_copy(
            src_ref=table.at[w],
            dst_ref=table.at[w],
            send_sem=info_send.at[b],
            recv_sem=info_recv.at[b],
            device_id=(z, peer(k)),
            device_id_type=MESH,
        )

    def send_table(table, b):
        def start(n, carry):
            table_copy(table, b, W - n).start()
            return carry

        lax.fori_loop(1, W, start, 0)

    def all_tables(table, b):
        return pltpu.make_async_remote_copy(
            src_ref=table.at[pl.ds(0, W - 1)],
            dst_ref=table.at[pl.ds(0, W - 1)],
            send_sem=info_send.at[b],
            recv_sem=info_recv.at[b],
            device_id=(z, peer(1)),
            device_id_type=MESH,
        )

    send_rows(1)
    tell(known.at[0])

    @pl.when(z == Z - 1)
    def _():
        with scope("split_end"):
            split_inverses()

    own_chunks = [pairs, *range(pairs)]

    def steps(t, first, stop=None):
        return [(t, c) for c in own_chunks[first:stop]]

    to_right = jnp.logical_and(z > 0, 2 * z >= Z)
    to_left = jnp.logical_and(z < Z - 1, 2 * z < Z)
    free_right = jnp.logical_and(to_right, z < Z - 1)
    free_left = jnp.logical_and(to_left, z > 0)

    def send_middle():
        @pl.when(middle)
        def _():
            for c in own_chunks[1:]:
                send_own(c, False)

    def send_ends():
        @pl.when(jnp.logical_not(middle))
        def _():
            for c in own_chunks[1:]:
                send_own(c, False)

    def send_own(c, free):
        right = free_right if free else jnp.logical_not(free_right)
        left = free_left if free else jnp.logical_not(free_left)

        @pl.when(jnp.logical_and(right, z < Z - 1))
        def _():
            z_copy(z, c, 0).start()

        @pl.when(jnp.logical_and(left, z > 0))
        def _():
            z_copy(z, c, 1).start()

    send_own(pairs, False)
    for c in own_chunks:
        send_own(c, True)

    column = lax.broadcasted_iota(jnp.int32, (1, width), 1)
    column_order = jnp.full((1, width), -1, jnp.int32)
    column_start = jnp.zeros((1, width), jnp.int32)
    for s in range(slots):
        inside = jnp.logical_and(column >= s * slot_width, column < (s + 1) * slot_width)
        column_order = jnp.where(inside, held[s], column_order)
        column_start = jnp.where(inside, s * slot_width, column_start)

    def choose():
        for ref, dimension in ((pick_extra, 0), (put_extra, 1)):
            row = lax.broadcasted_iota(jnp.int32, ref.shape, dimension)
            at = lax.broadcasted_iota(jnp.int32, ref.shape, 1 - dimension)
            k, own = lax.rem(row // LANES, W), lax.rem(row, LANES)
            first_half = row < W * LANES
            if dimension == 0:
                last = own - first_extra
                valid = jnp.logical_or(first_half, own < first_extra + 2)
                valid = jnp.logical_and(valid, own >= first_extra)
            else:
                last = own // spans
                valid = jnp.where(first_half, own - first_extra, 2 * spans - 1 - own) >= 0
            offset = jnp.where(first_half, own - first_extra, 2 * last_slot + last)
            wanted = jnp.where(valid, 2 * slots * k + offset, -1)
            ref[...] = jnp.where(at == wanted, 1.0, 0.0).astype(jnp.bfloat16)

    def drive_right():
        coefficient = (column - column_start) // 2
        degree = jnp.where(
            coefficient <= truncation - column_order, column_order + coefficient, coefficient - 1
        )
        lap_scale = (degree * (degree + 1)).astype(jnp.float32) / denom
        fetches[4].wait()
        fetches[5].wait()
        height = height_operator[...].astype(jnp.float32)
        pressure_row = jnp.broadcast_to(
            pressure_column[...].astype(jnp.float32).reshape(1, levels), height.shape
        )
        across = lax.broadcasted_iota(jnp.int32, height.shape, 1)
        down = lax.broadcasted_iota(jnp.int32, height.shape, 0)
        pressure_side = jnp.sum(
            jnp.where(across == down, pressure_row, 0.0), axis=1, keepdims=True
        )
        height = jnp.concatenate(
            [jnp.zeros((levels, tail), jnp.float32), height, pressure_side], axis=1
        ).astype(jnp.bfloat16)
        fetches[3].wait()
        drive = jnp.dot(height, state[LANES:, :], preferred_element_type=jnp.float32)
        right[0:levels, :] = (
            state[0:levels, :].astype(jnp.float32) + lap_scale * drive
        ).astype(jnp.bfloat16)

    for i in range(1, rounds):
        with scope(f"known{i}"):
            pl.semaphore_wait(known.at[i - 1], near_count)
        if i + 1 < Z:
            send_rows(i + 1)
        if i + 1 < rounds:
            tell(known.at[i])
        if i == 1:
            send_middle()
    send_ends()
    with scope("drive"):
        drive_right()
    choose()
    with scope("rows_wait"):
        wait_row(groups[1])
    table = [low_rows[groups[t]][0:pairs] for t in range(2)]
    table += [jnp.broadcast_to(orders, (TABLE_ROWS - 2 * pairs, LANES))]
    info[w] = jnp.concatenate(table, axis=0)
    send_table(info, 0)
    with scope("row_far"):
        wait_row(groups[2])
        wait_row(groups[3])
    table = [low_rows[groups[t]][0:pairs] for t in range(2, 4)]
    table += [jnp.zeros((TABLE_ROWS - 2 * pairs, LANES), jnp.int32)]
    far_info[w] = jnp.concatenate(table, axis=0)
    send_table(far_info, 1)

    @pl.when(middle)
    def _():
        with scope("relay_a"):
            relay_now(*steps(1, 0, 2), *steps(2, 0, 2), *steps(1, 2, 3))

    with scope("info_wait"):
        all_tables(info, 0).wait_recv()

    def low_of(d, t, j):
        row = t % 2 * pairs + j
        return (info if t < 2 else far_info)[d][row : row + 1]

    def target_of(b, k):
        d = peer(k)
        pair = lax.rem(lane_pair + block_pairs - lax.rem(k, block_pairs), block_pairs)
        low = jnp.zeros((1, LANES), jnp.int32)
        for p in range(block_pairs):
            low = jnp.where(pair == p, low_of(d, 2 * b + p // pairs, p % pairs), low)
        slot, order = lane_slot, orders
        used = lane >= 0
        if b == 0:
            slot = jnp.where(spare, last_slot, slot)
            order = jnp.where(spare, held[last_slot], order)
            used = lane < first_extra + 2
        merged = jnp.where(order <= low, low - order, truncation + 1 - low)
        position = jnp.where(lane_member == 0, merged, truncation - low - order)
        position = jnp.where(spare, truncation + 1 - order, position)
        target = slot * slot_width + 2 * position + lane_part
        return jnp.where(jnp.logical_and(used, order >= 0), target, -1)

    def build(b, i, place):
        at = lax.broadcasted_iota(jnp.int32, (width, LANES), 0)
        for h in range(2):
            pick[block_of(b), place, :, h * LANES : (h + 1) * LANES] = jnp.where(
                at == target_of(b, 2 * i + h), 1.0, 0.0
            ).astype(jnp.bfloat16)

    def block_of(b):
        return b if keep else 0

    def place_of(i):
        return i if keep else 0

    def out_copy(b, k):
        return pltpu.make_async_remote_copy(
            src_ref=outgoing.at[b, k],
            dst_ref=arrived.at[b, k],
            send_sem=out_send.at[b],
            recv_sem=out_recv.at[b],
            device_id=(z, peer(k)),
            device_id_type=MESH,
        )

    def back_copy(b, k):
        return pltpu.make_async_remote_copy(
            src_ref=solved.at[b, k],
            dst_ref=returned.at[b, k],
            send_sem=back_send.at[b],
            recv_sem=back_recv.at[b, k // 2],
            device_id=(z, peer(k)),
            device_id_type=MESH,
        )

    def send_block(b, first, stop):
        def send(step, carry):
            i = W // 2 - 1 - step
            targets = jnp.concatenate([target_of(b, 2 * i), target_of(b, 2 * i + 1)], axis=1)
            message = jnp.zeros((rows, 2 * LANES), jnp.float32)
            for start in range(0, width, CHUNK):
                count = min(CHUNK, width - start)
                at = lax.broadcasted_iota(jnp.int32, (count, 2 * LANES), 0) + start
                chosen = jnp.where(at == targets, 1.0, 0.0).astype(jnp.bfloat16)
                pick[block_of(b), place_of(i), start : start + count, :] = chosen
                message += jnp.dot(
                    right[:, start : start + count], chosen, preferred_element_type=jnp.float32
                )
            message = message.astype(jnp.bfloat16)
            k0, k1 = 2 * i, 2 * i + 1
            outgoing[b, k0] = message[:, :LANES]
            outgoing[b, k1] = message[:, LANES:]

            @pl.when(i > 0)
            def _():
                out_copy(b, k0).start()

            out_copy(b, k1).start()
            return carry

        lax.fori_loop(first, stop, send, 0)

    def all_out(b):
        return pltpu.make_async_remote_copy(
            src_ref=outgoing.at[b, pl.ds(1, W - 1)],
            dst_ref=arrived.at[b, pl.ds(1, W - 1)],
            send_sem=out_send.at[b],
            recv_sem=out_recv.at[b],
            device_id=(z, peer(1)),
            device_id_type=MESH,
        )

    def some_back(b, first, count):
        return pltpu.make_async_remote_copy(
            src_ref=solved.at[b, pl.ds(first, count)],
            dst_ref=returned.at[b, pl.ds(first, count)],
            send_sem=back_send.at[b],
            recv_sem=back_recv.at[b, first // 2],
            device_id=(z, peer(1)),
            device_id_type=MESH,
        )

    with scope("send0"):
        send_block(0, 0, W // 4)
    with scope("relay_b"):
        relay(*steps(1, 3), *steps(2, 2, 3))
    with scope("send0b"):
        send_block(0, W // 4, W // 2)
    with scope("relay_c"):
        relay(*steps(2, 3), *steps(3, 0, 1))
    with scope("far_wait"):
        all_tables(far_info, 1).wait_recv()
    with scope("send1"):
        send_block(1, 0, W // 4)
    with scope("relay_d"):
        relay(*steps(3, 1, 2))
    with scope("send1b"):
        send_block(1, W // 4, W // 2)
    with scope("relay_e"):
        relay(*steps(3, 2, 3))
    for b in range(2):
        arrived[b, 0] = outgoing[b, 0]

    def fill_edges(t):
        g = groups[t]
        edge = edges[g].astype(jnp.float32)
        across = edge.T
        for i in range(2 * pairs):
            at = i * tail
            side = across[:, border + at : border + at + tail]
            below = jnp.concatenate(
                [edge[at : at + tail], edge[2 * border : 2 * border + tail, at : at + tail]],
                axis=1,
            )
            matrices[g, i, 0:LANES, LANES:levels] = side.astype(jnp.bfloat16)
            matrices[g, i, LANES:levels, :] = below.astype(jnp.bfloat16)

    def spread(row):
        return jnp.concatenate([row] * tiles, axis=1)

    source_orders = [
        info[peer(k)][2 * pairs : 2 * pairs + 1] for k in range(W)
    ]

    def place(p, k):
        return lane_pair == (p + k) % block_pairs

    def pack(b, p):
        for v in range(tiles):
            first = v * block_pairs
            columns = arrived[b, first, 0:levels, :]
            order = source_orders[first]
            for k in range(first + 1, min(first + block_pairs, W)):
                columns = jnp.where(place(p, k), arrived[b, k, 0:levels, :], columns)
                order = jnp.where(place(p, k), source_orders[k], order)
            part = slice(v * LANES, (v + 1) * LANES)
            packed[b * block_pairs + p, 0:levels, part] = columns
            if b == 0:
                packed_orders[p : p + 1, part] = order

    wide_member = spread(lane_member)

    def times(t, j, member, x):
        return jnp.dot(
            matrices[groups[t], 2 * j + member], x, preferred_element_type=jnp.float32
        )

    def solve(b, p):
        t, j = 2 * b + p // pairs, p % pairs
        x = packed[b * block_pairs + p, 0:levels, :]
        low = spread(low_of(w, t, j))
        use_low = jnp.logical_and(wide_member == 0, packed_orders[p : p + 1, :] <= low)
        y = jnp.where(use_low, times(t, j, 0, x), times(t, j, 1, x))
        return y.astype(jnp.bfloat16)

    def deal(answers, k):
        part = slice(k // block_pairs * LANES, (k // block_pairs + 1) * LANES)
        block = answers[0][:, part]
        for p in range(1, block_pairs):
            block = jnp.where(place(p, k), answers[p][:, part], block)
        return block

    def gather_extra(b):
        columns = jnp.concatenate([arrived[b, k, 0:levels, :] for k in range(W)], axis=1)
        start = (1 - b) * W * LANES
        chosen = pick_extra[start : start + W * LANES, :]
        return jnp.dot(columns, chosen, preferred_element_type=jnp.float32)

    def fold_mask(shape):
        level = lax.broadcasted_iota(jnp.int32, shape, 0)
        own = lax.rem(lax.broadcasted_iota(jnp.int32, shape, 1), LANES)
        return jnp.logical_and(level // fold == lax.rem(own, spans), own < 2 * spans)

    def fold_rows(shape, dimension):
        level = lax.broadcasted_iota(jnp.int32, shape, 1 - dimension)
        at = lax.broadcasted_iota(jnp.int32, shape, dimension)
        inside = jnp.logical_and(level < levels, at - tail == lax.rem(level, fold))
        return jnp.where(inside, 1.0, 0.0).astype(jnp.bfloat16)

    extra_width = extra_in.shape[1]

    def along(row):
        return jnp.concatenate([row] * (extra_width // LANES), axis=1)

    extra_lane = lax.broadcasted_iota(jnp.int32, (1, extra_width), 1)
    extra_slot = lax.rem(extra_lane, 2 * slots) // 2
    extra_order = jnp.full((1, extra_width), -1, jnp.int32)
    for k in range(W):
        for s in range(slots):
            here = jnp.logical_and(extra_lane // (2 * slots) == k, extra_slot == s)
            value = source_orders[k][:, 2 * s : 2 * s + 1]
            extra_order = jnp.where(here, value, extra_order)

    def solve_extra(y, steps):
        x = extra_in[0:levels, :]
        for t, j in steps:
            hit = extra_order == along(low_of(w, t, j))
            y = jnp.where(hit, times(t, j, 1, x).astype(jnp.bfloat16), y)
        return y

    with scope("arrive1"):
        relay(*steps(3, 3))
        arrive((1, pairs), *[(1, c) for c in range(pairs)], (2, pairs))
    fill_edges(1)
    fill_edges(2)
    with scope("wait0"):
        all_out(0).wait_recv()
    with scope("pack0"):
        for p in range(block_pairs):
            pack(0, p)
    with scope("near"):
        answers = [solve(0, p) for p in range(block_pairs)]
        for k in range(W - 1, -1, -1):
            solved[0, k] = jnp.where(spare, jnp.zeros((), jnp.bfloat16), deal(answers, k))
            if k > 0:
                back_copy(0, k).start()
    with scope("extra0"):
        extra_part = gather_extra(0)
    with scope("edges3"):
        arrive((3, pairs))
        fill_edges(3)
    with scope("wait1"):
        all_out(1).wait_recv()
    with scope("arrive2"):
        arrive(*[(2, c) for c in range(pairs)], *[(3, c) for c in range(pairs - 1)])
    with scope("pack1"):
        extra_in[0:levels, :] = (gather_extra(1) + extra_part).astype(jnp.bfloat16)
        for p in range(block_pairs):
            pack(1, p)
    with scope("late"):
        answers = [solve(1, p) for p in range(block_pairs - 1)]
        order = [(t, j) for t in range(Z) for j in range(pairs)]
        extra = jnp.zeros(extra_in.shape, jnp.bfloat16)
        extra = solve_extra(extra, order[:-1])
    with scope("arrive3"):
        arrive((3, pairs - 1))
    with scope("last"):
        extra = solve_extra(extra, order[-1:])
        answers.append(solve(1, block_pairs - 1))
        extra_back = jnp.dot(extra, put_extra[...], preferred_element_type=jnp.float32)
        half = W * LANES
        spread_last = jnp.where(fold_mask((rows, half)), extra_back[:, half:], 0.0)
        folded = jnp.dot(
            fold_rows((rows - LANES, rows), 0),
            spread_last.astype(jnp.bfloat16),
            preferred_element_type=jnp.float32,
        )
        under = lax.broadcasted_iota(jnp.int32, (rows - LANES, LANES), 0) >= tail
        here = jnp.logical_and(under, lane < 2 * spans)
        for k in range(W - 1, -1, -1):
            part = slice(k * LANES, (k + 1) * LANES)
            block = deal(answers, k)
            block = jnp.where(spare, extra_back[:, part].astype(jnp.bfloat16), block)
            bottom = jnp.where(here, folded[:, part], block[LANES:].astype(jnp.float32))
            solved[1, k, 0:LANES, :] = block[0:LANES]
            solved[1, k, LANES:rows, :] = bottom.astype(jnp.bfloat16)
            if k > 0:
                back_copy(1, k).start()

    fetches[6].wait()
    fetches[7].wait()
    total[...] = jnp.zeros_like(total)
    through_row = lax.broadcasted_iota(jnp.int32, (tail, levels), 0)
    through_lane = lax.broadcasted_iota(jnp.int32, (tail, levels), 1)
    response = jnp.concatenate(
        [
            jnp.where(through_lane == through_row + LANES, -1.0, 0.0),
            thermal_response[...].astype(jnp.float32),
            mass_row[...].astype(jnp.float32).reshape(1, levels),
        ],
        axis=0,
    ).astype(jnp.bfloat16)

    def collect(b, i, first, second):
        if not keep:
            build(b, i, 0)
        total[...] += lax.dot_general(
            jnp.concatenate([first, second], axis=1),
            pick[block_of(b), place_of(i)],
            (((1,), (1,)), ((), ())),
            preferred_element_type=jnp.float32,
        )

    def gather_back(b):
        last_pair = W // 2 - 1
        with scope(f"back{b}_0"):
            some_back(b, 1, 1).wait_recv()
            collect(b, 0, solved[b, 0], returned[b, 1])

        def step(i, carry):
            some_back(b, 2 * i, 2).wait_recv()
            collect(b, i, returned[b, 2 * i], returned[b, 2 * i + 1])
            return carry

        with scope(f"back{b}"):
            lax.fori_loop(1, last_pair, step, 0)
        with scope(f"back{b}_wait"):
            some_back(b, W - 2, 2).wait_recv()
        with scope(f"back{b}_last"):
            if b == 0:
                collect(b, last_pair, returned[b, W - 2], returned[b, W - 1])
            else:
                bottom = solved[b, 0, LANES:rows, :].astype(jnp.float32)
                for k in range(1, W):
                    bottom = bottom + returned[b, k, LANES:rows, :].astype(jnp.float32)
                unfolded = jnp.dot(
                    fold_rows((rows, rows - LANES), 1),
                    bottom.astype(jnp.bfloat16),
                    preferred_element_type=jnp.float32,
                )
                unfolded = jnp.where(fold_mask((rows, LANES)), unfolded, 0.0)
                total[...] += jnp.dot(
                    jnp.concatenate(
                        [returned[b, W - 2], returned[b, W - 1], unfolded.astype(jnp.bfloat16)],
                        axis=1,
                    ),
                    last_pick[...],
                    preferred_element_type=jnp.float32,
                )

    gather_back(0)
    with scope("last_pick"):
        order = held[last_slot]
        folded_to = last_slot * slot_width + 2 * (truncation + 1 - order) + lane // spans
        folded_to = jnp.where(jnp.logical_and(order >= 0, lane < 2 * spans), folded_to, -1)
        targets = jnp.concatenate([target_of(1, W - 2), target_of(1, W - 1), folded_to], axis=1)
        targets = jnp.broadcast_to(targets.astype(jnp.float32), (TABLE_ROWS, 3 * LANES))
        targets = targets.T[:, 0:1].astype(jnp.int32)
        at = lax.broadcasted_iota(jnp.int32, (3 * LANES, width), 1)
        last_pick[...] = jnp.where(at == targets, 1.0, 0.0).astype(jnp.bfloat16)
    gather_back(1)

    with scope("final"):
        div = total[0:levels, :].astype(jnp.bfloat16)
        change = jnp.dot(response, div, preferred_element_type=jnp.float32)
        old = state[LANES:, :].astype(jnp.float32)
        below = lax.broadcasted_iota(jnp.int32, old.shape, 0) < tail
        new = jnp.where(below, 0.0, old) - change
        new = jnp.where(column_order >= 0, new, 0.0)
        out[0:LANES, :] = div[0:LANES, :]
        out[LANES:, :] = new.astype(jnp.bfloat16)

    for b, table in ((0, info), (1, far_info)):
        all_out(b).wait_send()
        pltpu.make_async_remote_copy(
            src_ref=solved.at[b, pl.ds(1, W - 1)],
            dst_ref=returned.at[b, pl.ds(1, W - 1)],
            send_sem=back_send.at[b],
            recv_sem=back_recv.at[b, 0],
            device_id=(z, peer(1)),
            device_id_type=MESH,
        ).wait_send()
        all_tables(table, b).wait_send()
    pltpu.make_async_remote_copy(
        src_ref=low_rows.at[pl.ds(0, Z - 1)],
        dst_ref=low_rows.at[pl.ds(0, Z - 1)],
        send_sem=row_send,
        recv_sem=row_recv.at[1],
        device_id=(lax.rem(z + 1, Z), w),
        device_id_type=MESH,
    ).wait_send()

    def wait_relayed(count, way):
        for kind, ref in (
            (0, matrices.at[pl.ds(0, count), :, pl.ds(0, LANES), pl.ds(0, LANES)]),
            (1, edges.at[pl.ds(0, count)]),
        ):
            pltpu.make_async_remote_copy(
                src_ref=ref,
                dst_ref=ref,
                send_sem=z_send.at[kind, way],
                recv_sem=z_recv.at[0, 0],
                device_id=(lax.rem(z + 1, Z), w),
                device_id_type=MESH,
            ).wait_send()

    for zz in range(Z):

        @pl.when(z == zz)
        def _():
            if zz < Z - 1:
                wait_relayed(zz + 1, 0)
            if zz > 0:
                wait_relayed(Z - zz, 1)


def shards(
    state,
    held_orders,
    pair_lows,
    inverses,
    height_operator,
    pressure_column,
    thermal_response_matrix,
    mass_row,
):
    levels = height_operator.shape[0]
    slots = held_orders.shape[0]
    pairs = pair_lows.shape[0]
    Z, W = lax.axis_size("grp"), lax.axis_size("wave")
    width = state.shape[1]
    rows = ceil_to(levels, ROWS_TILE)
    places = W // 2 if W * width * 4 * LANES <= KEEP_BYTES else 1
    tiles = -(-W // (2 * pairs))
    extra_width = ceil_to(2 * slots * W, LANES)
    block = pltpu.VMEM((2, W, rows, LANES), jnp.bfloat16)
    return pl.pallas_call(
        functools.partial(kernel, (Z, W, levels, slots, pairs)),
        out_shape=pltpu.VMEM(state.shape, jnp.bfloat16),
        in_specs=[pl.BlockSpec(memory_space=pl.ANY)] * 8,
        out_specs=pl.BlockSpec(memory_space=pltpu.VMEM),
        scratch_shapes=[
            pltpu.SMEM(held_orders.shape, jnp.int32),
            pltpu.SMEM(pair_lows.shape, jnp.int32),
            pltpu.VMEM(state.shape, jnp.bfloat16),
            pltpu.VMEM((pairs, levels, 2, levels), jnp.bfloat16),
            pltpu.VMEM(height_operator.shape, jnp.bfloat16),
            pltpu.VMEM(pressure_column.shape, jnp.bfloat16),
            pltpu.VMEM(thermal_response_matrix.shape, jnp.bfloat16),
            pltpu.VMEM(mass_row.shape, jnp.bfloat16),
            pltpu.VMEM((Z, TABLE_ROWS, LANES), jnp.int32),
            pltpu.VMEM((W, TABLE_ROWS, LANES), jnp.int32),
            pltpu.VMEM((W, TABLE_ROWS, LANES), jnp.int32),
            pltpu.VMEM((Z, 2 * pairs, rows, levels), jnp.bfloat16),
            pltpu.VMEM((Z, LANES, LANES), jnp.bfloat16),
            pltpu.VMEM((rows, width), jnp.bfloat16),
            pltpu.VMEM((2 if places > 1 else 1, places, width, 2 * LANES), jnp.bfloat16),
            block,
            block,
            block,
            block,
            pltpu.VMEM((4 * pairs, rows, tiles * LANES), jnp.bfloat16),
            pltpu.VMEM((ceil_to(2 * pairs, TABLE_ROWS), tiles * LANES), jnp.int32),
            pltpu.VMEM((2 * W * LANES, extra_width), jnp.bfloat16),
            pltpu.VMEM((rows, extra_width), jnp.bfloat16),
            pltpu.VMEM((extra_width, 2 * W * LANES), jnp.bfloat16),
            pltpu.VMEM((3 * LANES, width), jnp.bfloat16),
            pltpu.VMEM((rows, width), jnp.float32),
            pltpu.SemaphoreType.DMA,
            pltpu.SemaphoreType.DMA((Z,)),
            pltpu.SemaphoreType.DMA((2,)),
            pltpu.SemaphoreType.DMA((2,)),
            pltpu.SemaphoreType.DMA((2, 2)),
            pltpu.SemaphoreType.DMA((Z, pairs + 1)),
            pltpu.SemaphoreType.DMA((2,)),
            pltpu.SemaphoreType.DMA((2,)),
            pltpu.SemaphoreType.DMA((2,)),
            pltpu.SemaphoreType.DMA((2, W // 2)),
            pltpu.SemaphoreType.DMA((8,)),
            pltpu.SemaphoreType.REGULAR((max(W.bit_length() - 2, Z - 2),)),
        ],
        compiler_params=pltpu.CompilerParams(
            collective_id=0, has_side_effects=True, vmem_limit_bytes=61000 * 1024
        ),
    )(
        *[
            pltpu.with_memory_space_constraint(array, pltpu.HBM)
            for array in (
                held_orders,
                pair_lows,
                state,
                jnp.transpose(inverses, (0, 2, 1, 3)),
                height_operator,
                pressure_column,
                thermal_response_matrix,
                mass_row,
            )
        ]
    )


def solution(mesh):
    placed = (
        P(None, ("grp", "wave")),
        P(("grp", "wave")),
        P(("grp", "wave")),
        P(("grp", "wave"), None, None, None),
        P(),
        P(),
        P(),
        P(),
    )
    return jax.shard_map(
        shards, mesh=mesh, in_specs=placed, out_specs=P(None, ("grp", "wave")), check_vma=False
    )
```

```python
import functools

import jax
import jax.numpy as jnp
from jax import lax
from jax.experimental import pallas as pl
from jax.experimental.pallas import tpu as pltpu
from jax.sharding import PartitionSpec as P

MESH = pl.DeviceIdType.MESH
LANES = 128
ROWS_TILE = 16
TABLE_ROWS = 8
CHUNK = 256
KEEP_BYTES = 24 << 20
scope = jax.named_scope


def ceil_to(value, step):
    return -(-value // step) * step


def kernel(
    size,
    held_far,
    lows_far,
    state_far,
    inverses_far,
    height_far,
    pressure_far,
    thermal_far,
    mass_far,
    out,
    held,
    lows,
    state,
    inverses,
    height_operator,
    pressure_column,
    thermal_response,
    mass_row,
    low_rows,
    info,
    far_info,
    matrices,
    edges,
    right,
    pick,
    outgoing,
    arrived,
    solved,
    returned,
    packed,
    packed_orders,
    pick_extra,
    extra_in,
    put_extra,
    last_pick,
    total,
    row_send,
    row_recv,
    info_send,
    info_recv,
    z_send,
    z_recv,
    out_send,
    out_recv,
    back_send,
    back_recv,
    fetch_sem,
    known,
):
    Z, W, levels, slots, pairs = size
    half_count = Z * W * pairs
    truncation = 2 * half_count - 1
    slot_width = 2 * (truncation + 2)
    width = slots * slot_width
    rows = solved.shape[2]
    denom = float(truncation * (truncation + 1))
    per_pair = 4 * slots
    block_pairs = 2 * pairs
    first_extra = block_pairs * per_pair
    fold = rows - levels
    spans = -(-levels // fold)
    tiles = packed.shape[2] // LANES
    last_slot = slots - 1
    stages = W.bit_length() - 1
    rounds = max(stages, Z - 1)
    tail = levels - LANES
    border = 2 * pairs * tail
    keep = pick.shape[1] > 1
    z = lax.axis_index("grp")
    w = lax.axis_index("wave")
    middle = jnp.logical_and(z > 0, z < Z - 1)

    barrier = pltpu.get_barrier_semaphore()

    def peer(k):
        other = 0
        for i in range(W.bit_length() - 1):
            mine, flip = lax.rem(w // (1 << i), 2), lax.rem(k // (1 << i), 2)
            other = other + (1 << i) * (mine + flip - 2 * mine * flip)
        return other

    def tell(semaphore):
        for i in range(stages):
            pl.semaphore_signal(
                semaphore, inc=1, device_id=(z, peer(1 << i)), device_id_type=MESH
            )

        @pl.when(z > 0)
        def _():
            pl.semaphore_signal(
                semaphore, inc=1, device_id=(lax.rem(z + Z - 1, Z), w), device_id_type=MESH
            )

        @pl.when(z < Z - 1)
        def _():
            pl.semaphore_signal(
                semaphore, inc=1, device_id=(lax.rem(z + 1, Z), w), device_id_type=MESH
            )

    near_count = stages + jnp.where(z > 0, 1, 0) + jnp.where(z < Z - 1, 1, 0)

    fetches = [
        pltpu.make_async_copy(far, near, fetch_sem.at[i])
        for i, (far, near) in enumerate(
            [
                (lows_far, lows),
                (held_far, held),
                (inverses_far, inverses),
                (state_far, state),
                (height_far, height_operator),
                (pressure_far, pressure_column),
                (thermal_far, thermal_response),
                (mass_far, mass_row),
            ]
        )
    ]
    tell(barrier)
    for distance in range(2, Z):

        @pl.when(z + distance < Z)
        def _():
            pl.semaphore_signal(
                barrier, inc=1, device_id=(lax.rem(z + distance, Z), w), device_id_type=MESH
            )

    for fetch in fetches:
        fetch.start()

    lane = lax.broadcasted_iota(jnp.int32, (1, LANES), 1)
    lane_pair = lane // per_pair
    lane_member = lax.rem(lane, per_pair) // (2 * slots)
    lane_slot = lax.rem(lax.rem(lane, per_pair), 2 * slots) // 2
    lane_part = lax.rem(lane, 2)
    spare = lane >= first_extra
    table_row = lax.broadcasted_iota(jnp.int32, (TABLE_ROWS, LANES), 0)
    with scope("small_fetch"):
        fetches[0].wait()
        fetches[1].wait()
    orders = jnp.full((1, LANES), -1, jnp.int32)
    for s in range(slots):
        orders = jnp.where(lane_slot == s, held[s], orders)
    low_tile = jnp.zeros((TABLE_ROWS, LANES), jnp.int32)
    for j in range(pairs):
        low_tile = jnp.where(table_row == j, lows[j], low_tile)
    low_rows[z] = low_tile

    def split_inverses():
        fetches[2].wait()
        to_row = lax.broadcasted_iota(jnp.int32, (2 * rows, 2 * levels), 0)
        from_row = lax.broadcasted_iota(jnp.int32, (2 * rows, 2 * levels), 1)
        wanted = jnp.where(to_row < rows, 2 * to_row, 2 * (to_row - rows) + 1)
        split = jnp.where(wanted == from_row, 1.0, 0.0).astype(jnp.bfloat16)
        parts = []
        for j in range(pairs):
            both = jnp.dot(
                split,
                inverses[j].reshape(2 * levels, levels),
                preferred_element_type=jnp.float32,
            )
            for member in range(2):
                matrix = both[member * rows : (member + 1) * rows]
                matrices[z, 2 * j + member] = matrix.astype(jnp.bfloat16)
                parts.append(matrix)
        blank = jnp.zeros((LANES, LANES - border), jnp.float32)
        under = [matrix[LANES:levels, 0:LANES] for matrix in parts]
        aside = jnp.concatenate([m[0:LANES, LANES:levels] for m in parts] + [blank], axis=1)
        corner = [m[LANES:levels, LANES:levels] for m in parts] + [blank[0:tail]]
        corner = jnp.concatenate(corner, axis=1)
        filler = jnp.zeros((LANES - 2 * border - tail, LANES), jnp.float32)
        edge = jnp.concatenate([*under, aside.T[0:border], corner, filler], axis=0)
        edges[z] = edge.astype(jnp.bfloat16)

    @pl.when(z < Z - 1)
    def _():
        with scope("split"):
            split_inverses()

    with scope("barrier"):
        pl.semaphore_wait(barrier, near_count + jnp.where(z > 1, z - 1, 0))

    def z_copy(g, c, way):
        if c < pairs:
            ref = matrices.at[g, pl.ds(2 * c, 2), pl.ds(0, LANES), pl.ds(0, LANES)]
        else:
            ref = edges.at[g]
        step = 1 if way == 0 else -1
        return pltpu.make_async_remote_copy(
            src_ref=ref,
            dst_ref=ref,
            send_sem=z_send.at[0 if c < pairs else 1, way],
            recv_sem=z_recv.at[g, c],
            device_id=(z + step, w),
            device_id_type=MESH,
        )

    def forward(g, c):
        @pl.when(jnp.logical_and(g <= z, z < Z - 1))
        def _():
            z_copy(g, c, 0).start()

        @pl.when(jnp.logical_and(g >= z, z > 0))
        def _():
            z_copy(g, c, 1).start()

    def group_at(t):
        g = z
        for zz in range(Z):
            by_distance = sorted(range(Z), key=lambda a: (abs(a - zz), abs(2 * a - Z + 1)))
            g = jnp.where(z == zz, by_distance[t], g)
        return g

    def relay_now(*steps):
        for t, c in steps:
            g = group_at(t)
            z_copy(g, c, 0).wait_recv()
            forward(g, c)

    def relay(*steps):
        @pl.when(middle)
        def _():
            relay_now(*steps)

    def arrive(*steps):
        @pl.when(jnp.logical_not(middle))
        def _():
            for t, c in steps:
                z_copy(group_at(t), c, 0).wait_recv()

    groups = [group_at(t) for t in range(Z)]

    def row_copy(g):
        return pltpu.make_async_remote_copy(
            src_ref=low_rows.at[z],
            dst_ref=low_rows.at[z],
            send_sem=row_send,
            recv_sem=row_recv.at[z],
            device_id=(g, w),
            device_id_type=MESH,
        )

    def send_rows(*distances):
        for step in distances:

            @pl.when(jnp.logical_and(z + step >= 0, z + step < Z))
            def _():
                row_copy(z + step).start()

    def wait_row(g):
        pltpu.make_async_remote_copy(
            src_ref=low_rows.at[g],
            dst_ref=low_rows.at[g],
            send_sem=row_send,
            recv_sem=row_recv.at[g],
            device_id=(g, w),
            device_id_type=MESH,
        ).wait_recv()

    def table_copy(table, b, k):
        return pltpu.make_async_remote_copy(
            src_ref=table.at[w],
            dst_ref=table.at[w],
            send_sem=info_send.at[b],
            recv_sem=info_recv.at[b],
            device_id=(z, peer(k)),
            device_id_type=MESH,
        )

    def send_table(table, b):
        def start(n, carry):
            table_copy(table, b, W - n).start()
            return carry

        lax.fori_loop(1, W, start, 0)

    def all_tables(table, b):
        return pltpu.make_async_remote_copy(
            src_ref=table.at[pl.ds(0, W - 1)],
            dst_ref=table.at[pl.ds(0, W - 1)],
            send_sem=info_send.at[b],
            recv_sem=info_recv.at[b],
            device_id=(z, peer(1)),
            device_id_type=MESH,
        )

    send_rows(-1, 1, *range(-2, -Z, -1))
    tell(known.at[0])

    @pl.when(z == Z - 1)
    def _():
        with scope("split_end"):
            split_inverses()

    own_chunks = [pairs, *range(pairs)]

    def steps(t, first, stop=None):
        return [(t, c) for c in own_chunks[first:stop]]

    to_right = jnp.logical_and(z > 0, 2 * z >= Z)
    to_left = jnp.logical_and(z < Z - 1, 2 * z < Z)
    free_right = jnp.logical_and(to_right, z < Z - 1)
    free_left = jnp.logical_and(to_left, z > 0)

    def send_middle():
        @pl.when(middle)
        def _():
            for c in own_chunks[1:]:
                send_own(c, False)

    def send_ends():
        @pl.when(jnp.logical_not(middle))
        def _():
            for c in own_chunks[1:]:
                send_own(c, False)

    def send_own(c, free):
        right = free_right if free else jnp.logical_not(free_right)
        left = free_left if free else jnp.logical_not(free_left)

        @pl.when(jnp.logical_and(right, z < Z - 1))
        def _():
            z_copy(z, c, 0).start()

        @pl.when(jnp.logical_and(left, z > 0))
        def _():
            z_copy(z, c, 1).start()

    send_own(pairs, False)
    for c in own_chunks:
        send_own(c, True)

    column = lax.broadcasted_iota(jnp.int32, (1, width), 1)
    column_order = jnp.full((1, width), -1, jnp.int32)
    column_start = jnp.zeros((1, width), jnp.int32)
    for s in range(slots):
        inside = jnp.logical_and(column >= s * slot_width, column < (s + 1) * slot_width)
        column_order = jnp.where(inside, held[s], column_order)
        column_start = jnp.where(inside, s * slot_width, column_start)

    def choose():
        for ref, dimension in ((pick_extra, 0), (put_extra, 1)):
            row = lax.broadcasted_iota(jnp.int32, ref.shape, dimension)
            at = lax.broadcasted_iota(jnp.int32, ref.shape, 1 - dimension)
            k, own = lax.rem(row // LANES, W), lax.rem(row, LANES)
            first_half = row < W * LANES
            if dimension == 0:
                last = own - first_extra
                valid = jnp.logical_or(first_half, own < first_extra + 2)
                valid = jnp.logical_and(valid, own >= first_extra)
            else:
                last = own // spans
                valid = jnp.where(first_half, own - first_extra, 2 * spans - 1 - own) >= 0
            offset = jnp.where(first_half, own - first_extra, 2 * last_slot + last)
            wanted = jnp.where(valid, 2 * slots * k + offset, -1)
            ref[...] = jnp.where(at == wanted, 1.0, 0.0).astype(jnp.bfloat16)

    def drive_right():
        coefficient = (column - column_start) // 2
        degree = jnp.where(
            coefficient <= truncation - column_order, column_order + coefficient, coefficient - 1
        )
        lap_scale = (degree * (degree + 1)).astype(jnp.float32) / denom
        fetches[4].wait()
        fetches[5].wait()
        height = height_operator[...].astype(jnp.float32)
        pressure_row = jnp.broadcast_to(
            pressure_column[...].astype(jnp.float32).reshape(1, levels), height.shape
        )
        across = lax.broadcasted_iota(jnp.int32, height.shape, 1)
        down = lax.broadcasted_iota(jnp.int32, height.shape, 0)
        pressure_side = jnp.sum(
            jnp.where(across == down, pressure_row, 0.0), axis=1, keepdims=True
        )
        height = jnp.concatenate(
            [jnp.zeros((levels, tail), jnp.float32), height, pressure_side], axis=1
        ).astype(jnp.bfloat16)
        fetches[3].wait()
        drive = jnp.dot(height, state[LANES:, :], preferred_element_type=jnp.float32)
        right[0:levels, :] = (
            state[0:levels, :].astype(jnp.float32) + lap_scale * drive
        ).astype(jnp.bfloat16)

    for i in range(1, rounds):
        with scope(f"known{i}"):
            pl.semaphore_wait(known.at[i - 1], near_count)
        if i + 1 < Z:
            send_rows(i + 1)
        if i + 1 < rounds:
            tell(known.at[i])
        if i == 1:
            send_middle()
    send_ends()
    with scope("rows_wait"):
        wait_row(groups[1])
    table = [low_rows[groups[t]][0:pairs] for t in range(2)]
    table += [jnp.broadcast_to(orders, (TABLE_ROWS - 2 * pairs, LANES))]
    info[w] = jnp.concatenate(table, axis=0)
    send_table(info, 0)
    with scope("drive"):
        drive_right()
    choose()
    with scope("row_far"):
        wait_row(groups[2])
        wait_row(groups[3])
    table = [low_rows[groups[t]][0:pairs] for t in range(2, 4)]
    table += [jnp.zeros((TABLE_ROWS - 2 * pairs, LANES), jnp.int32)]
    far_info[w] = jnp.concatenate(table, axis=0)
    send_table(far_info, 1)

    @pl.when(middle)
    def _():
        with scope("relay_a"):
            relay_now(*steps(1, 0, 3), *steps(2, 0, 2))

    with scope("info_wait"):
        all_tables(info, 0).wait_recv()

    def low_of(d, t, j):
        row = t % 2 * pairs + j
        return (info if t < 2 else far_info)[d][row : row + 1]

    def target_of(b, k):
        d = peer(k)
        pair = lax.rem(lane_pair + block_pairs - lax.rem(k, block_pairs), block_pairs)
        low = jnp.zeros((1, LANES), jnp.int32)
        for p in range(block_pairs):
            low = jnp.where(pair == p, low_of(d, 2 * b + p // pairs, p % pairs), low)
        slot, order = lane_slot, orders
        used = lane >= 0
        if b == 0:
            slot = jnp.where(spare, last_slot, slot)
            order = jnp.where(spare, held[last_slot], order)
            used = lane < first_extra + 2
        merged = jnp.where(order <= low, low - order, truncation + 1 - low)
        position = jnp.where(lane_member == 0, merged, truncation - low - order)
        position = jnp.where(spare, truncation + 1 - order, position)
        target = slot * slot_width + 2 * position + lane_part
        return jnp.where(jnp.logical_and(used, order >= 0), target, -1)

    def build(b, i, place):
        at = lax.broadcasted_iota(jnp.int32, (width, LANES), 0)
        for h in range(2):
            pick[block_of(b), place, :, h * LANES : (h + 1) * LANES] = jnp.where(
                at == target_of(b, 2 * i + h), 1.0, 0.0
            ).astype(jnp.bfloat16)

    def block_of(b):
        return b if keep else 0

    def place_of(i):
        return i if keep else 0

    def out_copy(b, k):
        return pltpu.make_async_remote_copy(
            src_ref=outgoing.at[b, k],
            dst_ref=arrived.at[b, k],
            send_sem=out_send.at[b],
            recv_sem=out_recv.at[b],
            device_id=(z, peer(k)),
            device_id_type=MESH,
        )

    def back_copy(b, k):
        return pltpu.make_async_remote_copy(
            src_ref=solved.at[b, k],
            dst_ref=returned.at[b, k],
            send_sem=back_send.at[b],
            recv_sem=back_recv.at[b, k // 2],
            device_id=(z, peer(k)),
            device_id_type=MESH,
        )

    def send_block(b, first, stop):
        def send(step, carry):
            i = W // 2 - 1 - step
            targets = jnp.concatenate([target_of(b, 2 * i), target_of(b, 2 * i + 1)], axis=1)
            message = jnp.zeros((rows, 2 * LANES), jnp.float32)
            for start in range(0, width, CHUNK):
                count = min(CHUNK, width - start)
                at = lax.broadcasted_iota(jnp.int32, (count, 2 * LANES), 0) + start
                chosen = jnp.where(at == targets, 1.0, 0.0).astype(jnp.bfloat16)
                pick[block_of(b), place_of(i), start : start + count, :] = chosen
                message += jnp.dot(
                    right[:, start : start + count], chosen, preferred_element_type=jnp.float32
                )
            message = message.astype(jnp.bfloat16)
            k0, k1 = 2 * i, 2 * i + 1
            outgoing[b, k0] = message[:, :LANES]
            outgoing[b, k1] = message[:, LANES:]

            @pl.when(i > 0)
            def _():
                out_copy(b, k0).start()

            out_copy(b, k1).start()
            return carry

        lax.fori_loop(first, stop, send, 0)

    def all_out(b):
        return pltpu.make_async_remote_copy(
            src_ref=outgoing.at[b, pl.ds(1, W - 1)],
            dst_ref=arrived.at[b, pl.ds(1, W - 1)],
            send_sem=out_send.at[b],
            recv_sem=out_recv.at[b],
            device_id=(z, peer(1)),
            device_id_type=MESH,
        )

    def some_back(b, first, count):
        return pltpu.make_async_remote_copy(
            src_ref=solved.at[b, pl.ds(first, count)],
            dst_ref=returned.at[b, pl.ds(first, count)],
            send_sem=back_send.at[b],
            recv_sem=back_recv.at[b, first // 2],
            device_id=(z, peer(1)),
            device_id_type=MESH,
        )

    with scope("send0"):
        send_block(0, 0, W // 4)
    with scope("relay_b"):
        relay(*steps(1, 3), *steps(2, 2, 3))
    with scope("send0b"):
        send_block(0, W // 4, W // 2)
    with scope("relay_c"):
        relay(*steps(2, 3), *steps(3, 0, 1))
    with scope("far_wait"):
        all_tables(far_info, 1).wait_recv()
    with scope("send1"):
        send_block(1, 0, W // 4)
    with scope("relay_d"):
        relay(*steps(3, 1, 2))
    with scope("send1b"):
        send_block(1, W // 4, W // 2)
    with scope("relay_e"):
        relay(*steps(3, 2, 3))
    for b in range(2):
        arrived[b, 0] = outgoing[b, 0]

    def fill_edges(t):
        g = groups[t]
        edge = edges[g].astype(jnp.float32)
        across = edge.T
        for i in range(2 * pairs):
            at = i * tail
            side = across[:, border + at : border + at + tail]
            below = jnp.concatenate(
                [edge[at : at + tail], edge[2 * border : 2 * border + tail, at : at + tail]],
                axis=1,
            )
            matrices[g, i, 0:LANES, LANES:levels] = side.astype(jnp.bfloat16)
            matrices[g, i, LANES:levels, :] = below.astype(jnp.bfloat16)

    def spread(row):
        return jnp.concatenate([row] * tiles, axis=1)

    source_orders = [
        info[peer(k)][2 * pairs : 2 * pairs + 1] for k in range(W)
    ]

    def place(p, k):
        return lane_pair == (p + k) % block_pairs

    def pack(b, p):
        for v in range(tiles):
            first = v * block_pairs
            columns = arrived[b, first, 0:levels, :]
            order = source_orders[first]
            for k in range(first + 1, min(first + block_pairs, W)):
                columns = jnp.where(place(p, k), arrived[b, k, 0:levels, :], columns)
                order = jnp.where(place(p, k), source_orders[k], order)
            part = slice(v * LANES, (v + 1) * LANES)
            packed[b * block_pairs + p, 0:levels, part] = columns
            if b == 0:
                packed_orders[p : p + 1, part] = order

    wide_member = spread(lane_member)

    def times(t, j, member, x):
        return jnp.dot(
            matrices[groups[t], 2 * j + member], x, preferred_element_type=jnp.float32
        )

    def solve(b, p):
        t, j = 2 * b + p // pairs, p % pairs
        x = packed[b * block_pairs + p, 0:levels, :]
        low = spread(low_of(w, t, j))
        use_low = jnp.logical_and(wide_member == 0, packed_orders[p : p + 1, :] <= low)
        y = jnp.where(use_low, times(t, j, 0, x), times(t, j, 1, x))
        return y.astype(jnp.bfloat16)

    def deal(answers, k):
        part = slice(k // block_pairs * LANES, (k // block_pairs + 1) * LANES)
        block = answers[0][:, part]
        for p in range(1, block_pairs):
            block = jnp.where(place(p, k), answers[p][:, part], block)
        return block

    def gather_extra(b):
        columns = jnp.concatenate([arrived[b, k, 0:levels, :] for k in range(W)], axis=1)
        start = (1 - b) * W * LANES
        chosen = pick_extra[start : start + W * LANES, :]
        return jnp.dot(columns, chosen, preferred_element_type=jnp.float32)

    def fold_mask(shape):
        level = lax.broadcasted_iota(jnp.int32, shape, 0)
        own = lax.rem(lax.broadcasted_iota(jnp.int32, shape, 1), LANES)
        return jnp.logical_and(level // fold == lax.rem(own, spans), own < 2 * spans)

    def fold_rows(shape, dimension):
        level = lax.broadcasted_iota(jnp.int32, shape, 1 - dimension)
        at = lax.broadcasted_iota(jnp.int32, shape, dimension)
        inside = jnp.logical_and(level < levels, at - tail == lax.rem(level, fold))
        return jnp.where(inside, 1.0, 0.0).astype(jnp.bfloat16)

    extra_width = extra_in.shape[1]

    def along(row):
        return jnp.concatenate([row] * (extra_width // LANES), axis=1)

    extra_lane = lax.broadcasted_iota(jnp.int32, (1, extra_width), 1)
    extra_slot = lax.rem(extra_lane, 2 * slots) // 2
    extra_order = jnp.full((1, extra_width), -1, jnp.int32)
    for k in range(W):
        for s in range(slots):
            here = jnp.logical_and(extra_lane // (2 * slots) == k, extra_slot == s)
            value = source_orders[k][:, 2 * s : 2 * s + 1]
            extra_order = jnp.where(here, value, extra_order)

    def solve_extra(y, steps):
        x = extra_in[0:levels, :]
        for t, j in steps:
            hit = extra_order == along(low_of(w, t, j))
            y = jnp.where(hit, times(t, j, 1, x).astype(jnp.bfloat16), y)
        return y

    with scope("arrive1"):
        relay(*steps(3, 3))
        arrive((1, pairs), *[(1, c) for c in range(pairs)], (2, pairs))
    fill_edges(1)
    fill_edges(2)
    with scope("wait0"):
        all_out(0).wait_recv()
    with scope("pack0"):
        for p in range(block_pairs):
            pack(0, p)
    with scope("near"):
        answers = [solve(0, p) for p in range(block_pairs)]
        for k in range(W - 1, -1, -1):
            solved[0, k] = jnp.where(spare, jnp.zeros((), jnp.bfloat16), deal(answers, k))
            if k > 0:
                back_copy(0, k).start()
    with scope("extra0"):
        extra_part = gather_extra(0)
    with scope("edges3"):
        arrive((3, pairs))
        fill_edges(3)
    with scope("wait1"):
        all_out(1).wait_recv()
    with scope("arrive2"):
        arrive(*[(2, c) for c in range(pairs)], *[(3, c) for c in range(pairs - 1)])
    with scope("pack1"):
        extra_in[0:levels, :] = (gather_extra(1) + extra_part).astype(jnp.bfloat16)
        for p in range(block_pairs):
            pack(1, p)
    with scope("late"):
        answers = [solve(1, p) for p in range(block_pairs - 1)]
        order = [(t, j) for t in range(Z) for j in range(pairs)]
        extra = jnp.zeros(extra_in.shape, jnp.bfloat16)
        extra = solve_extra(extra, order[:-1])
    with scope("arrive3"):
        arrive((3, pairs - 1))
    with scope("last"):
        extra = solve_extra(extra, order[-1:])
        answers.append(solve(1, block_pairs - 1))
        extra_back = jnp.dot(extra, put_extra[...], preferred_element_type=jnp.float32)
        half = W * LANES
        spread_last = jnp.where(fold_mask((rows, half)), extra_back[:, half:], 0.0)
        folded = jnp.dot(
            fold_rows((rows - LANES, rows), 0),
            spread_last.astype(jnp.bfloat16),
            preferred_element_type=jnp.float32,
        )
        under = lax.broadcasted_iota(jnp.int32, (rows - LANES, LANES), 0) >= tail
        here = jnp.logical_and(under, lane < 2 * spans)
        for k in range(W - 1, -1, -1):
            part = slice(k * LANES, (k + 1) * LANES)
            block = deal(answers, k)
            block = jnp.where(spare, extra_back[:, part].astype(jnp.bfloat16), block)
            bottom = jnp.where(here, folded[:, part], block[LANES:].astype(jnp.float32))
            solved[1, k, 0:LANES, :] = block[0:LANES]
            solved[1, k, LANES:rows, :] = bottom.astype(jnp.bfloat16)
            if k > 0:
                back_copy(1, k).start()

    fetches[6].wait()
    fetches[7].wait()
    total[...] = jnp.zeros_like(total)
    through_row = lax.broadcasted_iota(jnp.int32, (tail, levels), 0)
    through_lane = lax.broadcasted_iota(jnp.int32, (tail, levels), 1)
    response = jnp.concatenate(
        [
            jnp.where(through_lane == through_row + LANES, -1.0, 0.0),
            thermal_response[...].astype(jnp.float32),
            mass_row[...].astype(jnp.float32).reshape(1, levels),
        ],
        axis=0,
    ).astype(jnp.bfloat16)

    def collect(b, i, first, second):
        if not keep:
            build(b, i, 0)
        total[...] += lax.dot_general(
            jnp.concatenate([first, second], axis=1),
            pick[block_of(b), place_of(i)],
            (((1,), (1,)), ((), ())),
            preferred_element_type=jnp.float32,
        )

    def gather_back(b):
        last_pair = W // 2 - 1
        with scope(f"back{b}_0"):
            some_back(b, 1, 1).wait_recv()
            collect(b, 0, solved[b, 0], returned[b, 1])

        def step(i, carry):
            some_back(b, 2 * i, 2).wait_recv()
            collect(b, i, returned[b, 2 * i], returned[b, 2 * i + 1])
            return carry

        with scope(f"back{b}"):
            lax.fori_loop(1, last_pair, step, 0)
        with scope(f"back{b}_wait"):
            some_back(b, W - 2, 2).wait_recv()
        with scope(f"back{b}_last"):
            if b == 0:
                collect(b, last_pair, returned[b, W - 2], returned[b, W - 1])
            else:
                bottom = solved[b, 0, LANES:rows, :].astype(jnp.float32)
                for k in range(1, W):
                    bottom = bottom + returned[b, k, LANES:rows, :].astype(jnp.float32)
                unfolded = jnp.dot(
                    fold_rows((rows, rows - LANES), 1),
                    bottom.astype(jnp.bfloat16),
                    preferred_element_type=jnp.float32,
                )
                unfolded = jnp.where(fold_mask((rows, LANES)), unfolded, 0.0)
                total[...] += jnp.dot(
                    jnp.concatenate(
                        [returned[b, W - 2], returned[b, W - 1], unfolded.astype(jnp.bfloat16)],
                        axis=1,
                    ),
                    last_pick[...],
                    preferred_element_type=jnp.float32,
                )

    gather_back(0)
    with scope("last_pick"):
        order = held[last_slot]
        folded_to = last_slot * slot_width + 2 * (truncation + 1 - order) + lane // spans
        folded_to = jnp.where(jnp.logical_and(order >= 0, lane < 2 * spans), folded_to, -1)
        targets = jnp.concatenate([target_of(1, W - 2), target_of(1, W - 1), folded_to], axis=1)
        targets = jnp.broadcast_to(targets.astype(jnp.float32), (TABLE_ROWS, 3 * LANES))
        targets = targets.T[:, 0:1].astype(jnp.int32)
        at = lax.broadcasted_iota(jnp.int32, (3 * LANES, width), 1)
        last_pick[...] = jnp.where(at == targets, 1.0, 0.0).astype(jnp.bfloat16)
    gather_back(1)

    with scope("final"):
        div = total[0:levels, :].astype(jnp.bfloat16)
        change = jnp.dot(response, div, preferred_element_type=jnp.float32)
        old = state[LANES:, :].astype(jnp.float32)
        below = lax.broadcasted_iota(jnp.int32, old.shape, 0) < tail
        new = jnp.where(below, 0.0, old) - change
        new = jnp.where(column_order >= 0, new, 0.0)
        out[0:LANES, :] = div[0:LANES, :]
        out[LANES:, :] = new.astype(jnp.bfloat16)

    for b, table in ((0, info), (1, far_info)):
        all_out(b).wait_send()
        pltpu.make_async_remote_copy(
            src_ref=solved.at[b, pl.ds(1, W - 1)],
            dst_ref=returned.at[b, pl.ds(1, W - 1)],
            send_sem=back_send.at[b],
            recv_sem=back_recv.at[b, 0],
            device_id=(z, peer(1)),
            device_id_type=MESH,
        ).wait_send()
        all_tables(table, b).wait_send()
    pltpu.make_async_remote_copy(
        src_ref=low_rows.at[pl.ds(0, Z - 1)],
        dst_ref=low_rows.at[pl.ds(0, Z - 1)],
        send_sem=row_send,
        recv_sem=row_recv.at[1],
        device_id=(lax.rem(z + 1, Z), w),
        device_id_type=MESH,
    ).wait_send()

    def wait_relayed(count, way):
        for kind, ref in (
            (0, matrices.at[pl.ds(0, count), :, pl.ds(0, LANES), pl.ds(0, LANES)]),
            (1, edges.at[pl.ds(0, count)]),
        ):
            pltpu.make_async_remote_copy(
                src_ref=ref,
                dst_ref=ref,
                send_sem=z_send.at[kind, way],
                recv_sem=z_recv.at[0, 0],
                device_id=(lax.rem(z + 1, Z), w),
                device_id_type=MESH,
            ).wait_send()

    for zz in range(Z):

        @pl.when(z == zz)
        def _():
            if zz < Z - 1:
                wait_relayed(zz + 1, 0)
            if zz > 0:
                wait_relayed(Z - zz, 1)


def shards(
    state,
    held_orders,
    pair_lows,
    inverses,
    height_operator,
    pressure_column,
    thermal_response_matrix,
    mass_row,
):
    levels = height_operator.shape[0]
    slots = held_orders.shape[0]
    pairs = pair_lows.shape[0]
    Z, W = lax.axis_size("grp"), lax.axis_size("wave")
    width = state.shape[1]
    rows = ceil_to(levels, ROWS_TILE)
    places = W // 2 if W * width * 4 * LANES <= KEEP_BYTES else 1
    tiles = -(-W // (2 * pairs))
    extra_width = ceil_to(2 * slots * W, LANES)
    block = pltpu.VMEM((2, W, rows, LANES), jnp.bfloat16)
    return pl.pallas_call(
        functools.partial(kernel, (Z, W, levels, slots, pairs)),
        out_shape=pltpu.VMEM(state.shape, jnp.bfloat16),
        in_specs=[pl.BlockSpec(memory_space=pl.ANY)] * 8,
        out_specs=pl.BlockSpec(memory_space=pltpu.VMEM),
        scratch_shapes=[
            pltpu.SMEM(held_orders.shape, jnp.int32),
            pltpu.SMEM(pair_lows.shape, jnp.int32),
            pltpu.VMEM(state.shape, jnp.bfloat16),
            pltpu.VMEM((pairs, levels, 2, levels), jnp.bfloat16),
            pltpu.VMEM(height_operator.shape, jnp.bfloat16),
            pltpu.VMEM(pressure_column.shape, jnp.bfloat16),
            pltpu.VMEM(thermal_response_matrix.shape, jnp.bfloat16),
            pltpu.VMEM(mass_row.shape, jnp.bfloat16),
            pltpu.VMEM((Z, TABLE_ROWS, LANES), jnp.int32),
            pltpu.VMEM((W, TABLE_ROWS, LANES), jnp.int32),
            pltpu.VMEM((W, TABLE_ROWS, LANES), jnp.int32),
            pltpu.VMEM((Z, 2 * pairs, rows, levels), jnp.bfloat16),
            pltpu.VMEM((Z, LANES, LANES), jnp.bfloat16),
            pltpu.VMEM((rows, width), jnp.bfloat16),
            pltpu.VMEM((2 if places > 1 else 1, places, width, 2 * LANES), jnp.bfloat16),
            block,
            block,
            block,
            block,
            pltpu.VMEM((4 * pairs, rows, tiles * LANES), jnp.bfloat16),
            pltpu.VMEM((ceil_to(2 * pairs, TABLE_ROWS), tiles * LANES), jnp.int32),
            pltpu.VMEM((2 * W * LANES, extra_width), jnp.bfloat16),
            pltpu.VMEM((rows, extra_width), jnp.bfloat16),
            pltpu.VMEM((extra_width, 2 * W * LANES), jnp.bfloat16),
            pltpu.VMEM((3 * LANES, width), jnp.bfloat16),
            pltpu.VMEM((rows, width), jnp.float32),
            pltpu.SemaphoreType.DMA,
            pltpu.SemaphoreType.DMA((Z,)),
            pltpu.SemaphoreType.DMA((2,)),
            pltpu.SemaphoreType.DMA((2,)),
            pltpu.SemaphoreType.DMA((2, 2)),
            pltpu.SemaphoreType.DMA((Z, pairs + 1)),
            pltpu.SemaphoreType.DMA((2,)),
            pltpu.SemaphoreType.DMA((2,)),
            pltpu.SemaphoreType.DMA((2,)),
            pltpu.SemaphoreType.DMA((2, W // 2)),
            pltpu.SemaphoreType.DMA((8,)),
            pltpu.SemaphoreType.REGULAR((max(W.bit_length() - 2, Z - 2),)),
        ],
        compiler_params=pltpu.CompilerParams(
            collective_id=0, has_side_effects=True, vmem_limit_bytes=61000 * 1024
        ),
    )(
        *[
            pltpu.with_memory_space_constraint(array, pltpu.HBM)
            for array in (
                held_orders,
                pair_lows,
                state,
                jnp.transpose(inverses, (0, 2, 1, 3)),
                height_operator,
                pressure_column,
                thermal_response_matrix,
                mass_row,
            )
        ]
    )


def solution(mesh):
    placed = (
        P(None, ("grp", "wave")),
        P(("grp", "wave")),
        P(("grp", "wave")),
        P(("grp", "wave"), None, None, None),
        P(),
        P(),
        P(),
        P(),
    )
    return jax.shard_map(
        shards, mesh=mesh, in_specs=placed, out_specs=P(None, ("grp", "wave")), check_vma=False
    )
```

```python
import functools

import jax
import jax.numpy as jnp
from jax import lax
from jax.experimental import pallas as pl
from jax.experimental.pallas import tpu as pltpu
from jax.sharding import PartitionSpec as P

MESH = pl.DeviceIdType.MESH
LANES = 128
ROWS_TILE = 16
TABLE_ROWS = 8
CHUNK = 256
KEEP_BYTES = 24 << 20
scope = jax.named_scope


def ceil_to(value, step):
    return -(-value // step) * step


def kernel(
    size,
    held_far,
    lows_far,
    state_far,
    inverses_far,
    height_far,
    pressure_far,
    thermal_far,
    mass_far,
    out,
    held,
    lows,
    state,
    inverses,
    height_operator,
    pressure_column,
    thermal_response,
    mass_row,
    low_rows,
    info,
    far_info,
    matrices,
    edges,
    right,
    pick,
    outgoing,
    arrived,
    solved,
    returned,
    packed,
    packed_orders,
    pick_extra,
    extra_in,
    put_extra,
    last_pick,
    total,
    row_send,
    row_recv,
    info_send,
    info_recv,
    z_send,
    z_recv,
    out_send,
    out_recv,
    back_send,
    back_recv,
    fetch_sem,
    known,
):
    Z, W, levels, slots, pairs = size
    half_count = Z * W * pairs
    truncation = 2 * half_count - 1
    slot_width = 2 * (truncation + 2)
    width = slots * slot_width
    rows = solved.shape[2]
    denom = float(truncation * (truncation + 1))
    per_pair = 4 * slots
    block_pairs = 2 * pairs
    first_extra = block_pairs * per_pair
    fold = rows - levels
    spans = -(-levels // fold)
    tiles = packed.shape[2] // LANES
    last_slot = slots - 1
    stages = W.bit_length() - 1
    rounds = max(stages, Z - 1)
    tail = levels - LANES
    border = 2 * pairs * tail
    keep = pick.shape[1] > 1
    z = lax.axis_index("grp")
    w = lax.axis_index("wave")
    middle = jnp.logical_and(z > 0, z < Z - 1)

    barrier = pltpu.get_barrier_semaphore()

    def peer(k):
        other = 0
        for i in range(W.bit_length() - 1):
            mine, flip = lax.rem(w // (1 << i), 2), lax.rem(k // (1 << i), 2)
            other = other + (1 << i) * (mine + flip - 2 * mine * flip)
        return other

    def tell(semaphore):
        for i in range(stages):
            pl.semaphore_signal(
                semaphore, inc=1, device_id=(z, peer(1 << i)), device_id_type=MESH
            )

        @pl.when(z > 0)
        def _():
            pl.semaphore_signal(
                semaphore, inc=1, device_id=(lax.rem(z + Z - 1, Z), w), device_id_type=MESH
            )

        @pl.when(z < Z - 1)
        def _():
            pl.semaphore_signal(
                semaphore, inc=1, device_id=(lax.rem(z + 1, Z), w), device_id_type=MESH
            )

    near_count = stages + jnp.where(z > 0, 1, 0) + jnp.where(z < Z - 1, 1, 0)

    fetches = [
        pltpu.make_async_copy(far, near, fetch_sem.at[i])
        for i, (far, near) in enumerate(
            [
                (lows_far, lows),
                (held_far, held),
                (inverses_far, inverses),
                (state_far, state),
                (height_far, height_operator),
                (pressure_far, pressure_column),
                (thermal_far, thermal_response),
                (mass_far, mass_row),
            ]
        )
    ]
    tell(barrier)
    for distance in range(2, Z):

        @pl.when(z + distance < Z)
        def _():
            pl.semaphore_signal(
                barrier, inc=1, device_id=(lax.rem(z + distance, Z), w), device_id_type=MESH
            )

    for fetch in fetches:
        fetch.start()

    lane = lax.broadcasted_iota(jnp.int32, (1, LANES), 1)
    lane_pair = lane // per_pair
    lane_member = lax.rem(lane, per_pair) // (2 * slots)
    lane_slot = lax.rem(lax.rem(lane, per_pair), 2 * slots) // 2
    lane_part = lax.rem(lane, 2)
    spare = lane >= first_extra
    table_row = lax.broadcasted_iota(jnp.int32, (TABLE_ROWS, LANES), 0)
    with scope("small_fetch"):
        fetches[0].wait()
        fetches[1].wait()
    orders = jnp.full((1, LANES), -1, jnp.int32)
    for s in range(slots):
        orders = jnp.where(lane_slot == s, held[s], orders)
    low_tile = jnp.zeros((TABLE_ROWS, LANES), jnp.int32)
    for j in range(pairs):
        low_tile = jnp.where(table_row == j, lows[j], low_tile)
    low_rows[z] = low_tile

    def split_inverses():
        fetches[2].wait()
        to_row = lax.broadcasted_iota(jnp.int32, (2 * rows, 2 * levels), 0)
        from_row = lax.broadcasted_iota(jnp.int32, (2 * rows, 2 * levels), 1)
        wanted = jnp.where(to_row < rows, 2 * to_row, 2 * (to_row - rows) + 1)
        split = jnp.where(wanted == from_row, 1.0, 0.0).astype(jnp.bfloat16)
        parts = []
        for j in range(pairs):
            both = jnp.dot(
                split,
                inverses[j].reshape(2 * levels, levels),
                preferred_element_type=jnp.float32,
            )
            for member in range(2):
                matrix = both[member * rows : (member + 1) * rows]
                matrices[z, 2 * j + member] = matrix.astype(jnp.bfloat16)
                parts.append(matrix)
        blank = jnp.zeros((LANES, LANES - border), jnp.float32)
        under = [matrix[LANES:levels, 0:LANES] for matrix in parts]
        aside = jnp.concatenate([m[0:LANES, LANES:levels] for m in parts] + [blank], axis=1)
        corner = [m[LANES:levels, LANES:levels] for m in parts] + [blank[0:tail]]
        corner = jnp.concatenate(corner, axis=1)
        filler = jnp.zeros((LANES - 2 * border - tail, LANES), jnp.float32)
        edge = jnp.concatenate([*under, aside.T[0:border], corner, filler], axis=0)
        edges[z] = edge.astype(jnp.bfloat16)

    @pl.when(z < Z - 1)
    def _():
        with scope("split"):
            split_inverses()

    with scope("barrier"):
        pl.semaphore_wait(barrier, near_count + jnp.where(z > 1, z - 1, 0))

    def z_copy(g, c, way):
        if c < pairs:
            ref = matrices.at[g, pl.ds(2 * c, 2), pl.ds(0, LANES), pl.ds(0, LANES)]
        else:
            ref = edges.at[g]
        step = 1 if way == 0 else -1
        return pltpu.make_async_remote_copy(
            src_ref=ref,
            dst_ref=ref,
            send_sem=z_send.at[0 if c < pairs else 1, way],
            recv_sem=z_recv.at[g, c],
            device_id=(z + step, w),
            device_id_type=MESH,
        )

    def forward(g, c):
        @pl.when(jnp.logical_and(g <= z, z < Z - 1))
        def _():
            z_copy(g, c, 0).start()

        @pl.when(jnp.logical_and(g >= z, z > 0))
        def _():
            z_copy(g, c, 1).start()

    def group_at(t):
        g = z
        for zz in range(Z):
            by_distance = sorted(range(Z), key=lambda a: (abs(a - zz), abs(2 * a - Z + 1)))
            g = jnp.where(z == zz, by_distance[t], g)
        return g

    def relay_now(*steps):
        for t, c in steps:
            g = group_at(t)
            z_copy(g, c, 0).wait_recv()
            forward(g, c)

    def relay(*steps):
        @pl.when(middle)
        def _():
            relay_now(*steps)

    def arrive(*steps):
        @pl.when(jnp.logical_not(middle))
        def _():
            for t, c in steps:
                z_copy(group_at(t), c, 0).wait_recv()

    groups = [group_at(t) for t in range(Z)]

    def row_copy(g):
        return pltpu.make_async_remote_copy(
            src_ref=low_rows.at[z],
            dst_ref=low_rows.at[z],
            send_sem=row_send,
            recv_sem=row_recv.at[z],
            device_id=(g, w),
            device_id_type=MESH,
        )

    def send_rows(*distances):
        for step in distances:

            @pl.when(jnp.logical_and(z + step >= 0, z + step < Z))
            def _():
                row_copy(z + step).start()

    def wait_row(g):
        pltpu.make_async_remote_copy(
            src_ref=low_rows.at[g],
            dst_ref=low_rows.at[g],
            send_sem=row_send,
            recv_sem=row_recv.at[g],
            device_id=(g, w),
            device_id_type=MESH,
        ).wait_recv()

    def table_copy(table, b, k):
        return pltpu.make_async_remote_copy(
            src_ref=table.at[w],
            dst_ref=table.at[w],
            send_sem=info_send.at[b],
            recv_sem=info_recv.at[b],
            device_id=(z, peer(k)),
            device_id_type=MESH,
        )

    def send_table(table, b):
        def start(n, carry):
            table_copy(table, b, W - n).start()
            return carry

        lax.fori_loop(1, W, start, 0)

    def all_tables(table, b):
        return pltpu.make_async_remote_copy(
            src_ref=table.at[pl.ds(0, W - 1)],
            dst_ref=table.at[pl.ds(0, W - 1)],
            send_sem=info_send.at[b],
            recv_sem=info_recv.at[b],
            device_id=(z, peer(1)),
            device_id_type=MESH,
        )

    send_rows(-1, 1, *range(-2, -Z, -1))
    tell(known.at[0])

    @pl.when(z == Z - 1)
    def _():
        with scope("split_end"):
            split_inverses()

    own_chunks = [pairs, *range(pairs)]

    def steps(t, first, stop=None):
        return [(t, c) for c in own_chunks[first:stop]]

    free_right = z == Z - 2
    free_left = z > 0

    def send_middle():
        @pl.when(middle)
        def _():
            for c in own_chunks[1:]:
                send_own(c, False)

    def send_ends():
        @pl.when(jnp.logical_not(middle))
        def _():
            for c in own_chunks[1:]:
                send_own(c, False)

    def send_own(c, free):
        right = free_right if free else jnp.logical_not(free_right)
        left = free_left if free else jnp.logical_not(free_left)

        @pl.when(jnp.logical_and(right, z < Z - 1))
        def _():
            z_copy(z, c, 0).start()

        @pl.when(jnp.logical_and(left, z > 0))
        def _():
            z_copy(z, c, 1).start()

    send_own(pairs, False)
    for c in own_chunks:
        send_own(c, True)

    column = lax.broadcasted_iota(jnp.int32, (1, width), 1)
    column_order = jnp.full((1, width), -1, jnp.int32)
    column_start = jnp.zeros((1, width), jnp.int32)
    for s in range(slots):
        inside = jnp.logical_and(column >= s * slot_width, column < (s + 1) * slot_width)
        column_order = jnp.where(inside, held[s], column_order)
        column_start = jnp.where(inside, s * slot_width, column_start)

    def choose():
        for ref, dimension in ((pick_extra, 0), (put_extra, 1)):
            row = lax.broadcasted_iota(jnp.int32, ref.shape, dimension)
            at = lax.broadcasted_iota(jnp.int32, ref.shape, 1 - dimension)
            k, own = lax.rem(row // LANES, W), lax.rem(row, LANES)
            first_half = row < W * LANES
            if dimension == 0:
                last = own - first_extra
                valid = jnp.logical_or(first_half, own < first_extra + 2)
                valid = jnp.logical_and(valid, own >= first_extra)
            else:
                last = own // spans
                valid = jnp.where(first_half, own - first_extra, 2 * spans - 1 - own) >= 0
            offset = jnp.where(first_half, own - first_extra, 2 * last_slot + last)
            wanted = jnp.where(valid, 2 * slots * k + offset, -1)
            ref[...] = jnp.where(at == wanted, 1.0, 0.0).astype(jnp.bfloat16)

    def drive_right():
        coefficient = (column - column_start) // 2
        degree = jnp.where(
            coefficient <= truncation - column_order, column_order + coefficient, coefficient - 1
        )
        lap_scale = (degree * (degree + 1)).astype(jnp.float32) / denom
        fetches[4].wait()
        fetches[5].wait()
        height = height_operator[...].astype(jnp.float32)
        pressure_row = jnp.broadcast_to(
            pressure_column[...].astype(jnp.float32).reshape(1, levels), height.shape
        )
        across = lax.broadcasted_iota(jnp.int32, height.shape, 1)
        down = lax.broadcasted_iota(jnp.int32, height.shape, 0)
        pressure_side = jnp.sum(
            jnp.where(across == down, pressure_row, 0.0), axis=1, keepdims=True
        )
        height = jnp.concatenate(
            [jnp.zeros((levels, tail), jnp.float32), height, pressure_side], axis=1
        ).astype(jnp.bfloat16)
        fetches[3].wait()
        drive = jnp.dot(height, state[LANES:, :], preferred_element_type=jnp.float32)
        right[0:levels, :] = (
            state[0:levels, :].astype(jnp.float32) + lap_scale * drive
        ).astype(jnp.bfloat16)

    for i in range(1, rounds):
        with scope(f"known{i}"):
            pl.semaphore_wait(known.at[i - 1], near_count)
        if i + 1 < Z:
            send_rows(i + 1)
        if i + 1 < rounds:
            tell(known.at[i])
        if i == 1:
            send_middle()
    send_ends()
    with scope("rows_wait"):
        wait_row(groups[1])
    table = [low_rows[groups[t]][0:pairs] for t in range(2)]
    table += [jnp.broadcast_to(orders, (TABLE_ROWS - 2 * pairs, LANES))]
    info[w] = jnp.concatenate(table, axis=0)
    send_table(info, 0)
    with scope("drive"):
        drive_right()
    choose()
    with scope("row_far"):
        wait_row(groups[2])
        wait_row(groups[3])
    table = [low_rows[groups[t]][0:pairs] for t in range(2, 4)]
    table += [jnp.zeros((TABLE_ROWS - 2 * pairs, LANES), jnp.int32)]
    far_info[w] = jnp.concatenate(table, axis=0)
    send_table(far_info, 1)

    @pl.when(middle)
    def _():
        with scope("relay_a"):
            relay_now(*steps(1, 0, 3), *steps(2, 0, 2))

    with scope("info_wait"):
        all_tables(info, 0).wait_recv()

    def low_of(d, t, j):
        row = t % 2 * pairs + j
        return (info if t < 2 else far_info)[d][row : row + 1]

    def target_of(b, k):
        d = peer(k)
        pair = lax.rem(lane_pair + block_pairs - lax.rem(k, block_pairs), block_pairs)
        low = jnp.zeros((1, LANES), jnp.int32)
        for p in range(block_pairs):
            low = jnp.where(pair == p, low_of(d, 2 * b + p // pairs, p % pairs), low)
        slot, order = lane_slot, orders
        used = lane >= 0
        if b == 0:
            slot = jnp.where(spare, last_slot, slot)
            order = jnp.where(spare, held[last_slot], order)
            used = lane < first_extra + 2
        merged = jnp.where(order <= low, low - order, truncation + 1 - low)
        position = jnp.where(lane_member == 0, merged, truncation - low - order)
        position = jnp.where(spare, truncation + 1 - order, position)
        target = slot * slot_width + 2 * position + lane_part
        return jnp.where(jnp.logical_and(used, order >= 0), target, -1)

    def build(b, i, place):
        at = lax.broadcasted_iota(jnp.int32, (width, LANES), 0)
        for h in range(2):
            pick[block_of(b), place, :, h * LANES : (h + 1) * LANES] = jnp.where(
                at == target_of(b, 2 * i + h), 1.0, 0.0
            ).astype(jnp.bfloat16)

    def block_of(b):
        return b if keep else 0

    def place_of(i):
        return i if keep else 0

    def out_copy(b, k):
        return pltpu.make_async_remote_copy(
            src_ref=outgoing.at[b, k],
            dst_ref=arrived.at[b, k],
            send_sem=out_send.at[b],
            recv_sem=out_recv.at[b],
            device_id=(z, peer(k)),
            device_id_type=MESH,
        )

    def back_copy(b, k):
        return pltpu.make_async_remote_copy(
            src_ref=solved.at[b, k],
            dst_ref=returned.at[b, k],
            send_sem=back_send.at[b],
            recv_sem=back_recv.at[b, k // 2],
            device_id=(z, peer(k)),
            device_id_type=MESH,
        )

    def send_block(b, first, stop):
        def send(step, carry):
            i = W // 2 - 1 - step
            targets = jnp.concatenate([target_of(b, 2 * i), target_of(b, 2 * i + 1)], axis=1)
            message = jnp.zeros((rows, 2 * LANES), jnp.float32)
            for start in range(0, width, CHUNK):
                count = min(CHUNK, width - start)
                at = lax.broadcasted_iota(jnp.int32, (count, 2 * LANES), 0) + start
                chosen = jnp.where(at == targets, 1.0, 0.0).astype(jnp.bfloat16)
                pick[block_of(b), place_of(i), start : start + count, :] = chosen
                message += jnp.dot(
                    right[:, start : start + count], chosen, preferred_element_type=jnp.float32
                )
            message = message.astype(jnp.bfloat16)
            k0, k1 = 2 * i, 2 * i + 1
            outgoing[b, k0] = message[:, :LANES]
            outgoing[b, k1] = message[:, LANES:]

            @pl.when(i > 0)
            def _():
                out_copy(b, k0).start()

            out_copy(b, k1).start()
            return carry

        lax.fori_loop(first, stop, send, 0)

    def all_out(b):
        return pltpu.make_async_remote_copy(
            src_ref=outgoing.at[b, pl.ds(1, W - 1)],
            dst_ref=arrived.at[b, pl.ds(1, W - 1)],
            send_sem=out_send.at[b],
            recv_sem=out_recv.at[b],
            device_id=(z, peer(1)),
            device_id_type=MESH,
        )

    def some_back(b, first, count):
        return pltpu.make_async_remote_copy(
            src_ref=solved.at[b, pl.ds(first, count)],
            dst_ref=returned.at[b, pl.ds(first, count)],
            send_sem=back_send.at[b],
            recv_sem=back_recv.at[b, first // 2],
            device_id=(z, peer(1)),
            device_id_type=MESH,
        )

    with scope("send0"):
        send_block(0, 0, W // 4)
    with scope("relay_b"):
        relay(*steps(1, 3), *steps(2, 2, 3))
    with scope("send0b"):
        send_block(0, W // 4, W // 2)
    with scope("relay_c"):
        relay(*steps(2, 3), *steps(3, 0, 1))
    with scope("far_wait"):
        all_tables(far_info, 1).wait_recv()
    with scope("send1"):
        send_block(1, 0, W // 4)
    with scope("relay_d"):
        relay(*steps(3, 1, 2))
    with scope("send1b"):
        send_block(1, W // 4, W // 2)
    with scope("relay_e"):
        relay(*steps(3, 2, 3))
    for b in range(2):
        arrived[b, 0] = outgoing[b, 0]

    def fill_edges(t):
        g = groups[t]
        edge = edges[g].astype(jnp.float32)
        across = edge.T
        for i in range(2 * pairs):
            at = i * tail
            side = across[:, border + at : border + at + tail]
            below = jnp.concatenate(
                [edge[at : at + tail], edge[2 * border : 2 * border + tail, at : at + tail]],
                axis=1,
            )
            matrices[g, i, 0:LANES, LANES:levels] = side.astype(jnp.bfloat16)
            matrices[g, i, LANES:levels, :] = below.astype(jnp.bfloat16)

    def spread(row):
        return jnp.concatenate([row] * tiles, axis=1)

    source_orders = [
        info[peer(k)][2 * pairs : 2 * pairs + 1] for k in range(W)
    ]

    def place(p, k):
        return lane_pair == (p + k) % block_pairs

    def pack(b, p):
        for v in range(tiles):
            first = v * block_pairs
            columns = arrived[b, first, 0:levels, :]
            order = source_orders[first]
            for k in range(first + 1, min(first + block_pairs, W)):
                columns = jnp.where(place(p, k), arrived[b, k, 0:levels, :], columns)
                order = jnp.where(place(p, k), source_orders[k], order)
            part = slice(v * LANES, (v + 1) * LANES)
            packed[b * block_pairs + p, 0:levels, part] = columns
            if b == 0:
                packed_orders[p : p + 1, part] = order

    wide_member = spread(lane_member)

    def times(t, j, member, x):
        return jnp.dot(
            matrices[groups[t], 2 * j + member], x, preferred_element_type=jnp.float32
        )

    def solve(b, p):
        t, j = 2 * b + p // pairs, p % pairs
        x = packed[b * block_pairs + p, 0:levels, :]
        low = spread(low_of(w, t, j))
        use_low = jnp.logical_and(wide_member == 0, packed_orders[p : p + 1, :] <= low)
        y = jnp.where(use_low, times(t, j, 0, x), times(t, j, 1, x))
        return y.astype(jnp.bfloat16)

    def deal(answers, k):
        part = slice(k // block_pairs * LANES, (k // block_pairs + 1) * LANES)
        block = answers[0][:, part]
        for p in range(1, block_pairs):
            block = jnp.where(place(p, k), answers[p][:, part], block)
        return block

    def gather_extra(b):
        columns = jnp.concatenate([arrived[b, k, 0:levels, :] for k in range(W)], axis=1)
        start = (1 - b) * W * LANES
        chosen = pick_extra[start : start + W * LANES, :]
        return jnp.dot(columns, chosen, preferred_element_type=jnp.float32)

    def fold_mask(shape):
        level = lax.broadcasted_iota(jnp.int32, shape, 0)
        own = lax.rem(lax.broadcasted_iota(jnp.int32, shape, 1), LANES)
        return jnp.logical_and(level // fold == lax.rem(own, spans), own < 2 * spans)

    def fold_rows(shape, dimension):
        level = lax.broadcasted_iota(jnp.int32, shape, 1 - dimension)
        at = lax.broadcasted_iota(jnp.int32, shape, dimension)
        inside = jnp.logical_and(level < levels, at - tail == lax.rem(level, fold))
        return jnp.where(inside, 1.0, 0.0).astype(jnp.bfloat16)

    extra_width = extra_in.shape[1]

    def along(row):
        return jnp.concatenate([row] * (extra_width // LANES), axis=1)

    extra_lane = lax.broadcasted_iota(jnp.int32, (1, extra_width), 1)
    extra_slot = lax.rem(extra_lane, 2 * slots) // 2
    extra_order = jnp.full((1, extra_width), -1, jnp.int32)
    for k in range(W):
        for s in range(slots):
            here = jnp.logical_and(extra_lane // (2 * slots) == k, extra_slot == s)
            value = source_orders[k][:, 2 * s : 2 * s + 1]
            extra_order = jnp.where(here, value, extra_order)

    def solve_extra(y, steps):
        x = extra_in[0:levels, :]
        for t, j in steps:
            hit = extra_order == along(low_of(w, t, j))
            y = jnp.where(hit, times(t, j, 1, x).astype(jnp.bfloat16), y)
        return y

    with scope("arrive1"):
        relay(*steps(3, 3))
        arrive((1, pairs), *[(1, c) for c in range(pairs)], (2, pairs))
    fill_edges(1)
    fill_edges(2)
    with scope("wait0"):
        all_out(0).wait_recv()
    with scope("pack0"):
        for p in range(block_pairs):
            pack(0, p)
    with scope("near"):
        answers = [solve(0, p) for p in range(block_pairs)]
        for k in range(W - 1, -1, -1):
            solved[0, k] = jnp.where(spare, jnp.zeros((), jnp.bfloat16), deal(answers, k))
            if k > 0:
                back_copy(0, k).start()
    with scope("extra0"):
        extra_part = gather_extra(0)
    with scope("edges3"):
        arrive((3, pairs))
        fill_edges(3)
    with scope("wait1"):
        all_out(1).wait_recv()
    with scope("arrive2"):
        arrive(*[(2, c) for c in range(pairs)], *[(3, c) for c in range(pairs - 1)])
    with scope("pack1"):
        extra_in[0:levels, :] = (gather_extra(1) + extra_part).astype(jnp.bfloat16)
        for p in range(block_pairs):
            pack(1, p)
    with scope("late"):
        answers = [solve(1, p) for p in range(block_pairs - 1)]
        order = [(t, j) for t in range(Z) for j in range(pairs)]
        extra = jnp.zeros(extra_in.shape, jnp.bfloat16)
        extra = solve_extra(extra, order[:-1])
    with scope("arrive3"):
        arrive((3, pairs - 1))
    with scope("last"):
        extra = solve_extra(extra, order[-1:])
        answers.append(solve(1, block_pairs - 1))
        extra_back = jnp.dot(extra, put_extra[...], preferred_element_type=jnp.float32)
        half = W * LANES
        spread_last = jnp.where(fold_mask((rows, half)), extra_back[:, half:], 0.0)
        folded = jnp.dot(
            fold_rows((rows - LANES, rows), 0),
            spread_last.astype(jnp.bfloat16),
            preferred_element_type=jnp.float32,
        )
        under = lax.broadcasted_iota(jnp.int32, (rows - LANES, LANES), 0) >= tail
        here = jnp.logical_and(under, lane < 2 * spans)
        for k in range(W - 1, -1, -1):
            part = slice(k * LANES, (k + 1) * LANES)
            block = deal(answers, k)
            block = jnp.where(spare, extra_back[:, part].astype(jnp.bfloat16), block)
            bottom = jnp.where(here, folded[:, part], block[LANES:].astype(jnp.float32))
            solved[1, k, 0:LANES, :] = block[0:LANES]
            solved[1, k, LANES:rows, :] = bottom.astype(jnp.bfloat16)
            if k > 0:
                back_copy(1, k).start()

    fetches[6].wait()
    fetches[7].wait()
    total[...] = jnp.zeros_like(total)
    through_row = lax.broadcasted_iota(jnp.int32, (tail, levels), 0)
    through_lane = lax.broadcasted_iota(jnp.int32, (tail, levels), 1)
    response = jnp.concatenate(
        [
            jnp.where(through_lane == through_row + LANES, -1.0, 0.0),
            thermal_response[...].astype(jnp.float32),
            mass_row[...].astype(jnp.float32).reshape(1, levels),
        ],
        axis=0,
    ).astype(jnp.bfloat16)

    def collect(b, i, first, second):
        if not keep:
            build(b, i, 0)
        total[...] += lax.dot_general(
            jnp.concatenate([first, second], axis=1),
            pick[block_of(b), place_of(i)],
            (((1,), (1,)), ((), ())),
            preferred_element_type=jnp.float32,
        )

    def gather_back(b):
        last_pair = W // 2 - 1
        with scope(f"back{b}_0"):
            some_back(b, 1, 1).wait_recv()
            collect(b, 0, solved[b, 0], returned[b, 1])

        def step(i, carry):
            some_back(b, 2 * i, 2).wait_recv()
            collect(b, i, returned[b, 2 * i], returned[b, 2 * i + 1])
            return carry

        with scope(f"back{b}"):
            lax.fori_loop(1, last_pair, step, 0)
        with scope(f"back{b}_wait"):
            some_back(b, W - 2, 2).wait_recv()
        with scope(f"back{b}_last"):
            if b == 0:
                collect(b, last_pair, returned[b, W - 2], returned[b, W - 1])
            else:
                bottom = solved[b, 0, LANES:rows, :].astype(jnp.float32)
                for k in range(1, W):
                    bottom = bottom + returned[b, k, LANES:rows, :].astype(jnp.float32)
                unfolded = jnp.dot(
                    fold_rows((rows, rows - LANES), 1),
                    bottom.astype(jnp.bfloat16),
                    preferred_element_type=jnp.float32,
                )
                unfolded = jnp.where(fold_mask((rows, LANES)), unfolded, 0.0)
                total[...] += jnp.dot(
                    jnp.concatenate(
                        [returned[b, W - 2], returned[b, W - 1], unfolded.astype(jnp.bfloat16)],
                        axis=1,
                    ),
                    last_pick[...],
                    preferred_element_type=jnp.float32,
                )

    gather_back(0)
    with scope("last_pick"):
        order = held[last_slot]
        folded_to = last_slot * slot_width + 2 * (truncation + 1 - order) + lane // spans
        folded_to = jnp.where(jnp.logical_and(order >= 0, lane < 2 * spans), folded_to, -1)
        targets = jnp.concatenate([target_of(1, W - 2), target_of(1, W - 1), folded_to], axis=1)
        targets = jnp.broadcast_to(targets.astype(jnp.float32), (TABLE_ROWS, 3 * LANES))
        targets = targets.T[:, 0:1].astype(jnp.int32)
        at = lax.broadcasted_iota(jnp.int32, (3 * LANES, width), 1)
        last_pick[...] = jnp.where(at == targets, 1.0, 0.0).astype(jnp.bfloat16)
    gather_back(1)

    with scope("final"):
        div = total[0:levels, :].astype(jnp.bfloat16)
        change = jnp.dot(response, div, preferred_element_type=jnp.float32)
        old = state[LANES:, :].astype(jnp.float32)
        below = lax.broadcasted_iota(jnp.int32, old.shape, 0) < tail
        new = jnp.where(below, 0.0, old) - change
        new = jnp.where(column_order >= 0, new, 0.0)
        out[0:LANES, :] = div[0:LANES, :]
        out[LANES:, :] = new.astype(jnp.bfloat16)

    for b, table in ((0, info), (1, far_info)):
        all_out(b).wait_send()
        pltpu.make_async_remote_copy(
            src_ref=solved.at[b, pl.ds(1, W - 1)],
            dst_ref=returned.at[b, pl.ds(1, W - 1)],
            send_sem=back_send.at[b],
            recv_sem=back_recv.at[b, 0],
            device_id=(z, peer(1)),
            device_id_type=MESH,
        ).wait_send()
        all_tables(table, b).wait_send()
    pltpu.make_async_remote_copy(
        src_ref=low_rows.at[pl.ds(0, Z - 1)],
        dst_ref=low_rows.at[pl.ds(0, Z - 1)],
        send_sem=row_send,
        recv_sem=row_recv.at[1],
        device_id=(lax.rem(z + 1, Z), w),
        device_id_type=MESH,
    ).wait_send()

    def wait_relayed(count, way):
        for kind, ref in (
            (0, matrices.at[pl.ds(0, count), :, pl.ds(0, LANES), pl.ds(0, LANES)]),
            (1, edges.at[pl.ds(0, count)]),
        ):
            pltpu.make_async_remote_copy(
                src_ref=ref,
                dst_ref=ref,
                send_sem=z_send.at[kind, way],
                recv_sem=z_recv.at[0, 0],
                device_id=(lax.rem(z + 1, Z), w),
                device_id_type=MESH,
            ).wait_send()

    for zz in range(Z):

        @pl.when(z == zz)
        def _():
            if zz < Z - 1:
                wait_relayed(zz + 1, 0)
            if zz > 0:
                wait_relayed(Z - zz, 1)


def shards(
    state,
    held_orders,
    pair_lows,
    inverses,
    height_operator,
    pressure_column,
    thermal_response_matrix,
    mass_row,
):
    levels = height_operator.shape[0]
    slots = held_orders.shape[0]
    pairs = pair_lows.shape[0]
    Z, W = lax.axis_size("grp"), lax.axis_size("wave")
    width = state.shape[1]
    rows = ceil_to(levels, ROWS_TILE)
    places = W // 2 if W * width * 4 * LANES <= KEEP_BYTES else 1
    tiles = -(-W // (2 * pairs))
    extra_width = ceil_to(2 * slots * W, LANES)
    block = pltpu.VMEM((2, W, rows, LANES), jnp.bfloat16)
    return pl.pallas_call(
        functools.partial(kernel, (Z, W, levels, slots, pairs)),
        out_shape=pltpu.VMEM(state.shape, jnp.bfloat16),
        in_specs=[pl.BlockSpec(memory_space=pl.ANY)] * 8,
        out_specs=pl.BlockSpec(memory_space=pltpu.VMEM),
        scratch_shapes=[
            pltpu.SMEM(held_orders.shape, jnp.int32),
            pltpu.SMEM(pair_lows.shape, jnp.int32),
            pltpu.VMEM(state.shape, jnp.bfloat16),
            pltpu.VMEM((pairs, levels, 2, levels), jnp.bfloat16),
            pltpu.VMEM(height_operator.shape, jnp.bfloat16),
            pltpu.VMEM(pressure_column.shape, jnp.bfloat16),
            pltpu.VMEM(thermal_response_matrix.shape, jnp.bfloat16),
            pltpu.VMEM(mass_row.shape, jnp.bfloat16),
            pltpu.VMEM((Z, TABLE_ROWS, LANES), jnp.int32),
            pltpu.VMEM((W, TABLE_ROWS, LANES), jnp.int32),
            pltpu.VMEM((W, TABLE_ROWS, LANES), jnp.int32),
            pltpu.VMEM((Z, 2 * pairs, rows, levels), jnp.bfloat16),
            pltpu.VMEM((Z, LANES, LANES), jnp.bfloat16),
            pltpu.VMEM((rows, width), jnp.bfloat16),
            pltpu.VMEM((2 if places > 1 else 1, places, width, 2 * LANES), jnp.bfloat16),
            block,
            block,
            block,
            block,
            pltpu.VMEM((4 * pairs, rows, tiles * LANES), jnp.bfloat16),
            pltpu.VMEM((ceil_to(2 * pairs, TABLE_ROWS), tiles * LANES), jnp.int32),
            pltpu.VMEM((2 * W * LANES, extra_width), jnp.bfloat16),
            pltpu.VMEM((rows, extra_width), jnp.bfloat16),
            pltpu.VMEM((extra_width, 2 * W * LANES), jnp.bfloat16),
            pltpu.VMEM((3 * LANES, width), jnp.bfloat16),
            pltpu.VMEM((rows, width), jnp.float32),
            pltpu.SemaphoreType.DMA,
            pltpu.SemaphoreType.DMA((Z,)),
            pltpu.SemaphoreType.DMA((2,)),
            pltpu.SemaphoreType.DMA((2,)),
            pltpu.SemaphoreType.DMA((2, 2)),
            pltpu.SemaphoreType.DMA((Z, pairs + 1)),
            pltpu.SemaphoreType.DMA((2,)),
            pltpu.SemaphoreType.DMA((2,)),
            pltpu.SemaphoreType.DMA((2,)),
            pltpu.SemaphoreType.DMA((2, W // 2)),
            pltpu.SemaphoreType.DMA((8,)),
            pltpu.SemaphoreType.REGULAR((max(W.bit_length() - 2, Z - 2),)),
        ],
        compiler_params=pltpu.CompilerParams(
            collective_id=0, has_side_effects=True, vmem_limit_bytes=61000 * 1024
        ),
    )(
        *[
            pltpu.with_memory_space_constraint(array, pltpu.HBM)
            for array in (
                held_orders,
                pair_lows,
                state,
                jnp.transpose(inverses, (0, 2, 1, 3)),
                height_operator,
                pressure_column,
                thermal_response_matrix,
                mass_row,
            )
        ]
    )


def solution(mesh):
    placed = (
        P(None, ("grp", "wave")),
        P(("grp", "wave")),
        P(("grp", "wave")),
        P(("grp", "wave"), None, None, None),
        P(),
        P(),
        P(),
        P(),
    )
    return jax.shard_map(
        shards, mesh=mesh, in_specs=placed, out_specs=P(None, ("grp", "wave")), check_vma=False
    )
```
